32 devices in a mesh: dp: 8 (over z, x), fsdp: 4 (over y, core).
Axes of the slice: x: 2, y: 2, z: 4, core: 2. Of those that a mesh axis runs over, the one named last changes fastest.
Arguments:
- tokens: bfloat16 [16384, 1024], P(('dp', 'fsdp')), may hold values from -6 to 6
- cluster_lengths: int32 [32, 8], P(('dp', 'fsdp')), may hold values from 1 to 128, 512 in all within a row
- norm_gain: bfloat16 [1024], P('fsdp'), may hold values from 0.099609375 to 1.8984375
- in_weight: bfloat16 [1024, 4096], P('fsdp'), may hold values from -0.1875 to 0.1875
- conv_weight: bfloat16 [4, 2048], P(None, 'fsdp'), may hold values from -3 to 3
- conv_bias: bfloat16 [2048], P('fsdp'), may hold values from -3 to 3
- xproj_weight: bfloat16 [2048, 96], P('fsdp'), may hold values from -0.125 to 0.125
- dt_weight: bfloat16 [64, 2048], P(None, 'fsdp'), may hold values from -0.75 to 0.75
- dt_bias: bfloat16 [2048], P('fsdp'), may hold values from -6.5 to -2
- a_log: bfloat16 [16, 2048], P(None, 'fsdp'), may hold values from 0 to 2.796875
- skip_gain: bfloat16 [2048], P('fsdp'), may hold values from 0.5 to 1.5
- out_weight: bfloat16 [2048, 1024], P('fsdp'), may hold values from -0.375 to 0.375
- cotangent: bfloat16 [16384, 1024], P(('dp', 'fsdp')), may hold values from -6 to 6
Outputs:
- output: bfloat16 [16384, 1024], P(('dp', 'fsdp'))
- input_grad: float32 [16384, 1024], P(('dp', 'fsdp'))
- gain_grad: float32 [1024], P('fsdp')
- in_grad: float32 [1024, 4096], P('fsdp')
- conv_weight_grad: float32 [4, 2048], P(None, 'fsdp')
- conv_bias_grad: float32 [2048], P('fsdp')
- xproj_grad: float32 [2048, 96], P('fsdp')
- dt_weight_grad: float32 [64, 2048], P(None, 'fsdp')
- dt_bias_grad: float32 [2048], P('fsdp')
- a_log_grad: float32 [16, 2048], P(None, 'fsdp')
- skip_grad: float32 [2048], P('fsdp')
- out_grad: float32 [2048, 1024], P('fsdp')
The draws below stay inside these ranges and needn't reach their ends.
Inputs may be any that keep to these rules, and one draw needn't show every extreme that they name: `cluster_lengths`: each row holds the lengths of the 8 clusters packed into one context, in order; they sum to 512 and the longest is exactly 128.
All inputs are finite; a program needn't handle non-finite values.
Results may differ from the reference program's by a relative error of at most 0.011.
Values may be sent and summed in bfloat16 or wider, within the bound.
A program may use at most 256 MiB of HBM per device.

```python
import math
import jax
import jax.numpy as jnp
import numpy as np
from jax import lax

D = 1024
DI = 2048
NSTATE = 16
KCONV = 4
RANK = 64
LENGTH = 512
CLUSTERS = 8
BLOCK = 16
MOST = 128
XW = 96
CONTEXTS = 32
TOKENS = 16384


def steps_of(own_key, extent, split, least, top_value):
    level = 1.0
    for axis_at, shards_of in split:
        steps = jax.random.uniform(jax.random.fold_in(jax.random.fold_in(own_key, 6), axis_at), (shards_of,), jnp.float32, least / len(split), top_value / len(split))
        level = level * jnp.repeat(jnp.exp(steps), extent[axis_at] // shards_of).reshape((-1,) + (1,) * (len(extent) - 1 - axis_at))
    return level


def profile(amount, total, bound, lean):
    portions = [(1 << 20) // math.isqrt(grade ** lean) + 1 for grade in range(2, amount + 1)]
    surplus, given = total - bound - (amount - 1), [1] * (amount - 1)
    while surplus > 0:
        candidates = [i for i in range(amount - 1) if given[i] < bound]
        pool, budget = sum([portions[i] for i in candidates]), surplus
        for i in candidates:
            extra = min(bound - given[i], max(1, budget * portions[i] // pool), surplus)
            given[i] = given[i] + extra
            surplus = surplus - extra
    return np.array([bound] + given)


def ragged_sizes(key, amount, total, limit, skew):
    if amount == 2:
        one = jax.random.randint(key, (), max(1, total - limit), min(limit, total - 1) + 1)
        return jnp.stack([one, total - one])
    tallies = jnp.asarray(profile(amount, total, limit, skew), jnp.int32)
    couples = (amount - 1) // 2
    giver, sink = tallies[1:1 + 2 * couples:2], tallies[2:2 + 2 * couples:2]
    margin = jnp.minimum(giver - 1, limit - sink)
    moved = jax.random.randint(jax.random.fold_in(key, 1), (couples,), 0, 1 << 20) % (margin + 1)
    tallies = tallies.at[1:1 + 2 * couples:2].set(giver - moved).at[2:2 + 2 * couples:2].set(sink + moved)
    return tallies[jax.random.permutation(jax.random.fold_in(key, 2), amount)]


def bell_draw(own_key, dims, spread, limit, shards=(), kind=jnp.bfloat16):
    level = steps_of(own_key, dims, shards, -0.22, 0.18) if shards else 1.0
    entries = jax.random.normal(own_key, dims, jnp.float32) * spread * level
    return jnp.minimum(jnp.maximum(entries, -limit), limit).astype(kind)


def setup_inputs(seed: int = 0) -> dict:
    splits = jax.random.split(jax.random.key(seed), 14)
    return {
        "tokens": bell_draw(splits[0], (TOKENS, D), 1.0, 6.0, ((0, 32),)),
        "cluster_lengths": jax.vmap(lambda own: ragged_sizes(own, CLUSTERS, LENGTH, MOST, 1))(jax.random.split(splits[1], CONTEXTS)).reshape((CONTEXTS, CLUSTERS)).astype(jnp.int32),
        "norm_gain": jnp.clip(1.0 + 0.18 * jax.random.normal(splits[2], (D,), jnp.float32), 0.099609375, 1.8984375).astype(jnp.bfloat16),
        "in_weight": bell_draw(splits[3], (D, 2 * DI), D ** -0.5, 0.1875, ((0, 4),)),
        "conv_weight": bell_draw(splits[4], (KCONV, DI), KCONV ** -0.5, 3.0, ((1, 4),)),
        "conv_bias": bell_draw(splits[5], (DI,), 0.5, 3.0, ((0, 4),)),
        "xproj_weight": bell_draw(splits[6], (DI, XW), DI ** -0.5, 0.125, ((0, 4),)),
        "dt_weight": bell_draw(splits[7], (RANK, DI), RANK ** -0.5, 0.75, ((1, 4),)),
        "dt_bias": jnp.clip(-6.5 + 4.5 * jax.random.uniform(splits[8], (DI,), jnp.float32) ** steps_of(splits[8], (DI,), ((0, 4),), -0.2, 0.2), -6.5, -2.0).astype(jnp.bfloat16),
        "a_log": jnp.clip(2.796875 * jax.random.uniform(splits[9], (NSTATE, DI), jnp.float32) ** steps_of(splits[9], (NSTATE, DI), ((1, 4),), -0.2, 0.2), 0.0, 2.796875).astype(jnp.bfloat16),
        "skip_gain": jnp.clip(0.5 + 1.0 * jax.random.uniform(splits[10], (DI,), jnp.float32) ** steps_of(splits[10], (DI,), ((0, 4),), -0.2, 0.2), 0.5, 1.5).astype(jnp.bfloat16),
        "out_weight": bell_draw(splits[11], (DI, D), (DI // 8) ** -0.5, 0.375, ((0, 4),)),
        "cotangent": bell_draw(splits[12], (TOKENS, D), 1.0, 6.0, ((0, 32),)),
    }


@jax.custom_vjp
def low(v):
    return lax.optimization_barrier(v.astype(jnp.bfloat16)).astype(jnp.float32)

@jax.custom_vjp
def low_back(v):
    return v

def low_keep(v):
    return (low(v), None)

def low_pass(kept, grad):
    return (grad,)

def back_keep(v):
    return (v, None)

def back_low(kept, grad):
    return (low(grad),)
low.defvjp(low_keep, low_pass)
low_back.defvjp(back_keep, back_low)
epsilon = 1e-05

def product(former, latter):
    return jnp.einsum('gtk,kn->gtn', former, latter, precision=lax.Precision.HIGHEST)

def silu_of(values):
    return values * jax.nn.sigmoid(values)

def cluster_masks(lengths):
    cluster_ends = jnp.cumsum(lengths, axis=-1)
    starts = cluster_ends - lengths
    positions = jnp.arange(LENGTH, dtype=jnp.int32)
    before = starts[:, None, :] <= positions[None, :, None]
    segment_start = lax.optimization_barrier(jnp.max(jnp.where(before, starts[:, None, :], 0), axis=-1))
    keep_mask = (positions[None, :] > segment_start).astype(jnp.float32)
    lag_index = jnp.arange(KCONV, dtype=jnp.int32)
    tap_valid = (positions[None, :, None] - lag_index[None, None, :] >= segment_start[:, :, None]).astype(jnp.float32)
    return (tap_valid, keep_mask)

def selective_scan(step_size, drive, b_mat, c_mat, keep_mask, decay_rate):
    blocks = LENGTH // BLOCK

    def arrange(values):
        rotated = jnp.moveaxis(values, 1, 0)
        return rotated.reshape((blocks, BLOCK) + rotated.shape[1:])

    def one_step(carried, inputs):
        step_t, drive_t, b_t, c_t, keep_t = inputs
        factor = keep_t[:, None, None] * jnp.exp(step_t[:, None, :] * decay_rate[None])
        carried = factor * carried + b_t[:, :, None] * drive_t[:, None, :]
        return (carried, lax.optimization_barrier(jnp.sum(c_t[:, :, None] * carried, axis=1)))

    @jax.checkpoint
    def one_block(carried, inputs):
        return lax.scan(one_step, carried, inputs)
    initial = jnp.zeros((step_size.shape[0], NSTATE, DI), jnp.float32)
    last_state, emitted = lax.scan(one_block, initial, tuple((arrange(values) for values in (step_size, drive, b_mat, c_mat, keep_mask))))
    emitted = emitted.reshape((LENGTH,) + emitted.shape[2:])
    return jnp.moveaxis(emitted, 0, 1)

def mamba_layer(tokens_in, norm_gain, in_weight, conv_weight, conv_bias, xproj_weight, dt_weight, dt_bias, a_log, skip_gain, out_weight, tap_valid, keep_mask):
    mean_square = lax.optimization_barrier(jnp.mean(tokens_in * tokens_in, axis=-1, keepdims=True))
    normed = tokens_in * lax.rsqrt(mean_square + epsilon) * norm_gain
    mixed_in = low_back(product(low(normed), in_weight))
    inner_in = mixed_in[..., :DI]
    gate_in = mixed_in[..., DI:]
    padded = jnp.pad(inner_in, ((0, 0), (KCONV - 1, 0), (0, 0)))
    conv_out = jnp.zeros_like(inner_in) + conv_bias
    for offset in range(KCONV):
        lag_now = KCONV - 1 - offset
        conv_out = conv_out + conv_weight[offset] * padded[:, offset:offset + LENGTH, :] * tap_valid[:, :, lag_now][:, :, None]
    conv_act = silu_of(conv_out)
    projected = low_back(product(low(conv_act), xproj_weight))
    dt_low = projected[..., :RANK]
    b_mat = projected[..., RANK:RANK + NSTATE]
    c_mat = projected[..., RANK + NSTATE:]
    step_size = jax.nn.softplus(low_back(product(low(dt_low), dt_weight)) + dt_bias)
    decay_rate = -jnp.exp(a_log)
    scanned = selective_scan(step_size, step_size * conv_act, b_mat, c_mat, keep_mask, decay_rate)
    gated = (scanned + skip_gain * conv_act) * silu_of(gate_in)
    return tokens_in + product(low(gated), out_weight)

def reference(tokens, cluster_lengths, norm_gain, in_weight, conv_weight, conv_bias, xproj_weight, dt_weight, dt_bias, a_log, skip_gain, out_weight, cotangent):
    weights = (norm_gain.astype(jnp.float32), in_weight.astype(jnp.float32), conv_weight.astype(jnp.float32), conv_bias.astype(jnp.float32), xproj_weight.astype(jnp.float32), dt_weight.astype(jnp.float32), dt_bias.astype(jnp.float32), a_log.astype(jnp.float32), skip_gain.astype(jnp.float32), out_weight.astype(jnp.float32))
    contexts = max(1, min(CONTEXTS, 4096 // LENGTH))
    group_count = CONTEXTS // contexts
    inputs = tokens.astype(jnp.float32).reshape(group_count, contexts, LENGTH, D)
    upstream = cotangent.astype(jnp.float32).reshape(group_count, contexts, LENGTH, D)
    grouped_lengths = cluster_lengths.reshape(group_count, contexts, CLUSTERS)

    def one_group(summed, element):
        group_tokens, group_upstream, group_lengths = element
        tap_valid, keep_mask = cluster_masks(group_lengths)

        def forward(tokens_in, gain_in, in_w, conv_w, conv_b, xproj_w, dt_w, dt_b, alog_in, skip_in, out_w):
            return mamba_layer(tokens_in, gain_in, in_w, conv_w, conv_b, xproj_w, dt_w, dt_b, alog_in, skip_in, out_w, tap_valid, keep_mask)
        result, pullback = jax.vjp(forward, group_tokens, *weights)
        gradients = pullback(group_upstream)
        summed = tuple((former + latter for former, latter in zip(summed, gradients[1:])))
        return (summed, (result, gradients[0]))
    initial = tuple((jnp.zeros_like(weight) for weight in weights))
    summed, (results, token_grads) = lax.scan(one_group, initial, (inputs, upstream, grouped_lengths))
    return (results.reshape(TOKENS, D).astype(jnp.bfloat16), token_grads.reshape(TOKENS, D), summed[0], summed[1], summed[2], summed[3], summed[4], summed[5], summed[6], summed[7], summed[8], summed[9])
```

```python
import jax
import jax.numpy as jnp
import numpy as np
from jax import lax
from jax.experimental import pallas as pl
from jax.experimental.pallas import tpu as pltpu
from jax.sharding import PartitionSpec as P

KCONV = 4
LENGTH = 512
LOG2E = float(np.log2(np.e))
LN2 = float(np.log(2.0))
FAR = 1e30


epsilon = 1e-05


def matmul(former, latter):
    return jnp.dot(former, latter, preferred_element_type=jnp.float32)


def left_inner(former, latter):
    return lax.dot_general(
        former, latter, (((0,), (0,)), ((), ())), preferred_element_type=jnp.float32
    )


def right_inner(former, latter):
    return lax.dot_general(
        former, latter, (((1,), (1,)), ((), ())), preferred_element_type=jnp.float32
    )


def silu_of(values):
    return values * jax.nn.sigmoid(values)


def silu_slope(values):
    logistic = jax.nn.sigmoid(values)
    return logistic * (1.0 + values * (1.0 - logistic))


def cluster_masks(lengths):
    cluster_ends = jnp.cumsum(lengths, axis=-1)
    starts = cluster_ends - lengths
    positions = jnp.arange(LENGTH, dtype=jnp.int32)
    before = starts[:, None, :] <= positions[None, :, None]
    segment_start = jnp.max(jnp.where(before, starts[:, None, :], 0), axis=-1)
    keep_mask = (positions[None, :] > segment_start).astype(jnp.float32)
    lag_index = jnp.arange(KCONV, dtype=jnp.int32)
    tap_valid = (
        positions[None, :, None] - lag_index[None, None, :] >= segment_start[:, :, None]
    ).astype(jnp.float32)
    return (tap_valid[0], keep_mask[0])

LANE = 128
NS = 16
TC = 32
CGF = 1024
CGB = 512


def bcast(ref, i, row):
    v = ref[i, pl.ds(row, 8, stride=0), :]
    return jnp.concatenate([v, v], axis=0)


def stage(src, dst):
    for i in range(dst.shape[0]):
        dst[i] = src[:, i * LANE:(i + 1) * LANE]


def fold(src, i):
    s = [src[i, pl.ds(q, 8, stride=8), :] for q in range(8)]
    return ((s[0] + s[1]) + (s[2] + s[3])) + ((s[4] + s[5]) + (s[6] + s[7]))


def fwd_kernel(dt_ref, dr_ref, b_ref, c_ref, a_ref, y_ref, hs_ref, part, dts, drs, hst):
    cg = dt_ref.shape[1]
    tiles = cg // LANE
    tc = dt_ref.shape[0]

    @pl.when(pl.program_id(1) == 0)
    def _():
        hst[...] = jnp.zeros_like(hst)

    hs_ref[0] = hst[...]
    stage(dt_ref, dts)
    stage(dr_ref, drs)

    def group(g, carry):
        t0 = pl.multiple_of(g * 8, 8)
        hs = list(carry)
        for k in range(8):
            bt = b_ref[t0 + k]
            ct = c_ref[t0 + k]
            for i in range(tiles):
                ln = slice(i * LANE, (i + 1) * LANE)
                d = bcast(dts, i, t0 + k)
                u = bcast(drs, i, t0 + k)
                a = jnp.exp2(d * a_ref[:, ln])
                h = a * hs[i] + bt * u
                hs[i] = h
                p = ct * h
                part[i, k * 8:(k + 1) * 8, :] = p[:8] + p[8:]
        for i in range(tiles):
            ln = slice(i * LANE, (i + 1) * LANE)
            y_ref[pl.ds(t0, 8), ln] = fold(part, i)
        return tuple(hs)

    init = tuple(hst[:, i * LANE:(i + 1) * LANE] for i in range(tiles))
    out = lax.fori_loop(0, tc // 8, group, init)
    for i in range(tiles):
        hst[:, i * LANE:(i + 1) * LANE] = out[i]


def scan_forward(dt, dr, bx, cx, a2, tc=TC, cg=CGF):
    t, c = dt.shape
    nt, nc = t // tc, c // cg
    return pl.pallas_call(
        fwd_kernel,
        grid=(nc, nt),
        in_specs=[
            pl.BlockSpec((tc, cg), lambda j, i: (i, j)),
            pl.BlockSpec((tc, cg), lambda j, i: (i, j)),
            pl.BlockSpec((tc, NS, LANE), lambda j, i: (i, 0, 0)),
            pl.BlockSpec((tc, NS, LANE), lambda j, i: (i, 0, 0)),
            pl.BlockSpec((NS, cg), lambda j, i: (0, j)),
        ],
        out_specs=[
            pl.BlockSpec((tc, cg), lambda j, i: (i, j)),
            pl.BlockSpec((1, NS, cg), lambda j, i: (i, 0, j)),
        ],
        out_shape=[
            jax.ShapeDtypeStruct((t, c), jnp.float32),
            jax.ShapeDtypeStruct((nt, NS, c), jnp.float32),
        ],
        scratch_shapes=[pltpu.VMEM((cg // LANE, 64, LANE), jnp.float32)] + [pltpu.VMEM((cg // LANE, tc, LANE), jnp.float32)] * 2 + [pltpu.VMEM((NS, cg), jnp.float32)],
        name="scan_forward",
    )(dt, dr, bx, cx, a2)


def bwd_kernel(dt_ref, dr_ref, dy_ref, b_ref, c_ref, a_ref, hs_ref,
               za_ref, gb_ref, db_ref, dc_ref, rate_ref, asc, hsc, pz, pg, dts, drs, dys, gst, rst):
    cg = dt_ref.shape[1]
    tiles = cg // LANE
    tc = dt_ref.shape[0]
    j = pl.program_id(0)
    i_t = pl.program_id(1)
    nt = pl.num_programs(1)

    @pl.when(i_t == 0)
    def _():
        gst[...] = jnp.zeros_like(gst)
        rst[...] = jnp.zeros_like(rst)

    stage(dt_ref, dts)
    stage(dr_ref, drs)
    stage(dy_ref, dys)
    lanes = [slice(i * LANE, (i + 1) * LANE) for i in range(tiles)]

    def fgroup(g, carry):
        t0 = pl.multiple_of(g * 8, 8)
        hs = list(carry)
        for k in range(8):
            bt = b_ref[t0 + k]
            for i in range(tiles):
                ln = lanes[i]
                d = bcast(dts, i, t0 + k)
                u = bcast(drs, i, t0 + k)
                a = jnp.exp2(d * a_ref[:, ln])
                asc[t0 + k, :, ln] = a
                hsc[t0 + k, :, ln] = hs[i]
                hs[i] = a * hs[i] + bt * u
        return tuple(hs)

    out = lax.fori_loop(0, tc // 8, fgroup, tuple(hs_ref[0, :, ln] for ln in lanes))
    for i in range(tiles):
        hsc[tc, :, lanes[i]] = out[i]

    base = pl.multiple_of((nt - 1 - i_t) * tc, tc)
    first = j == 0

    def bgroup(gi, carry):
        g = tc // 8 - 1 - gi
        t0 = pl.multiple_of(g * 8, 8)
        gs = list(carry[0])
        rs = list(carry[1])
        for k in range(7, -1, -1):
            bt = b_ref[t0 + k]
            ct = c_ref[t0 + k]
            accb = None
            for i in range(tiles):
                ln = lanes[i]
                d = bcast(dts, i, t0 + k)
                u = bcast(drs, i, t0 + k)
                w = bcast(dys, i, t0 + k)
                hnow = hsc[t0 + k + 1, :, ln]
                hprev = hsc[t0 + k, :, ln]
                a = asc[t0 + k, :, ln]
                gg = ct * w + gs[i]
                ga = gg * a
                z = ga * hprev
                rs[i] = rs[i] + z * d
                gs[i] = ga
                pa = z * a_ref[:, ln]
                pz[i, k * 8:(k + 1) * 8, :] = pa[:8] + pa[8:]
                pb = gg * bt
                pg[i, k * 8:(k + 1) * 8, :] = pb[:8] + pb[8:]
                vb = gg * u
                vc = w * hnow
                accb = vb if accb is None else accb + vb
                accc = vc if i == 0 else accc + vc
            row = base + t0 + k

            @pl.when(first)
            def _():
                db_ref[row] = accb
                dc_ref[row] = accc

            @pl.when(jnp.logical_not(first))
            def _():
                db_ref[row] = db_ref[row] + accb
                dc_ref[row] = dc_ref[row] + accc
        for i in range(tiles):
            ln = lanes[i]
            za_ref[pl.ds(t0, 8), ln] = fold(pz, i)
            gb_ref[pl.ds(t0, 8), ln] = fold(pg, i)
        return tuple(gs), tuple(rs)

    gs, rs = lax.fori_loop(0, tc // 8, bgroup, (tuple(gst[:, ln] for ln in lanes), tuple(rst[:, ln] for ln in lanes)))
    for i in range(tiles):
        gst[:, lanes[i]] = gs[i]
        rst[:, lanes[i]] = rs[i]

    @pl.when(i_t == nt - 1)
    def _():
        rate_ref[...] = rst[...]


def scan_backward(dt, dr, dy, bx, cx, a2, hs, tc=TC, cg=CGB):
    t, c = dt.shape
    nt, nc = t // tc, c // cg
    row = pl.BlockSpec((tc, cg), lambda j, i: (nt - 1 - i, j))
    bc = pl.BlockSpec((tc, NS, LANE), lambda j, i: (nt - 1 - i, 0, 0))
    full = pl.BlockSpec((t, NS, LANE), lambda j, i: (0, 0, 0))
    return pl.pallas_call(
        bwd_kernel,
        grid=(nc, nt),
        in_specs=[row, row, row, bc, bc, pl.BlockSpec((NS, cg), lambda j, i: (0, j)),
                  pl.BlockSpec((1, NS, cg), lambda j, i: (nt - 1 - i, 0, j))],
        out_specs=[row, row, full, full, pl.BlockSpec((NS, cg), lambda j, i: (0, j))],
        out_shape=[
            jax.ShapeDtypeStruct((t, c), jnp.float32),
            jax.ShapeDtypeStruct((t, c), jnp.float32),
            jax.ShapeDtypeStruct((t, NS, LANE), jnp.float32),
            jax.ShapeDtypeStruct((t, NS, LANE), jnp.float32),
            jax.ShapeDtypeStruct((NS, c), jnp.float32),
        ],
        scratch_shapes=[
            pltpu.VMEM((tc, NS, cg), jnp.float32), pltpu.VMEM((tc + 1, NS, cg), jnp.float32),
            pltpu.VMEM((cg // LANE, 64, LANE), jnp.float32), pltpu.VMEM((cg // LANE, 64, LANE), jnp.float32),
            pltpu.VMEM((cg // LANE, tc, LANE), jnp.float32), pltpu.VMEM((cg // LANE, tc, LANE), jnp.float32), pltpu.VMEM((cg // LANE, tc, LANE), jnp.float32),
            pltpu.VMEM((NS, cg), jnp.float32), pltpu.VMEM((NS, cg), jnp.float32),
        ],
        compiler_params=pltpu.CompilerParams(vmem_limit_bytes=56 << 20),
        name="scan_backward",
    )(dt, dr, dy, bx, cx, a2, hs)


def pack_small(gain, conv_w, conv_b, xproj, dt_w, dt_b, alog, skip):
    width = conv_b.shape[-1]
    gain_row = jnp.pad(gain[None], ((0, 0), (0, width - gain.shape[0])))
    return jnp.concatenate(
        [xproj.T, dt_w, alog, conv_w, conv_b[None], dt_b[None], skip[None], gain_row], axis=0
    )


def body(
    tokens,
    cluster_lengths,
    norm_gain,
    in_weight,
    conv_weight,
    conv_bias,
    xproj_weight,
    dt_weight,
    dt_bias,
    a_log,
    skip_gain,
    out_weight,
    cotangent,
):
    low = jnp.bfloat16
    gain_shard = norm_gain.shape[0]
    width = conv_bias.shape[0]
    packed = pack_small(norm_gain, conv_weight, conv_bias, xproj_weight, dt_weight, dt_bias, a_log, skip_gain)
    in_full = lax.all_gather(in_weight, "fsdp", axis=0, tiled=True)
    small = lax.all_gather(packed, "fsdp", axis=0)
    out_full = lax.all_gather(out_weight, "fsdp", axis=0, tiled=True)
    shards = small.shape[0]
    xw, rank, state = xproj_weight.shape[1], dt_weight.shape[0], a_log.shape[0]
    rows = jnp.moveaxis(small, 0, 1).reshape(small.shape[1], shards * width)
    xproj_t = rows[:xw]
    dt_full = rows[xw : xw + rank]
    at = xw + rank
    alog_full = rows[at : at + state]
    at += state
    conv_taps = rows[at : at + KCONV].astype(jnp.float32)
    at += KCONV
    conv_offset = rows[at].astype(jnp.float32)
    dt_offset = rows[at + 1].astype(jnp.float32)
    skip_value = rows[at + 2].astype(jnp.float32)
    gain_value = small[:, at + 3, :gain_shard].reshape(-1).astype(jnp.float32)
    decay_rate = -jnp.exp(alog_full.astype(jnp.float32))
    inner_width = shards * width
    length = tokens.shape[0]
    tap_valid, keep_mask = cluster_masks(cluster_lengths)
    inputs_full = tokens.astype(jnp.float32)
    mean_square = jnp.mean(inputs_full * inputs_full, axis=-1, keepdims=True)
    inverse_rms = lax.rsqrt(mean_square + epsilon)
    unit_rows = inputs_full * inverse_rms
    normed_low = (unit_rows * gain_value).astype(low)
    mixed_in = matmul(normed_low, in_full)
    inner_in = mixed_in[:, :inner_width]
    gate_in = mixed_in[:, inner_width:]
    padded = jnp.pad(inner_in, ((KCONV - 1, 0), (0, 0)))
    conv_out = jnp.zeros_like(inner_in) + conv_offset
    for offset in range(KCONV):
        lag_now = KCONV - 1 - offset
        conv_out = (
            conv_out
            + conv_taps[offset]
            * padded[offset : offset + length]
            * tap_valid[:, lag_now : lag_now + 1]
        )
    conv_act = silu_of(conv_out)
    act_low = conv_act.astype(low)
    projected = right_inner(act_low, xproj_t)
    dt_rounded = projected[:, :rank].astype(low)
    b_mat = projected[:, rank : rank + state]
    c_mat = projected[:, rank + state :]
    dt_pre = matmul(dt_rounded, dt_full) + dt_offset
    step_size = jax.nn.softplus(dt_pre)
    drive = step_size * conv_act
    step_far = jnp.where(keep_mask[:, None] > 0, step_size, FAR)
    rate2 = decay_rate * LOG2E
    bx = jnp.broadcast_to(b_mat[:, :, None], (length, state, LANE))
    cx = jnp.broadcast_to(c_mat[:, :, None], (length, state, LANE))
    scanned, starts = scan_forward(step_far, drive, bx, cx, rate2)
    with_skip = scanned + skip_value * conv_act
    gate_act = silu_of(gate_in)
    gated_low = (with_skip * gate_act).astype(low)
    result = inputs_full + matmul(gated_low, out_full)
    output = result.astype(low)
    out_grad = left_inner(gated_low, cotangent)
    gated_grad = right_inner(cotangent, out_full)
    skip_part = gated_grad * gate_act
    gate_grad = gated_grad * with_skip * silu_slope(gate_in)
    gate_low = gate_grad.astype(low)
    gate_in_grad = left_inner(normed_low, gate_low)
    out_share = reduce_grad(out_grad)
    gate_share = reduce_grad(gate_in_grad)
    skip_grad = jnp.sum(skip_part * conv_act, axis=0)
    za, gb, dbx, dcx, rate_grad = scan_backward(step_far, drive, skip_part, bx, cx, rate2, starts)
    a_log_grad = rate_grad * decay_rate
    step_grad = za * LN2 + gb * conv_act
    act_scan = gb * step_size
    b_grad = jnp.sum(dbx, axis=-1)
    c_grad = jnp.sum(dcx, axis=-1)
    pre_grad = step_grad * jax.nn.sigmoid(dt_pre)
    dt_bias_grad = jnp.sum(pre_grad, axis=0)
    pre_low = pre_grad.astype(low)
    dt_weight_grad = left_inner(dt_rounded, pre_low)
    rank_grad = right_inner(pre_low, dt_full)
    proj_grad = jnp.concatenate([rank_grad, b_grad, c_grad], axis=1).astype(low)
    xproj_grad = left_inner(proj_grad, act_low)
    act_grad = matmul(proj_grad, xproj_t) + skip_part * skip_value + act_scan
    conv_grad = act_grad * silu_slope(conv_out)
    conv_bias_grad = jnp.sum(conv_grad, axis=0)
    inner_grad = jnp.zeros_like(inner_in)
    tap_grads = []
    for offset in range(KCONV):
        lag_now = KCONV - 1 - offset
        masked = conv_grad * tap_valid[:, lag_now : lag_now + 1]
        tap_grads.append(jnp.sum(masked * padded[offset : offset + length], axis=0))
        inner_grad = (
            inner_grad + conv_taps[offset] * jnp.pad(masked, ((0, lag_now), (0, 0)))[lag_now:]
        )
    conv_weight_grad = jnp.stack(tap_grads)
    inner_low = inner_grad.astype(low)
    inner_in_grad = left_inner(normed_low, inner_low)
    normed_grad = right_inner(inner_low, in_full[:, :inner_width]) + right_inner(
        gate_low, in_full[:, inner_width:]
    )
    gain_grad = jnp.sum(normed_grad * unit_rows, axis=0)
    scaled = normed_grad * gain_value
    input_grad = cotangent.astype(jnp.float32) + inverse_rms * (
        scaled - unit_rows * jnp.mean(scaled * unit_rows, axis=-1, keepdims=True)
    )
    gain_rows = jnp.pad(gain_grad.reshape(shards, gain_shard), ((0, 0), (0, width - gain_shard)))
    small_grad = jnp.concatenate(
        [
            xproj_grad,
            dt_weight_grad,
            a_log_grad,
            conv_weight_grad,
            conv_bias_grad[None],
            dt_bias_grad[None],
            skip_grad[None],
            gain_rows.reshape(1, -1),
        ],
        axis=0,
    )
    unit = lax.axis_size("dp") * 8
    small_grad = jnp.pad(small_grad, ((0, -small_grad.shape[0] % unit), (0, 0)))
    small_rows = small_grad.shape[0]
    small_grad = jnp.moveaxis(small_grad.reshape(small_rows, shards, width), 1, 0)
    inner_share = reduce_grad(inner_in_grad)
    small_share = reduce_grad(small_grad.reshape(shards * small_rows, width))
    at = xw + rank + state
    return (
        output,
        input_grad,
        small_share[at + KCONV + 3, :gain_shard],
        jnp.concatenate([inner_share, gate_share], axis=1),
        small_share[at : at + KCONV],
        small_share[at + KCONV],
        small_share[:xw].T,
        small_share[xw : xw + rank],
        small_share[at + KCONV + 1],
        small_share[xw + rank : at],
        small_share[at + KCONV + 2],
        out_share,
    )


def reduce_grad(value):
    part = lax.psum_scatter(value.astype(jnp.bfloat16), "fsdp", scatter_dimension=0, tiled=True)
    part = lax.psum_scatter(part, "dp", scatter_dimension=0, tiled=True)
    return lax.all_gather(part, "dp", axis=0, tiled=True).astype(jnp.float32)


def solution(mesh):
    in_specs = (
        P(("dp", "fsdp"), None),
        P(("dp", "fsdp"), None),
        P("fsdp"),
        P("fsdp", None),
        P(None, "fsdp"),
        P("fsdp"),
        P("fsdp", None),
        P(None, "fsdp"),
        P("fsdp"),
        P(None, "fsdp"),
        P("fsdp"),
        P("fsdp", None),
        P(("dp", "fsdp"), None),
    )
    out_specs = (
        P(("dp", "fsdp"), None),
        P(("dp", "fsdp"), None),
        P("fsdp"),
        P("fsdp", None),
        P(None, "fsdp"),
        P("fsdp"),
        P("fsdp", None),
        P(None, "fsdp"),
        P("fsdp"),
        P(None, "fsdp"),
        P("fsdp"),
        P("fsdp", None),
    )
    return jax.shard_map(body, mesh=mesh, in_specs=in_specs, out_specs=out_specs, check_vma=False)
```

```python
import jax
import jax.numpy as jnp
import numpy as np
from jax import lax
from jax.experimental import pallas as pl
from jax.experimental.pallas import tpu as pltpu
from jax.sharding import PartitionSpec as P

KCONV = 4
LENGTH = 512
LOG2E = float(np.log2(np.e))
LN2 = float(np.log(2.0))
FAR = 1e30


epsilon = 1e-05


def matmul(former, latter):
    return jnp.dot(former, latter, preferred_element_type=jnp.float32)


def left_inner(former, latter):
    return lax.dot_general(
        former, latter, (((0,), (0,)), ((), ())), preferred_element_type=jnp.float32
    )


def right_inner(former, latter):
    return lax.dot_general(
        former, latter, (((1,), (1,)), ((), ())), preferred_element_type=jnp.float32
    )


def silu_of(values):
    return values * jax.nn.sigmoid(values)


def silu_slope(values):
    logistic = jax.nn.sigmoid(values)
    return logistic * (1.0 + values * (1.0 - logistic))


def cluster_masks(lengths):
    cluster_ends = jnp.cumsum(lengths, axis=-1)
    starts = cluster_ends - lengths
    positions = jnp.arange(LENGTH, dtype=jnp.int32)
    before = starts[:, None, :] <= positions[None, :, None]
    segment_start = jnp.max(jnp.where(before, starts[:, None, :], 0), axis=-1)
    keep_mask = (positions[None, :] > segment_start).astype(jnp.float32)
    lag_index = jnp.arange(KCONV, dtype=jnp.int32)
    tap_valid = (
        positions[None, :, None] - lag_index[None, None, :] >= segment_start[:, :, None]
    ).astype(jnp.float32)
    return (tap_valid[0], keep_mask[0])

LANE = 128
NS = 16
TC = 32
CGF = 1024
CGB = 512


def bcast(ref, i, row):
    v = ref[i, pl.ds(row, 8, stride=0), :]
    return jnp.concatenate([v, v], axis=0)


def stage(src, dst):
    for i in range(dst.shape[0]):
        dst[i] = src[:, i * LANE:(i + 1) * LANE]


def fold(src, i):
    s = [src[i, pl.ds(q, 8, stride=8), :] for q in range(8)]
    return ((s[0] + s[1]) + (s[2] + s[3])) + ((s[4] + s[5]) + (s[6] + s[7]))


def fwd_kernel(dt_ref, dr_ref, b_ref, c_ref, a_ref, y_ref, hs_ref, part, dts, drs, hst):
    cg = dt_ref.shape[1]
    tiles = cg // LANE
    tc = dt_ref.shape[0]

    @pl.when(pl.program_id(1) == 0)
    def _():
        hst[...] = jnp.zeros_like(hst)

    hs_ref[0] = hst[...]
    stage(dt_ref, dts)
    stage(dr_ref, drs)

    def group(g, carry):
        t0 = pl.multiple_of(g * 8, 8)
        hs = list(carry)
        for k in range(8):
            bt = b_ref[t0 + k]
            ct = c_ref[t0 + k]
            for i in range(tiles):
                ln = slice(i * LANE, (i + 1) * LANE)
                d = bcast(dts, i, t0 + k)
                u = bcast(drs, i, t0 + k)
                a = jnp.exp2(d * a_ref[:, ln])
                h = a * hs[i] + bt * u
                hs[i] = h
                p = ct * h
                part[i, k * 8:(k + 1) * 8, :] = p[:8] + p[8:]
        for i in range(tiles):
            ln = slice(i * LANE, (i + 1) * LANE)
            y_ref[pl.ds(t0, 8), ln] = fold(part, i)
        return tuple(hs)

    init = tuple(hst[:, i * LANE:(i + 1) * LANE] for i in range(tiles))
    out = lax.fori_loop(0, tc // 8, group, init)
    for i in range(tiles):
        hst[:, i * LANE:(i + 1) * LANE] = out[i]


def scan_forward(dt, dr, bx, cx, a2, tc=TC, cg=CGF):
    t, c = dt.shape
    nt, nc = t // tc, c // cg
    return pl.pallas_call(
        fwd_kernel,
        grid=(nc, nt),
        in_specs=[
            pl.BlockSpec((tc, cg), lambda j, i: (i, j)),
            pl.BlockSpec((tc, cg), lambda j, i: (i, j)),
            pl.BlockSpec((tc, NS, LANE), lambda j, i: (i, 0, 0)),
            pl.BlockSpec((tc, NS, LANE), lambda j, i: (i, 0, 0)),
            pl.BlockSpec((NS, cg), lambda j, i: (0, j)),
        ],
        out_specs=[
            pl.BlockSpec((tc, cg), lambda j, i: (i, j)),
            pl.BlockSpec((1, NS, cg), lambda j, i: (i, 0, j)),
        ],
        out_shape=[
            jax.ShapeDtypeStruct((t, c), jnp.float32),
            jax.ShapeDtypeStruct((nt, NS, c), jnp.float32),
        ],
        scratch_shapes=[pltpu.VMEM((cg // LANE, 64, LANE), jnp.float32)] + [pltpu.VMEM((cg // LANE, tc, LANE), jnp.float32)] * 2 + [pltpu.VMEM((NS, cg), jnp.float32)],
        name="scan_forward",
    )(dt, dr, bx, cx, a2)


def bwd_kernel(dt_ref, dr_ref, dy_ref, b_ref, c_ref, a_ref, hs_ref,
               za_ref, gb_ref, db_ref, dc_ref, rate_ref, asc, hsc, pz, pg, dts, drs, dys, gst, rst):
    cg = dt_ref.shape[1]
    tiles = cg // LANE
    tc = dt_ref.shape[0]
    j = pl.program_id(0)
    i_t = pl.program_id(1)
    nt = pl.num_programs(1)

    @pl.when(i_t == 0)
    def _():
        gst[...] = jnp.zeros_like(gst)
        rst[...] = jnp.zeros_like(rst)

    stage(dt_ref, dts)
    stage(dr_ref, drs)
    stage(dy_ref, dys)
    lanes = [slice(i * LANE, (i + 1) * LANE) for i in range(tiles)]

    def fgroup(g, carry):
        t0 = pl.multiple_of(g * 8, 8)
        hs = list(carry)
        for k in range(8):
            bt = b_ref[t0 + k]
            for i in range(tiles):
                ln = lanes[i]
                d = bcast(dts, i, t0 + k)
                u = bcast(drs, i, t0 + k)
                a = jnp.exp2(d * a_ref[:, ln])
                asc[t0 + k, :, ln] = a
                hsc[t0 + k, :, ln] = hs[i]
                hs[i] = a * hs[i] + bt * u
        return tuple(hs)

    out = lax.fori_loop(0, tc // 8, fgroup, tuple(hs_ref[0, :, ln] for ln in lanes))
    for i in range(tiles):
        hsc[tc, :, lanes[i]] = out[i]

    base = pl.multiple_of((nt - 1 - i_t) * tc, tc)
    first = j == 0

    def bgroup(gi, carry):
        g = tc // 8 - 1 - gi
        t0 = pl.multiple_of(g * 8, 8)
        gs = list(carry[0])
        rs = list(carry[1])
        for k in range(7, -1, -1):
            bt = b_ref[t0 + k]
            ct = c_ref[t0 + k]
            accb = None
            for i in range(tiles):
                ln = lanes[i]
                d = bcast(dts, i, t0 + k)
                u = bcast(drs, i, t0 + k)
                w = bcast(dys, i, t0 + k)
                hnow = hsc[t0 + k + 1, :, ln]
                hprev = hsc[t0 + k, :, ln]
                a = asc[t0 + k, :, ln]
                gg = ct * w + gs[i]
                ga = gg * a
                z = ga * hprev
                rs[i] = rs[i] + z * d
                gs[i] = ga
                pa = z * a_ref[:, ln]
                pz[i, k * 8:(k + 1) * 8, :] = pa[:8] + pa[8:]
                pb = gg * bt
                pg[i, k * 8:(k + 1) * 8, :] = pb[:8] + pb[8:]
                vb = gg * u
                vc = w * hnow
                accb = vb if accb is None else accb + vb
                accc = vc if i == 0 else accc + vc
            row = base + t0 + k

            @pl.when(first)
            def _():
                db_ref[row] = accb
                dc_ref[row] = accc

            @pl.when(jnp.logical_not(first))
            def _():
                db_ref[row] = db_ref[row] + accb
                dc_ref[row] = dc_ref[row] + accc
        for i in range(tiles):
            ln = lanes[i]
            za_ref[pl.ds(t0, 8), ln] = fold(pz, i)
            gb_ref[pl.ds(t0, 8), ln] = fold(pg, i)
        return tuple(gs), tuple(rs)

    gs, rs = lax.fori_loop(0, tc // 8, bgroup, (tuple(gst[:, ln] for ln in lanes), tuple(rst[:, ln] for ln in lanes)))
    for i in range(tiles):
        gst[:, lanes[i]] = gs[i]
        rst[:, lanes[i]] = rs[i]

    @pl.when(i_t == nt - 1)
    def _():
        rate_ref[...] = rst[...]


def scan_backward(dt, dr, dy, bx, cx, a2, hs, tc=TC, cg=CGB):
    t, c = dt.shape
    nt, nc = t // tc, c // cg
    row = pl.BlockSpec((tc, cg), lambda j, i: (nt - 1 - i, j))
    bc = pl.BlockSpec((tc, NS, LANE), lambda j, i: (nt - 1 - i, 0, 0))
    full = pl.BlockSpec((t, NS, LANE), lambda j, i: (0, 0, 0))
    return pl.pallas_call(
        bwd_kernel,
        grid=(nc, nt),
        in_specs=[row, row, row, bc, bc, pl.BlockSpec((NS, cg), lambda j, i: (0, j)),
                  pl.BlockSpec((1, NS, cg), lambda j, i: (nt - 1 - i, 0, j))],
        out_specs=[row, row, full, full, pl.BlockSpec((NS, cg), lambda j, i: (0, j))],
        out_shape=[
            jax.ShapeDtypeStruct((t, c), jnp.float32),
            jax.ShapeDtypeStruct((t, c), jnp.float32),
            jax.ShapeDtypeStruct((t, NS, LANE), jnp.float32),
            jax.ShapeDtypeStruct((t, NS, LANE), jnp.float32),
            jax.ShapeDtypeStruct((NS, c), jnp.float32),
        ],
        scratch_shapes=[
            pltpu.VMEM((tc, NS, cg), jnp.float32), pltpu.VMEM((tc + 1, NS, cg), jnp.float32),
            pltpu.VMEM((cg // LANE, 64, LANE), jnp.float32), pltpu.VMEM((cg // LANE, 64, LANE), jnp.float32),
            pltpu.VMEM((cg // LANE, tc, LANE), jnp.float32), pltpu.VMEM((cg // LANE, tc, LANE), jnp.float32), pltpu.VMEM((cg // LANE, tc, LANE), jnp.float32),
            pltpu.VMEM((NS, cg), jnp.float32), pltpu.VMEM((NS, cg), jnp.float32),
        ],
        compiler_params=pltpu.CompilerParams(vmem_limit_bytes=56 << 20),
        name="scan_backward",
    )(dt, dr, dy, bx, cx, a2, hs)


MESH = pl.DeviceIdType.MESH
COLS = 1024
ROWS = 32
SLACK = 3


class Reducer:

    def __init__(self, dp, sources, targets, scratch):
        self.nz = dp // 2
        self.sources, self.targets = sources, targets
        (self.rc, self.ry, self.rx, self.rz, self.s_one, self.r_one, self.s_rs, self.r_rs, self.s_ag, self.r_ag) = scratch
        self.me_dp, self.me_f = lax.axis_index("dp"), lax.axis_index("fsdp")
        self.fh, self.fl = self.me_f // 2, self.me_f % 2
        self.z, self.x = self.me_dp // 2, self.me_dp % 2
        self.pieces_c, self.rows = split_of(dp)
        self.pieces_r = self.nz // self.pieces_c
        self.chunks = chunk_list([t.shape for t in targets], self.rows)
        self.core = (self.me_dp, self.fh * 2 + (1 - self.fl))
        self.other = (self.me_dp, (1 - self.fh) * 2 + self.fl)
        self.pair = (self.z * 2 + (1 - self.x), self.me_f)

    def peer(self, o):
        return lax.rem(self.z + o, self.nz)

    def entry(self):
        barrier = pltpu.get_barrier_semaphore()
        ids = [self.core, self.other, self.pair] + [(self.peer(o) * 2 + self.x, self.me_f) for o in range(1, self.nz)]
        for d in ids:
            pl.semaphore_signal(barrier, inc=1, device_id=d, device_id_type=MESH)
        pl.semaphore_wait(barrier, len(ids))

    def copy(self, src, dst, send, recv, device):
        return pltpu.make_async_remote_copy(src_ref=src, dst_ref=dst, send_sem=send, recv_sem=recv, device_id=device, device_id_type=MESH)

    def copies(self, stage, k):
        a, r0, c0, w = self.chunks[k]
        r, hr = self.rows, self.rows // 2
        if stage == 0:
            src = self.sources[a].at[:, 1 - self.fl, r0:r0 + r, c0:c0 + w]
            return [self.copy(src, self.rc.at[k, :, :, :w], self.s_one.at[0, k], self.r_one.at[0, k], self.core)]
        if stage == 1:
            return [self.copy(self.rc.at[k, 1 - self.fh, :, :w], self.ry.at[k, :, :w], self.s_one.at[1, k], self.r_one.at[1, k], self.other)]
        if stage == 2:
            src = self.ry.at[k, pl.ds(pl.multiple_of((1 - self.x) * hr, hr), hr), :w]
            return [self.copy(src, self.rx.at[k, :, :w], self.s_one.at[2, k], self.r_one.at[2, k], self.pair)]
        out = []
        if stage == 5:
            rows = pl.ds(pl.multiple_of(r0 + self.x * hr, hr), hr)
            t = self.targets[a].at[rows, c0:c0 + w]
            return [self.copy(t, t, self.s_one.at[3, k], self.r_one.at[3, k], self.pair)]
        for o in range(1, self.nz):
            j = self.peer(o)
            device = (j * 2 + self.x, self.me_f)
            if stage == 3:
                pr, pc = self.place(j, w)
                out.append(self.copy(self.rx.at[k, pr, pc], self.rz.at[k, o - 1, :, :w // self.pieces_c], self.s_rs.at[k, o - 1], self.r_rs.at[k, o - 1], device))
            else:
                t = self.own(k)
                out.append(self.copy(t, t, self.s_ag.at[k, o - 1], self.r_ag.at[k, o - 1], device))
        return out

    def place(self, j, w, r0=0, c0=0):
        pr, pw = self.rows // 2 // self.pieces_r, w // self.pieces_c
        return (pl.ds(pl.multiple_of(r0 + (j // self.pieces_c) * pr, 16), pr), pl.ds(pl.multiple_of(c0 + lax.rem(j, self.pieces_c) * pw, 128), pw))

    def own(self, k):
        a, r0, c0, w = self.chunks[k]
        pr, pc = self.place(self.z, w, r0 + self.x * (self.rows // 2), c0)
        return self.targets[a].at[pr, pc]

    def absorb(self, stage, k):
        a, r0, c0, w = self.chunks[k]
        r, hr = self.rows, self.rows // 2
        for c in self.copies(stage, k):
            c.wait_recv()
        if stage == 0:
            for h in range(2):
                self.rc[k, h, :, :w] = self.rc[k, h, :, :w] + self.sources[a][h, self.fl, r0:r0 + r, c0:c0 + w]
        elif stage == 1:
            self.ry[k, :, :w] = self.ry[k, :, :w] + self.rc[k, self.fh, :, :w]
        elif stage == 2:
            mine = self.ry[k, pl.ds(pl.multiple_of(self.x * hr, hr), hr), :w]
            self.rx[k, :, :w] = self.rx[k, :, :w] + mine
        elif stage == 3:
            pr, pc = self.place(self.z, w)
            total = self.rx[k, pr, pc].astype(jnp.float32)
            for o in range(1, self.nz):
                total = total + self.rz[k, o - 1, :, :w // self.pieces_c].astype(jnp.float32)
            self.own(k)[...] = total.astype(jnp.bfloat16)

    def ticks(self):
        return len(self.chunks) + 6 * SLACK

    def tick(self, n):
        live = [(s, n - SLACK * s) for s in range(7) if 0 <= n - SLACK * s < len(self.chunks)]
        for s, k in reversed(live):
            if s > 0:
                self.absorb(s - 1, k)
        for s, k in reversed(live):
            if s < 6:
                for c in self.copies(s, k):
                    c.start()

    def finish(self):
        for k in range(len(self.chunks)):
            for s in range(6):
                for c in self.copies(s, k):
                    c.wait_send()


def split_of(dp):
    nz = dp // 2
    pieces_c = min(nz, COLS // 128, 4)
    return pieces_c, max(ROWS, 32 * (nz // pieces_c))


def chunk_list(shapes, rows):
    out = []
    for a, (r, c) in enumerate(shapes):
        w = min(c, COLS)
        for r0 in range(0, r, rows):
            for c0 in range(0, c, w):
                out.append((a, r0, c0, w))
    return out


def reducer_scratch(dp, shapes):
    nz = dp // 2
    pieces_c, rows = split_of(dp)
    n = len(chunk_list(shapes, rows))
    low = jnp.bfloat16
    return [
        pltpu.VMEM((n, 2, rows, COLS), low),
        pltpu.VMEM((n, rows, COLS), low),
        pltpu.VMEM((n, rows // 2, COLS), low),
        pltpu.VMEM((n, nz - 1, rows // 2 // (nz // pieces_c), COLS // pieces_c), low),
        pltpu.SemaphoreType.DMA((4, n)),
        pltpu.SemaphoreType.DMA((4, n)),
        pltpu.SemaphoreType.DMA((n, nz - 1)),
        pltpu.SemaphoreType.DMA((n, nz - 1)),
        pltpu.SemaphoreType.DMA((n, nz - 1)),
        pltpu.SemaphoreType.DMA((n, nz - 1)),
    ]


def reduce_all(dp, arrays, collective_id):
    shapes = [a.shape[1:] for a in arrays]
    na = len(arrays)
    scratch = reducer_scratch(dp, shapes)

    def kernel(*refs):
        red = Reducer(dp, refs[:na], refs[na:2 * na], refs[2 * na:])
        red.entry()
        for n in range(red.ticks()):
            red.tick(n)
        red.finish()

    return pl.pallas_call(
        kernel,
        out_shape=[jax.ShapeDtypeStruct(s, jnp.bfloat16) for s in shapes],
        in_specs=[pl.BlockSpec(memory_space=pltpu.VMEM)] * na,
        out_specs=[pl.BlockSpec(memory_space=pltpu.VMEM)] * na,
        scratch_shapes=scratch,
        compiler_params=pltpu.CompilerParams(collective_id=collective_id, has_side_effects=True, vmem_limit_bytes=60 << 20),
        name="reduce_all",
    )(*[a.reshape((2, 2) + a.shape[1:]) for a in arrays])


def pack_small(gain, conv_w, conv_b, xproj, dt_w, dt_b, alog, skip):
    width = conv_b.shape[-1]
    gain_row = jnp.pad(gain[None], ((0, 0), (0, width - gain.shape[0])))
    return jnp.concatenate(
        [xproj.T, dt_w, alog, conv_w, conv_b[None], dt_b[None], skip[None], gain_row], axis=0
    )


def body(
    tokens,
    cluster_lengths,
    norm_gain,
    in_weight,
    conv_weight,
    conv_bias,
    xproj_weight,
    dt_weight,
    dt_bias,
    a_log,
    skip_gain,
    out_weight,
    cotangent,
):
    low = jnp.bfloat16
    gain_shard = norm_gain.shape[0]
    width = conv_bias.shape[0]
    packed = pack_small(norm_gain, conv_weight, conv_bias, xproj_weight, dt_weight, dt_bias, a_log, skip_gain)
    in_full = lax.all_gather(in_weight, "fsdp", axis=0, tiled=True)
    small = lax.all_gather(packed, "fsdp", axis=0)
    out_full = lax.all_gather(out_weight, "fsdp", axis=0, tiled=True)
    shards = small.shape[0]
    xw, rank, state = xproj_weight.shape[1], dt_weight.shape[0], a_log.shape[0]
    rows = jnp.moveaxis(small, 0, 1).reshape(small.shape[1], shards * width)
    xproj_t = rows[:xw]
    dt_full = rows[xw : xw + rank]
    at = xw + rank
    alog_full = rows[at : at + state]
    at += state
    conv_taps = rows[at : at + KCONV].astype(jnp.float32)
    at += KCONV
    conv_offset = rows[at].astype(jnp.float32)
    dt_offset = rows[at + 1].astype(jnp.float32)
    skip_value = rows[at + 2].astype(jnp.float32)
    gain_value = small[:, at + 3, :gain_shard].reshape(-1).astype(jnp.float32)
    decay_rate = -jnp.exp(alog_full.astype(jnp.float32))
    inner_width = shards * width
    length = tokens.shape[0]
    tap_valid, keep_mask = cluster_masks(cluster_lengths)
    inputs_full = tokens.astype(jnp.float32)
    mean_square = jnp.mean(inputs_full * inputs_full, axis=-1, keepdims=True)
    inverse_rms = lax.rsqrt(mean_square + epsilon)
    unit_rows = inputs_full * inverse_rms
    normed_low = (unit_rows * gain_value).astype(low)
    mixed_in = matmul(normed_low, in_full)
    inner_in = mixed_in[:, :inner_width]
    gate_in = mixed_in[:, inner_width:]
    padded = jnp.pad(inner_in, ((KCONV - 1, 0), (0, 0)))
    conv_out = jnp.zeros_like(inner_in) + conv_offset
    for offset in range(KCONV):
        lag_now = KCONV - 1 - offset
        conv_out = (
            conv_out
            + conv_taps[offset]
            * padded[offset : offset + length]
            * tap_valid[:, lag_now : lag_now + 1]
        )
    conv_act = silu_of(conv_out)
    act_low = conv_act.astype(low)
    projected = right_inner(act_low, xproj_t)
    dt_rounded = projected[:, :rank].astype(low)
    b_mat = projected[:, rank : rank + state]
    c_mat = projected[:, rank + state :]
    dt_pre = matmul(dt_rounded, dt_full) + dt_offset
    step_size = jax.nn.softplus(dt_pre)
    drive = step_size * conv_act
    step_far = jnp.where(keep_mask[:, None] > 0, step_size, FAR)
    rate2 = decay_rate * LOG2E
    bx = jnp.broadcast_to(b_mat[:, :, None], (length, state, LANE))
    cx = jnp.broadcast_to(c_mat[:, :, None], (length, state, LANE))
    scanned, starts = scan_forward(step_far, drive, bx, cx, rate2)
    with_skip = scanned + skip_value * conv_act
    gate_act = silu_of(gate_in)
    gated_low = (with_skip * gate_act).astype(low)
    result = inputs_full + matmul(gated_low, out_full)
    output = result.astype(low)
    out_grad = left_inner(gated_low, cotangent)
    gated_grad = right_inner(cotangent, out_full)
    skip_part = gated_grad * gate_act
    gate_grad = gated_grad * with_skip * silu_slope(gate_in)
    gate_low = gate_grad.astype(low)
    gate_in_grad = left_inner(normed_low, gate_low)
    skip_grad = jnp.sum(skip_part * conv_act, axis=0)
    za, gb, dbx, dcx, rate_grad = scan_backward(step_far, drive, skip_part, bx, cx, rate2, starts)
    a_log_grad = rate_grad * decay_rate
    step_grad = za * LN2 + gb * conv_act
    act_scan = gb * step_size
    b_grad = jnp.sum(dbx, axis=-1)
    c_grad = jnp.sum(dcx, axis=-1)
    pre_grad = step_grad * jax.nn.sigmoid(dt_pre)
    dt_bias_grad = jnp.sum(pre_grad, axis=0)
    pre_low = pre_grad.astype(low)
    dt_weight_grad = left_inner(dt_rounded, pre_low)
    rank_grad = right_inner(pre_low, dt_full)
    proj_grad = jnp.concatenate([rank_grad, b_grad, c_grad], axis=1).astype(low)
    xproj_grad = left_inner(proj_grad, act_low)
    act_grad = matmul(proj_grad, xproj_t) + skip_part * skip_value + act_scan
    conv_grad = act_grad * silu_slope(conv_out)
    conv_bias_grad = jnp.sum(conv_grad, axis=0)
    inner_grad = jnp.zeros_like(inner_in)
    tap_grads = []
    for offset in range(KCONV):
        lag_now = KCONV - 1 - offset
        masked = conv_grad * tap_valid[:, lag_now : lag_now + 1]
        tap_grads.append(jnp.sum(masked * padded[offset : offset + length], axis=0))
        inner_grad = (
            inner_grad + conv_taps[offset] * jnp.pad(masked, ((0, lag_now), (0, 0)))[lag_now:]
        )
    conv_weight_grad = jnp.stack(tap_grads)
    inner_low = inner_grad.astype(low)
    inner_in_grad = left_inner(normed_low, inner_low)
    normed_grad = right_inner(inner_low, in_full[:, :inner_width]) + right_inner(
        gate_low, in_full[:, inner_width:]
    )
    gain_grad = jnp.sum(normed_grad * unit_rows, axis=0)
    scaled = normed_grad * gain_value
    input_grad = cotangent.astype(jnp.float32) + inverse_rms * (
        scaled - unit_rows * jnp.mean(scaled * unit_rows, axis=-1, keepdims=True)
    )
    gain_rows = jnp.pad(gain_grad.reshape(shards, gain_shard), ((0, 0), (0, width - gain_shard)))
    small_grad = jnp.concatenate(
        [
            xproj_grad,
            dt_weight_grad,
            a_log_grad,
            conv_weight_grad,
            conv_bias_grad[None],
            dt_bias_grad[None],
            skip_grad[None],
            gain_rows.reshape(1, -1),
        ],
        axis=0,
    )
    dp = lax.axis_size("dp")
    unit = split_of(dp)[1]
    small_grad = jnp.pad(small_grad, ((0, -small_grad.shape[0] % unit), (0, 0)))
    small_rows = small_grad.shape[0]
    small_grad = jnp.moveaxis(small_grad.reshape(small_rows, shards, width), 1, 0)
    reduced = reduce_all(
        dp,
        [
            out_grad.astype(low).reshape(shards, -1, out_grad.shape[1]),
            gate_in_grad.astype(low).reshape(shards, -1, inner_width),
            inner_in_grad.astype(low).reshape(shards, -1, inner_width),
            small_grad.astype(low),
        ],
        collective_id=1,
    )
    out_share, gate_share, inner_share, small_share = (v.astype(jnp.float32) for v in reduced)
    at = xw + rank + state
    return (
        output,
        input_grad,
        small_share[at + KCONV + 3, :gain_shard],
        jnp.concatenate([inner_share, gate_share], axis=1),
        small_share[at : at + KCONV],
        small_share[at + KCONV],
        small_share[:xw].T,
        small_share[xw : xw + rank],
        small_share[at + KCONV + 1],
        small_share[xw + rank : at],
        small_share[at + KCONV + 2],
        out_share,
    )


def solution(mesh):
    in_specs = (
        P(("dp", "fsdp"), None),
        P(("dp", "fsdp"), None),
        P("fsdp"),
        P("fsdp", None),
        P(None, "fsdp"),
        P("fsdp"),
        P("fsdp", None),
        P(None, "fsdp"),
        P("fsdp"),
        P(None, "fsdp"),
        P("fsdp"),
        P("fsdp", None),
        P(("dp", "fsdp"), None),
    )
    out_specs = (
        P(("dp", "fsdp"), None),
        P(("dp", "fsdp"), None),
        P("fsdp"),
        P("fsdp", None),
        P(None, "fsdp"),
        P("fsdp"),
        P("fsdp", None),
        P(None, "fsdp"),
        P("fsdp"),
        P(None, "fsdp"),
        P("fsdp"),
        P("fsdp", None),
    )
    return jax.shard_map(body, mesh=mesh, in_specs=in_specs, out_specs=out_specs, check_vma=False)
```

```python
import functools

import jax
import jax.numpy as jnp
import numpy as np
from jax import lax
from jax.experimental import pallas as pl
from jax.experimental.pallas import tpu as pltpu
from jax.sharding import PartitionSpec as P

KCONV = 4
LENGTH = 512
LOG2E = float(np.log2(np.e))
LN2 = float(np.log(2.0))
FAR = 1e30


epsilon = 1e-05


def matmul(former, latter):
    return jnp.dot(former, latter, preferred_element_type=jnp.float32)


def left_inner(former, latter):
    return lax.dot_general(
        former, latter, (((0,), (0,)), ((), ())), preferred_element_type=jnp.float32
    )


def right_inner(former, latter):
    return lax.dot_general(
        former, latter, (((1,), (1,)), ((), ())), preferred_element_type=jnp.float32
    )


def silu_of(values):
    return values * jax.nn.sigmoid(values)


def silu_slope(values):
    logistic = jax.nn.sigmoid(values)
    return logistic * (1.0 + values * (1.0 - logistic))


def cluster_masks(lengths):
    cluster_ends = jnp.cumsum(lengths, axis=-1)
    starts = cluster_ends - lengths
    positions = jnp.arange(LENGTH, dtype=jnp.int32)
    before = starts[:, None, :] <= positions[None, :, None]
    segment_start = jnp.max(jnp.where(before, starts[:, None, :], 0), axis=-1)
    keep_mask = (positions[None, :] > segment_start).astype(jnp.float32)
    lag_index = jnp.arange(KCONV, dtype=jnp.int32)
    tap_valid = (
        positions[None, :, None] - lag_index[None, None, :] >= segment_start[:, :, None]
    ).astype(jnp.float32)
    return (tap_valid[0], keep_mask[0])

MESH = pl.DeviceIdType.MESH
COLS = 1024
ROWS = 32
SLACK = 3


class Reducer:

    def __init__(self, dp, sources, targets, scratch, slack=SLACK):
        self.slack = slack
        self.nz = dp // 2
        self.sources, self.targets = sources, targets
        (self.rc, self.ry, self.rx, self.rz, self.s_one, self.r_one, self.s_rs, self.r_rs, self.s_ag, self.r_ag) = scratch
        self.me_dp, self.me_f = lax.axis_index("dp"), lax.axis_index("fsdp")
        self.fh, self.fl = self.me_f // 2, self.me_f % 2
        self.z, self.x = self.me_dp // 2, self.me_dp % 2
        self.pieces_c, self.rows = split_of(dp)
        self.pieces_r = self.nz // self.pieces_c
        self.chunks = chunk_list([t.shape for t in targets], self.rows)
        self.core = (self.me_dp, self.fh * 2 + (1 - self.fl))
        self.other = (self.me_dp, (1 - self.fh) * 2 + self.fl)
        self.pair = (self.z * 2 + (1 - self.x), self.me_f)

    def peer(self, o):
        return lax.rem(self.z + o, self.nz)

    def entry(self):
        barrier = pltpu.get_barrier_semaphore()
        ids = [self.core, self.other, self.pair] + [(self.peer(o) * 2 + self.x, self.me_f) for o in range(1, self.nz)]
        for d in ids:
            pl.semaphore_signal(barrier, inc=1, device_id=d, device_id_type=MESH)
        pl.semaphore_wait(barrier, len(ids))

    def copy(self, src, dst, send, recv, device):
        return pltpu.make_async_remote_copy(src_ref=src, dst_ref=dst, send_sem=send, recv_sem=recv, device_id=device, device_id_type=MESH)

    def copies(self, stage, k):
        a, r0, c0, w = self.chunks[k]
        r, hr = self.rows, self.rows // 2
        if stage == 0:
            src = self.sources[a].at[:, 1 - self.fl, r0:r0 + r, c0:c0 + w]
            return [self.copy(src, self.rc.at[k, :, :, :w], self.s_one.at[0, k], self.r_one.at[0, k], self.core)]
        if stage == 1:
            return [self.copy(self.rc.at[k, 1 - self.fh, :, :w], self.ry.at[k, :, :w], self.s_one.at[1, k], self.r_one.at[1, k], self.other)]
        if stage == 2:
            src = self.ry.at[k, pl.ds(pl.multiple_of((1 - self.x) * hr, hr), hr), :w]
            return [self.copy(src, self.rx.at[k, :, :w], self.s_one.at[2, k], self.r_one.at[2, k], self.pair)]
        out = []
        if stage == 5:
            rows = pl.ds(pl.multiple_of(r0 + self.x * hr, hr), hr)
            t = self.targets[a].at[rows, c0:c0 + w]
            return [self.copy(t, t, self.s_one.at[3, k], self.r_one.at[3, k], self.pair)]
        for o in range(1, self.nz):
            j = self.peer(o)
            device = (j * 2 + self.x, self.me_f)
            if stage == 3:
                pr, pc = self.place(j, w)
                out.append(self.copy(self.rx.at[k, pr, pc], self.rz.at[k, o - 1, :, :w // self.pieces_c], self.s_rs.at[k, o - 1], self.r_rs.at[k, o - 1], device))
            else:
                t = self.own(k)
                out.append(self.copy(t, t, self.s_ag.at[k, o - 1], self.r_ag.at[k, o - 1], device))
        return out

    def place(self, j, w, r0=0, c0=0):
        pr, pw = self.rows // 2 // self.pieces_r, w // self.pieces_c
        return (pl.ds(pl.multiple_of(r0 + (j // self.pieces_c) * pr, 16), pr), pl.ds(pl.multiple_of(c0 + lax.rem(j, self.pieces_c) * pw, 128), pw))

    def own(self, k):
        a, r0, c0, w = self.chunks[k]
        pr, pc = self.place(self.z, w, r0 + self.x * (self.rows // 2), c0)
        return self.targets[a].at[pr, pc]

    def absorb(self, stage, k):
        a, r0, c0, w = self.chunks[k]
        r, hr = self.rows, self.rows // 2
        for c in self.copies(stage, k):
            c.wait_recv()
        if stage == 0:
            for h in range(2):
                self.rc[k, h, :, :w] = self.rc[k, h, :, :w] + self.sources[a][h, self.fl, r0:r0 + r, c0:c0 + w]
        elif stage == 1:
            self.ry[k, :, :w] = self.ry[k, :, :w] + self.rc[k, self.fh, :, :w]
        elif stage == 2:
            mine = self.ry[k, pl.ds(pl.multiple_of(self.x * hr, hr), hr), :w]
            self.rx[k, :, :w] = self.rx[k, :, :w] + mine
        elif stage == 3:
            pr, pc = self.place(self.z, w)
            total = self.rx[k, pr, pc].astype(jnp.float32)
            for o in range(1, self.nz):
                total = total + self.rz[k, o - 1, :, :w // self.pieces_c].astype(jnp.float32)
            self.own(k)[...] = total.astype(jnp.bfloat16)

    def ticks(self):
        return len(self.chunks) + 6 * self.slack

    def tick(self, n):
        live = [(s, n - self.slack * s) for s in range(7) if 0 <= n - self.slack * s < len(self.chunks)]
        for s, k in reversed(live):
            if s > 0:
                self.absorb(s - 1, k)
        for s, k in reversed(live):
            if s < 6:
                for c in self.copies(s, k):
                    c.start()

    def finish(self):
        for k in range(len(self.chunks)):
            for s in range(6):
                for c in self.copies(s, k):
                    c.wait_send()


def split_of(dp):
    nz = dp // 2
    pieces_c = min(nz, COLS // 128, 4)
    return pieces_c, max(ROWS, 32 * (nz // pieces_c))


def chunk_list(shapes, rows):
    out = []
    for a, (r, c) in enumerate(shapes):
        w = min(c, COLS)
        for r0 in range(0, r, rows):
            for c0 in range(0, c, w):
                out.append((a, r0, c0, w))
    return out


def reducer_scratch(dp, shapes):
    nz = dp // 2
    pieces_c, rows = split_of(dp)
    n = len(chunk_list(shapes, rows))
    low = jnp.bfloat16
    return [
        pltpu.VMEM((n, 2, rows, COLS), low),
        pltpu.VMEM((n, rows, COLS), low),
        pltpu.VMEM((n, rows // 2, COLS), low),
        pltpu.VMEM((n, nz - 1, rows // 2 // (nz // pieces_c), COLS // pieces_c), low),
        pltpu.SemaphoreType.DMA((4, n)),
        pltpu.SemaphoreType.DMA((4, n)),
        pltpu.SemaphoreType.DMA((n, nz - 1)),
        pltpu.SemaphoreType.DMA((n, nz - 1)),
        pltpu.SemaphoreType.DMA((n, nz - 1)),
        pltpu.SemaphoreType.DMA((n, nz - 1)),
    ]


def reduce_all(dp, arrays, collective_id):
    shapes = [a.shape[1:] for a in arrays]
    na = len(arrays)
    scratch = reducer_scratch(dp, shapes)

    def kernel(*refs):
        red = Reducer(dp, refs[:na], refs[na:2 * na], refs[2 * na:])
        red.entry()
        for n in range(red.ticks()):
            red.tick(n)
        red.finish()

    return pl.pallas_call(
        kernel,
        out_shape=[jax.ShapeDtypeStruct(s, jnp.bfloat16) for s in shapes],
        in_specs=[pl.BlockSpec(memory_space=pltpu.VMEM)] * na,
        out_specs=[pl.BlockSpec(memory_space=pltpu.VMEM)] * na,
        scratch_shapes=scratch,
        compiler_params=pltpu.CompilerParams(collective_id=collective_id, has_side_effects=True, vmem_limit_bytes=60 << 20),
        name="reduce_all",
    )(*[a.reshape((2, 2) + a.shape[1:]) for a in arrays])


LANE = 128
NS = 16
TC = 32
CGF = 1024
CGB = 512


def bcast(ref, i, row):
    v = ref[i, pl.ds(row, 8, stride=0), :]
    return jnp.concatenate([v, v], axis=0)


def stage(src, dst):
    for i in range(dst.shape[0]):
        dst[i] = src[:, i * LANE:(i + 1) * LANE]


def fold(src, i):
    s = [src[i, pl.ds(q, 8, stride=8), :] for q in range(8)]
    return ((s[0] + s[1]) + (s[2] + s[3])) + ((s[4] + s[5]) + (s[6] + s[7]))


def fwd_kernel(dt_ref, dr_ref, b_ref, c_ref, a_ref, y_ref, hs_ref, part, dts, drs, hst):
    cg = dt_ref.shape[1]
    tiles = cg // LANE
    tc = dt_ref.shape[0]

    @pl.when(pl.program_id(1) == 0)
    def _():
        hst[...] = jnp.zeros_like(hst)

    hs_ref[0] = hst[...]
    stage(dt_ref, dts)
    stage(dr_ref, drs)

    def group(g, carry):
        t0 = pl.multiple_of(g * 8, 8)
        hs = list(carry)
        for k in range(8):
            bt = b_ref[t0 + k]
            ct = c_ref[t0 + k]
            for i in range(tiles):
                ln = slice(i * LANE, (i + 1) * LANE)
                d = bcast(dts, i, t0 + k)
                u = bcast(drs, i, t0 + k)
                a = jnp.exp2(d * a_ref[:, ln])
                h = a * hs[i] + bt * u
                hs[i] = h
                p = ct * h
                part[i, k * 8:(k + 1) * 8, :] = p[:8] + p[8:]
        for i in range(tiles):
            ln = slice(i * LANE, (i + 1) * LANE)
            y_ref[pl.ds(t0, 8), ln] = fold(part, i)
        return tuple(hs)

    init = tuple(hst[:, i * LANE:(i + 1) * LANE] for i in range(tiles))
    out = lax.fori_loop(0, tc // 8, group, init)
    for i in range(tiles):
        hst[:, i * LANE:(i + 1) * LANE] = out[i]


def scan_forward(dt, dr, bx, cx, a2, tc=TC, cg=CGF):
    t, c = dt.shape
    nt, nc = t // tc, c // cg
    return pl.pallas_call(
        fwd_kernel,
        grid=(nc, nt),
        in_specs=[
            pl.BlockSpec((tc, cg), lambda j, i: (i, j)),
            pl.BlockSpec((tc, cg), lambda j, i: (i, j)),
            pl.BlockSpec((tc, NS, LANE), lambda j, i: (i, 0, 0)),
            pl.BlockSpec((tc, NS, LANE), lambda j, i: (i, 0, 0)),
            pl.BlockSpec((NS, cg), lambda j, i: (0, j)),
        ],
        out_specs=[
            pl.BlockSpec((tc, cg), lambda j, i: (i, j)),
            pl.BlockSpec((1, NS, cg), lambda j, i: (i, 0, j)),
        ],
        out_shape=[
            jax.ShapeDtypeStruct((t, c), jnp.float32),
            jax.ShapeDtypeStruct((nt, NS, c), jnp.float32),
        ],
        scratch_shapes=[pltpu.VMEM((cg // LANE, 64, LANE), jnp.float32)] + [pltpu.VMEM((cg // LANE, tc, LANE), jnp.float32)] * 2 + [pltpu.VMEM((NS, cg), jnp.float32)],
        name="scan_forward",
    )(dt, dr, bx, cx, a2)


def bwd_kernel(dp, dt_ref, dr_ref, dy_ref, b_ref, c_ref, a_ref, hs_ref, og_ref, gg_ref,
               za_ref, gb_ref, db_ref, dc_ref, rate_ref, os_ref, gs_ref,
               asc, hsc, pz, pg, dts, drs, dys, gst, rst, ores, gres, *comm):
    red = Reducer(dp, (og_ref, gg_ref), (ores, gres), comm)
    step = pl.program_id(0) * pl.num_programs(1) + pl.program_id(1)
    for n in range(red.ticks()):
        @pl.when(step == n)
        def _(n=n):
            if n == 0:
                red.entry()
            red.tick(n)

    @pl.when(step == pl.num_programs(0) * pl.num_programs(1) - 1)
    def _():
        red.finish()
        os_ref[...] = ores[...]
        gs_ref[...] = gres[...]

    cg = dt_ref.shape[1]
    tiles = cg // LANE
    tc = dt_ref.shape[0]
    j = pl.program_id(0)
    i_t = pl.program_id(1)
    nt = pl.num_programs(1)

    @pl.when(i_t == 0)
    def _():
        gst[...] = jnp.zeros_like(gst)
        rst[...] = jnp.zeros_like(rst)

    stage(dt_ref, dts)
    stage(dr_ref, drs)
    stage(dy_ref, dys)
    lanes = [slice(i * LANE, (i + 1) * LANE) for i in range(tiles)]

    def fgroup(g, carry):
        t0 = pl.multiple_of(g * 8, 8)
        hs = list(carry)
        for k in range(8):
            bt = b_ref[t0 + k]
            for i in range(tiles):
                ln = lanes[i]
                d = bcast(dts, i, t0 + k)
                u = bcast(drs, i, t0 + k)
                a = jnp.exp2(d * a_ref[:, ln])
                asc[t0 + k, :, ln] = a
                hsc[t0 + k, :, ln] = hs[i]
                hs[i] = a * hs[i] + bt * u
        return tuple(hs)

    out = lax.fori_loop(0, tc // 8, fgroup, tuple(hs_ref[0, :, ln] for ln in lanes))
    for i in range(tiles):
        hsc[tc, :, lanes[i]] = out[i]

    base = pl.multiple_of((nt - 1 - i_t) * tc, tc)
    first = j == 0

    def bgroup(gi, carry):
        g = tc // 8 - 1 - gi
        t0 = pl.multiple_of(g * 8, 8)
        gs = list(carry[0])
        rs = list(carry[1])
        for k in range(7, -1, -1):
            bt = b_ref[t0 + k]
            ct = c_ref[t0 + k]
            accb = None
            for i in range(tiles):
                ln = lanes[i]
                d = bcast(dts, i, t0 + k)
                u = bcast(drs, i, t0 + k)
                w = bcast(dys, i, t0 + k)
                hnow = hsc[t0 + k + 1, :, ln]
                hprev = hsc[t0 + k, :, ln]
                a = asc[t0 + k, :, ln]
                gg = ct * w + gs[i]
                ga = gg * a
                z = ga * hprev
                rs[i] = rs[i] + z * d
                gs[i] = ga
                pa = z * a_ref[:, ln]
                pz[i, k * 8:(k + 1) * 8, :] = pa[:8] + pa[8:]
                pb = gg * bt
                pg[i, k * 8:(k + 1) * 8, :] = pb[:8] + pb[8:]
                vb = gg * u
                vc = w * hnow
                accb = vb if accb is None else accb + vb
                accc = vc if i == 0 else accc + vc
            row = base + t0 + k

            @pl.when(first)
            def _():
                db_ref[row] = accb
                dc_ref[row] = accc

            @pl.when(jnp.logical_not(first))
            def _():
                db_ref[row] = db_ref[row] + accb
                dc_ref[row] = dc_ref[row] + accc
        for i in range(tiles):
            ln = lanes[i]
            za_ref[pl.ds(t0, 8), ln] = fold(pz, i)
            gb_ref[pl.ds(t0, 8), ln] = fold(pg, i)
        return tuple(gs), tuple(rs)

    gs, rs = lax.fori_loop(0, tc // 8, bgroup, (tuple(gst[:, ln] for ln in lanes), tuple(rst[:, ln] for ln in lanes)))
    for i in range(tiles):
        gst[:, lanes[i]] = gs[i]
        rst[:, lanes[i]] = rs[i]

    @pl.when(i_t == nt - 1)
    def _():
        rate_ref[...] = rst[...]


def scan_backward(dp, dt, dr, dy, bx, cx, a2, hs, og, gg, tc=TC, cg=CGB):
    t, c = dt.shape
    nt, nc = t // tc, c // cg
    row = pl.BlockSpec((tc, cg), lambda j, i: (nt - 1 - i, j))
    bc = pl.BlockSpec((tc, NS, LANE), lambda j, i: (nt - 1 - i, 0, 0))
    full = pl.BlockSpec((t, NS, LANE), lambda j, i: (0, 0, 0), pipeline_mode=pl.Buffered(1))
    once = lambda s: pl.BlockSpec(s, lambda j, i: (0,) * len(s), pipeline_mode=pl.Buffered(1))
    og = og.reshape((2, 2) + og.shape[1:])
    gg = gg.reshape((2, 2) + gg.shape[1:])
    parts = [og.shape[2:], gg.shape[2:]]
    return pl.pallas_call(
        functools.partial(bwd_kernel, dp),
        grid=(nc, nt),
        in_specs=[row, row, row, bc, bc, pl.BlockSpec((NS, cg), lambda j, i: (0, j)),
                  pl.BlockSpec((1, NS, cg), lambda j, i: (nt - 1 - i, 0, j)), once(og.shape), once(gg.shape)],
        out_specs=[row, row, full, full, pl.BlockSpec((NS, cg), lambda j, i: (0, j)), once(parts[0]), once(parts[1])],
        out_shape=[
            jax.ShapeDtypeStruct((t, c), jnp.float32),
            jax.ShapeDtypeStruct((t, c), jnp.float32),
            jax.ShapeDtypeStruct((t, NS, LANE), jnp.float32),
            jax.ShapeDtypeStruct((t, NS, LANE), jnp.float32),
            jax.ShapeDtypeStruct((NS, c), jnp.float32),
            jax.ShapeDtypeStruct(parts[0], jnp.bfloat16),
            jax.ShapeDtypeStruct(parts[1], jnp.bfloat16),
        ],
        scratch_shapes=[
            pltpu.VMEM((tc, NS, cg), jnp.float32), pltpu.VMEM((tc + 1, NS, cg), jnp.float32),
            pltpu.VMEM((cg // LANE, 64, LANE), jnp.float32), pltpu.VMEM((cg // LANE, 64, LANE), jnp.float32),
            pltpu.VMEM((cg // LANE, tc, LANE), jnp.float32), pltpu.VMEM((cg // LANE, tc, LANE), jnp.float32), pltpu.VMEM((cg // LANE, tc, LANE), jnp.float32),
            pltpu.VMEM((NS, cg), jnp.float32), pltpu.VMEM((NS, cg), jnp.float32),
            pltpu.VMEM(parts[0], jnp.bfloat16), pltpu.VMEM(parts[1], jnp.bfloat16),
        ] + reducer_scratch(dp, parts),
        compiler_params=pltpu.CompilerParams(vmem_limit_bytes=60 << 20, collective_id=2, has_side_effects=True),
        name="scan_backward",
    )(dt, dr, dy, bx, cx, a2, hs, og, gg)


def pack_small(gain, conv_w, conv_b, xproj, dt_w, dt_b, alog, skip):
    width = conv_b.shape[-1]
    gain_row = jnp.pad(gain[None], ((0, 0), (0, width - gain.shape[0])))
    return jnp.concatenate(
        [xproj.T, dt_w, alog, conv_w, conv_b[None], dt_b[None], skip[None], gain_row], axis=0
    )


def body(
    tokens,
    cluster_lengths,
    norm_gain,
    in_weight,
    conv_weight,
    conv_bias,
    xproj_weight,
    dt_weight,
    dt_bias,
    a_log,
    skip_gain,
    out_weight,
    cotangent,
):
    low = jnp.bfloat16
    gain_shard = norm_gain.shape[0]
    width = conv_bias.shape[0]
    packed = pack_small(norm_gain, conv_weight, conv_bias, xproj_weight, dt_weight, dt_bias, a_log, skip_gain)
    in_full = lax.all_gather(in_weight, "fsdp", axis=0, tiled=True)
    small = lax.all_gather(packed, "fsdp", axis=0)
    out_full = lax.all_gather(out_weight, "fsdp", axis=0, tiled=True)
    shards = small.shape[0]
    xw, rank, state = xproj_weight.shape[1], dt_weight.shape[0], a_log.shape[0]
    rows = jnp.moveaxis(small, 0, 1).reshape(small.shape[1], shards * width)
    xproj_t = rows[:xw]
    dt_full = rows[xw : xw + rank]
    at = xw + rank
    alog_full = rows[at : at + state]
    at += state
    conv_taps = rows[at : at + KCONV].astype(jnp.float32)
    at += KCONV
    conv_offset = rows[at].astype(jnp.float32)
    dt_offset = rows[at + 1].astype(jnp.float32)
    skip_value = rows[at + 2].astype(jnp.float32)
    gain_value = small[:, at + 3, :gain_shard].reshape(-1).astype(jnp.float32)
    decay_rate = -jnp.exp(alog_full.astype(jnp.float32))
    inner_width = shards * width
    length = tokens.shape[0]
    tap_valid, keep_mask = cluster_masks(cluster_lengths)
    inputs_full = tokens.astype(jnp.float32)
    mean_square = jnp.mean(inputs_full * inputs_full, axis=-1, keepdims=True)
    inverse_rms = lax.rsqrt(mean_square + epsilon)
    unit_rows = inputs_full * inverse_rms
    normed_low = (unit_rows * gain_value).astype(low)
    mixed_in = matmul(normed_low, in_full)
    inner_in = mixed_in[:, :inner_width]
    gate_in = mixed_in[:, inner_width:]
    padded = jnp.pad(inner_in, ((KCONV - 1, 0), (0, 0)))
    conv_out = jnp.zeros_like(inner_in) + conv_offset
    for offset in range(KCONV):
        lag_now = KCONV - 1 - offset
        conv_out = (
            conv_out
            + conv_taps[offset]
            * padded[offset : offset + length]
            * tap_valid[:, lag_now : lag_now + 1]
        )
    conv_act = silu_of(conv_out)
    act_low = conv_act.astype(low)
    projected = right_inner(act_low, xproj_t)
    dt_rounded = projected[:, :rank].astype(low)
    b_mat = projected[:, rank : rank + state]
    c_mat = projected[:, rank + state :]
    dt_pre = matmul(dt_rounded, dt_full) + dt_offset
    step_size = jax.nn.softplus(dt_pre)
    drive = step_size * conv_act
    step_far = jnp.where(keep_mask[:, None] > 0, step_size, FAR)
    rate2 = decay_rate * LOG2E
    bx = jnp.broadcast_to(b_mat[:, :, None], (length, state, LANE))
    cx = jnp.broadcast_to(c_mat[:, :, None], (length, state, LANE))
    scanned, starts = scan_forward(step_far, drive, bx, cx, rate2)
    with_skip = scanned + skip_value * conv_act
    gate_act = silu_of(gate_in)
    gated_low = (with_skip * gate_act).astype(low)
    result = inputs_full + matmul(gated_low, out_full)
    output = result.astype(low)
    out_grad = left_inner(gated_low, cotangent)
    gated_grad = right_inner(cotangent, out_full)
    skip_part = gated_grad * gate_act
    gate_grad = gated_grad * with_skip * silu_slope(gate_in)
    gate_low = gate_grad.astype(low)
    gate_in_grad = left_inner(normed_low, gate_low)
    skip_grad = jnp.sum(skip_part * conv_act, axis=0)
    dp = lax.axis_size("dp")
    za, gb, dbx, dcx, rate_grad, out_share, gate_share = scan_backward(
        dp,
        step_far,
        drive,
        skip_part,
        bx,
        cx,
        rate2,
        starts,
        out_grad.astype(low).reshape(shards, -1, out_grad.shape[1]),
        gate_in_grad.astype(low).reshape(shards, -1, inner_width),
    )
    a_log_grad = rate_grad * decay_rate
    step_grad = za * LN2 + gb * conv_act
    act_scan = gb * step_size
    b_grad = jnp.sum(dbx, axis=-1)
    c_grad = jnp.sum(dcx, axis=-1)
    pre_grad = step_grad * jax.nn.sigmoid(dt_pre)
    dt_bias_grad = jnp.sum(pre_grad, axis=0)
    pre_low = pre_grad.astype(low)
    dt_weight_grad = left_inner(dt_rounded, pre_low)
    rank_grad = right_inner(pre_low, dt_full)
    proj_grad = jnp.concatenate([rank_grad, b_grad, c_grad], axis=1).astype(low)
    xproj_grad = left_inner(proj_grad, act_low)
    act_grad = matmul(proj_grad, xproj_t) + skip_part * skip_value + act_scan
    conv_grad = act_grad * silu_slope(conv_out)
    conv_bias_grad = jnp.sum(conv_grad, axis=0)
    inner_grad = jnp.zeros_like(inner_in)
    tap_grads = []
    for offset in range(KCONV):
        lag_now = KCONV - 1 - offset
        masked = conv_grad * tap_valid[:, lag_now : lag_now + 1]
        tap_grads.append(jnp.sum(masked * padded[offset : offset + length], axis=0))
        inner_grad = (
            inner_grad + conv_taps[offset] * jnp.pad(masked, ((0, lag_now), (0, 0)))[lag_now:]
        )
    conv_weight_grad = jnp.stack(tap_grads)
    inner_low = inner_grad.astype(low)
    inner_in_grad = left_inner(normed_low, inner_low)
    normed_grad = right_inner(inner_low, in_full[:, :inner_width]) + right_inner(
        gate_low, in_full[:, inner_width:]
    )
    gain_grad = jnp.sum(normed_grad * unit_rows, axis=0)
    scaled = normed_grad * gain_value
    input_grad = cotangent.astype(jnp.float32) + inverse_rms * (
        scaled - unit_rows * jnp.mean(scaled * unit_rows, axis=-1, keepdims=True)
    )
    gain_rows = jnp.pad(gain_grad.reshape(shards, gain_shard), ((0, 0), (0, width - gain_shard)))
    small_grad = jnp.concatenate(
        [
            xproj_grad,
            dt_weight_grad,
            a_log_grad,
            conv_weight_grad,
            conv_bias_grad[None],
            dt_bias_grad[None],
            skip_grad[None],
            gain_rows.reshape(1, -1),
        ],
        axis=0,
    )
    unit = split_of(dp)[1]
    small_grad = jnp.pad(small_grad, ((0, -small_grad.shape[0] % unit), (0, 0)))
    small_rows = small_grad.shape[0]
    small_grad = jnp.moveaxis(small_grad.reshape(small_rows, shards, width), 1, 0)
    reduced = reduce_all(
        dp,
        [
            inner_in_grad.astype(low).reshape(shards, -1, inner_width),
            small_grad.astype(low),
        ],
        collective_id=1,
    )
    inner_share, small_share = (v.astype(jnp.float32) for v in reduced)
    out_share, gate_share = out_share.astype(jnp.float32), gate_share.astype(jnp.float32)
    at = xw + rank + state
    return (
        output,
        input_grad,
        small_share[at + KCONV + 3, :gain_shard],
        jnp.concatenate([inner_share, gate_share], axis=1),
        small_share[at : at + KCONV],
        small_share[at + KCONV],
        small_share[:xw].T,
        small_share[xw : xw + rank],
        small_share[at + KCONV + 1],
        small_share[xw + rank : at],
        small_share[at + KCONV + 2],
        out_share,
    )


def solution(mesh):
    in_specs = (
        P(("dp", "fsdp"), None),
        P(("dp", "fsdp"), None),
        P("fsdp"),
        P("fsdp", None),
        P(None, "fsdp"),
        P("fsdp"),
        P("fsdp", None),
        P(None, "fsdp"),
        P("fsdp"),
        P(None, "fsdp"),
        P("fsdp"),
        P("fsdp", None),
        P(("dp", "fsdp"), None),
    )
    out_specs = (
        P(("dp", "fsdp"), None),
        P(("dp", "fsdp"), None),
        P("fsdp"),
        P("fsdp", None),
        P(None, "fsdp"),
        P("fsdp"),
        P("fsdp", None),
        P(None, "fsdp"),
        P("fsdp"),
        P(None, "fsdp"),
        P("fsdp"),
        P("fsdp", None),
    )
    return jax.shard_map(body, mesh=mesh, in_specs=in_specs, out_specs=out_specs, check_vma=False)
```

```python
import functools

import jax
import jax.numpy as jnp
import numpy as np
from jax import lax
from jax.experimental import pallas as pl
from jax.experimental.pallas import tpu as pltpu
from jax.sharding import PartitionSpec as P

KCONV = 4
LENGTH = 512
LOG2E = float(np.log2(np.e))
LN2 = float(np.log(2.0))
FAR = 1e30


epsilon = 1e-05


def matmul(former, latter):
    return jnp.dot(former, latter, preferred_element_type=jnp.float32)


def left_inner(former, latter):
    return lax.dot_general(
        former, latter, (((0,), (0,)), ((), ())), preferred_element_type=jnp.float32
    )


def right_inner(former, latter):
    return lax.dot_general(
        former, latter, (((1,), (1,)), ((), ())), preferred_element_type=jnp.float32
    )


def silu_of(values):
    return values * jax.nn.sigmoid(values)


def silu_slope(values):
    logistic = jax.nn.sigmoid(values)
    return logistic * (1.0 + values * (1.0 - logistic))


def cluster_masks(lengths):
    cluster_ends = jnp.cumsum(lengths, axis=-1)
    starts = cluster_ends - lengths
    positions = jnp.arange(LENGTH, dtype=jnp.int32)
    before = starts[:, None, :] <= positions[None, :, None]
    segment_start = jnp.max(jnp.where(before, starts[:, None, :], 0), axis=-1)
    keep_mask = (positions[None, :] > segment_start).astype(jnp.float32)
    lag_index = jnp.arange(KCONV, dtype=jnp.int32)
    tap_valid = (
        positions[None, :, None] - lag_index[None, None, :] >= segment_start[:, :, None]
    ).astype(jnp.float32)
    return (tap_valid[0], keep_mask[0])

MESH = pl.DeviceIdType.MESH
COLS = 1024
ROWS = 32
SLACK = 3
ROWS_B = 64
SLACK_B = 2


class Reducer:

    def __init__(self, dp, sources, targets, scratch, rows=ROWS, slack=SLACK):
        self.slack = slack
        self.nz = dp // 2
        self.sources, self.targets = sources, targets
        (self.rc, self.ry, self.rx, self.rz, self.s_one, self.r_one, self.s_rs, self.r_rs, self.s_ag, self.r_ag) = scratch
        self.me_dp, self.me_f = lax.axis_index("dp"), lax.axis_index("fsdp")
        self.fh, self.fl = self.me_f // 2, self.me_f % 2
        self.z, self.x = self.me_dp // 2, self.me_dp % 2
        self.pieces_c, self.rows = split_of(dp, rows)
        self.pieces_r = self.nz // self.pieces_c
        self.chunks = chunk_list([t.shape for t in targets], self.rows)
        self.core = (self.me_dp, self.fh * 2 + (1 - self.fl))
        self.other = (self.me_dp, (1 - self.fh) * 2 + self.fl)
        self.pair = (self.z * 2 + (1 - self.x), self.me_f)

    def peer(self, o):
        return lax.rem(self.z + o, self.nz)

    def entry(self):
        barrier = pltpu.get_barrier_semaphore()
        ids = [self.core, self.other, self.pair] + [(self.peer(o) * 2 + self.x, self.me_f) for o in range(1, self.nz)]
        for d in ids:
            pl.semaphore_signal(barrier, inc=1, device_id=d, device_id_type=MESH)
        pl.semaphore_wait(barrier, len(ids))

    def copy(self, src, dst, send, recv, device):
        return pltpu.make_async_remote_copy(src_ref=src, dst_ref=dst, send_sem=send, recv_sem=recv, device_id=device, device_id_type=MESH)

    def copies(self, stage, k):
        a, r0, c0, w = self.chunks[k]
        r, hr = self.rows, self.rows // 2
        if stage == 0:
            src = self.sources[a].at[:, 1 - self.fl, r0:r0 + r, c0:c0 + w]
            return [self.copy(src, self.rc.at[k, :, :, :w], self.s_one.at[0, k], self.r_one.at[0, k], self.core)]
        if stage == 1:
            return [self.copy(self.rc.at[k, 1 - self.fh, :, :w], self.ry.at[k, :, :w], self.s_one.at[1, k], self.r_one.at[1, k], self.other)]
        if stage == 2:
            src = self.ry.at[k, pl.ds(pl.multiple_of((1 - self.x) * hr, hr), hr), :w]
            return [self.copy(src, self.rx.at[k, :, :w], self.s_one.at[2, k], self.r_one.at[2, k], self.pair)]
        out = []
        if stage == 5:
            rows = pl.ds(pl.multiple_of(r0 + self.x * hr, hr), hr)
            t = self.targets[a].at[rows, c0:c0 + w]
            return [self.copy(t, t, self.s_one.at[3, k], self.r_one.at[3, k], self.pair)]
        for o in range(1, self.nz):
            j = self.peer(o)
            device = (j * 2 + self.x, self.me_f)
            if stage == 3:
                pr, pc = self.place(j, w)
                out.append(self.copy(self.rx.at[k, pr, pc], self.rz.at[k, o - 1, :, :w // self.pieces_c], self.s_rs.at[k, o - 1], self.r_rs.at[k, o - 1], device))
            else:
                t = self.own(k)
                out.append(self.copy(t, t, self.s_ag.at[k, o - 1], self.r_ag.at[k, o - 1], device))
        return out

    def place(self, j, w, r0=0, c0=0):
        pr, pw = self.rows // 2 // self.pieces_r, w // self.pieces_c
        return (pl.ds(pl.multiple_of(r0 + (j // self.pieces_c) * pr, 16), pr), pl.ds(pl.multiple_of(c0 + lax.rem(j, self.pieces_c) * pw, 128), pw))

    def own(self, k):
        a, r0, c0, w = self.chunks[k]
        pr, pc = self.place(self.z, w, r0 + self.x * (self.rows // 2), c0)
        return self.targets[a].at[pr, pc]

    def absorb(self, stage, k):
        a, r0, c0, w = self.chunks[k]
        r, hr = self.rows, self.rows // 2
        for c in self.copies(stage, k):
            c.wait_recv()
        if stage == 0:
            for h in range(2):
                self.rc[k, h, :, :w] = self.rc[k, h, :, :w] + self.sources[a][h, self.fl, r0:r0 + r, c0:c0 + w]
        elif stage == 1:
            self.ry[k, :, :w] = self.ry[k, :, :w] + self.rc[k, self.fh, :, :w]
        elif stage == 2:
            mine = self.ry[k, pl.ds(pl.multiple_of(self.x * hr, hr), hr), :w]
            self.rx[k, :, :w] = self.rx[k, :, :w] + mine
        elif stage == 3:
            pr, pc = self.place(self.z, w)
            total = self.rx[k, pr, pc].astype(jnp.float32)
            for o in range(1, self.nz):
                total = total + self.rz[k, o - 1, :, :w // self.pieces_c].astype(jnp.float32)
            self.own(k)[...] = total.astype(jnp.bfloat16)

    def ticks(self):
        return len(self.chunks) + 6 * self.slack

    def tick(self, n):
        live = [(s, n - self.slack * s) for s in range(7) if 0 <= n - self.slack * s < len(self.chunks)]
        for s, k in reversed(live):
            if s > 0:
                self.absorb(s - 1, k)
        for s, k in reversed(live):
            if s < 6:
                for c in self.copies(s, k):
                    c.start()

    def finish(self):
        for k in range(len(self.chunks)):
            for s in range(6):
                for c in self.copies(s, k):
                    c.wait_send()


def split_of(dp, rows=ROWS):
    nz = dp // 2
    pieces_c = min(nz, COLS // 128, 4)
    return pieces_c, max(rows, 32 * (nz // pieces_c))


def chunk_list(shapes, rows):
    out = []
    for a, (r, c) in enumerate(shapes):
        w = min(c, COLS)
        for r0 in range(0, r, rows):
            for c0 in range(0, c, w):
                out.append((a, r0, c0, w))
    return out


def reducer_scratch(dp, shapes, rows=ROWS):
    nz = dp // 2
    pieces_c, rows = split_of(dp, rows)
    n = len(chunk_list(shapes, rows))
    low = jnp.bfloat16
    return [
        pltpu.VMEM((n, 2, rows, COLS), low),
        pltpu.VMEM((n, rows, COLS), low),
        pltpu.VMEM((n, rows // 2, COLS), low),
        pltpu.VMEM((n, nz - 1, rows // 2 // (nz // pieces_c), COLS // pieces_c), low),
        pltpu.SemaphoreType.DMA((4, n)),
        pltpu.SemaphoreType.DMA((4, n)),
        pltpu.SemaphoreType.DMA((n, nz - 1)),
        pltpu.SemaphoreType.DMA((n, nz - 1)),
        pltpu.SemaphoreType.DMA((n, nz - 1)),
        pltpu.SemaphoreType.DMA((n, nz - 1)),
    ]


def reduce_all(dp, arrays, collective_id):
    shapes = [a.shape[1:] for a in arrays]
    na = len(arrays)
    scratch = reducer_scratch(dp, shapes)

    def kernel(*refs):
        red = Reducer(dp, refs[:na], refs[na:2 * na], refs[2 * na:])
        red.entry()
        for n in range(red.ticks()):
            red.tick(n)
        red.finish()

    return pl.pallas_call(
        kernel,
        out_shape=[jax.ShapeDtypeStruct(s, jnp.bfloat16) for s in shapes],
        in_specs=[pl.BlockSpec(memory_space=pltpu.VMEM)] * na,
        out_specs=[pl.BlockSpec(memory_space=pltpu.VMEM)] * na,
        scratch_shapes=scratch,
        compiler_params=pltpu.CompilerParams(collective_id=collective_id, has_side_effects=True, vmem_limit_bytes=60 << 20),
        name="reduce_all",
    )(*[a.reshape((2, 2) + a.shape[1:]) for a in arrays])


PARTS = 4


class Spread:

    def __init__(self, shard, full, s_one, r_one, s_part, r_part, parts):
        dp, f = lax.axis_index("dp"), lax.axis_index("fsdp")
        fh, fl = f // 2, f % 2
        self.f, self.x = f, dp % 2
        self.far = (1 - fh) * 2 + fl
        self.core = (dp, fh * 2 + (1 - fl))
        self.other = (dp, self.far)
        self.pair = ((dp // 2) * 2 + (1 - self.x), f)
        self.shard, self.full, self.parts = shard, full, parts
        self.s_one, self.r_one, self.s_part, self.r_part = s_one, r_one, s_part, r_part
        self.half = shard.shape[0] // 2
        self.rows = self.half // parts

    def span(self, half, i):
        return pl.ds(pl.multiple_of(half * self.half + i * self.rows, self.rows), self.rows)

    def send(self, src, dst, s, r, device):
        return pltpu.make_async_remote_copy(src_ref=src, dst_ref=dst, send_sem=s, recv_sem=r, device_id=device, device_id_type=pl.DeviceIdType.MESH)

    def whole(self):
        return self.send(self.shard, self.full.at[self.f], self.s_one, self.r_one, self.core)

    def across(self, i):
        rows = self.span(self.x, i)
        return self.send(self.shard.at[rows], self.full.at[self.f, rows], self.s_part.at[0, i], self.r_part.at[0, i], self.other)

    def onward(self, kind, i):
        rows = self.span(self.x if kind < 3 else 1 - self.x, i)
        ref = self.full.at[self.far, rows]
        return self.send(ref, ref, self.s_part.at[kind, i], self.r_part.at[kind, i], self.pair if kind == 1 else self.core)

    def begin(self):
        self.whole().start()
        for i in range(self.parts):
            self.across(i).start()

    def pump(self, i):
        self.across(i).wait_recv()
        self.onward(1, i).start()
        self.onward(2, i).start()

    def pump_pair(self, i):
        self.onward(1, i).wait_recv()
        self.onward(3, i).start()

    def land(self):
        for i in range(self.parts):
            self.onward(2, i).wait_recv()
            self.onward(3, i).wait_recv()

    def finish(self):
        self.whole().wait_send()
        for i in range(self.parts):
            self.across(i).wait_send()
            for kind in (1, 2, 3):
                self.onward(kind, i).wait_send()


def spread_sems(parts):
    return [pltpu.SemaphoreType.DMA, pltpu.SemaphoreType.DMA, pltpu.SemaphoreType.DMA((4, parts)), pltpu.SemaphoreType.DMA((4, parts))]


def enter_square():
    dp, f = lax.axis_index("dp"), lax.axis_index("fsdp")
    fh, fl = f // 2, f % 2
    barrier = pltpu.get_barrier_semaphore()
    for d in ((dp, fh * 2 + (1 - fl)), (dp, (1 - fh) * 2 + fl), ((dp // 2) * 2 + (1 - dp % 2), f)):
        pl.semaphore_signal(barrier, inc=1, device_id=d, device_id_type=pl.DeviceIdType.MESH)
    pl.semaphore_wait(barrier, 3)


def nt(a, b):
    return lax.dot_general(a, b, (((1,), (1,)), ((), ())), preferred_element_type=jnp.float32)


def front_kernel(dims, tok_ref, tap_ref, keep_ref, sml_ref, inw_ref, outw_ref,
                 in_out, out_out, sml_out, norm_out, inner_out, gate_out, conv_out, pre_out, far_out, drive_out, bx_out, cx_out, dtr_out,
                 in_vm, out_vm, norm_vm, inner, gate, conv, pre, far, drive, act, bx, cx, osem,
                 a0, a1, a2, a3, b0, b1, b2, b3, c0, c1, c2, c3):
    xw, rank, state, gain_w, width = dims
    t = tok_ref.shape[0]
    low = jnp.bfloat16
    f = lax.axis_index("fsdp")
    fh = f // 2
    outs = []

    def put(src, dst):
        c = pltpu.make_async_copy(src, dst, osem.at[len(outs)])
        c.start()
        outs.append(c)

    enter_square()
    sm = Spread(sml_ref, sml_out, a0, a1, a2, a3, 1)
    wi = Spread(inw_ref, in_vm, b0, b1, b2, b3, PARTS)
    wo = Spread(outw_ref, out_vm, c0, c1, c2, c3, PARTS)
    own_i = pltpu.make_async_copy(inw_ref, in_vm.at[f], osem.at[40])
    own_o = pltpu.make_async_copy(outw_ref, out_vm.at[f], osem.at[41])
    sm.begin()
    wi.begin()
    wo.begin()
    own_i.start()
    own_o.start()
    sml_out[f] = sml_ref[...]

    x = tok_ref[...].astype(jnp.float32)
    unit = (x * lax.rsqrt(jnp.mean(x * x, axis=-1, keepdims=True) + 1e-05))
    conv[:, :x.shape[1]] = unit

    sm.pump(0)
    sm.pump_pair(0)
    sm.whole().wait_recv()
    sm.land()
    at = xw + rank + state
    for s in range(4):
        g = sml_out[s, at + 7:at + 8, :gain_w].astype(jnp.float32)
        norm_vm[s // 2, :, (s % 2) * gain_w:(s % 2 + 1) * gain_w] = (conv[:, s * gain_w:(s + 1) * gain_w] * g).astype(low)
        norm_out[:, s * gain_w:(s + 1) * gain_w] = norm_vm[s // 2, :, (s % 2) * gain_w:(s % 2 + 1) * gain_w]

    own_i.wait()
    wi.whole().wait_recv()
    tile = 256

    def block(h, first, base, dst):
        def go(n, _):
            cols = pl.ds(pl.multiple_of(base + n * tile, tile), tile)
            here = pl.ds(pl.multiple_of(n * tile, tile), tile)
            acc = jnp.dot(norm_vm[h], jnp.concatenate([in_vm[2 * h, :, cols], in_vm[2 * h + 1, :, cols]], axis=0), preferred_element_type=jnp.float32)
            dst[:, here] = acc if first else dst[:, here] + acc
            return 0
        lax.fori_loop(0, dst.shape[1] // tile, go, 0)

    di = inner.shape[1]
    block(fh, True, 0, inner)
    block(fh, True, di, gate)
    for i in range(PARTS):
        wi.pump(i)
        if i > 0:
            wi.pump_pair(i - 1)
    wi.pump_pair(PARTS - 1)
    wi.land()
    for s in range(4):
        put(in_vm.at[s], in_out.at[s])
    block(1 - fh, False, 0, inner)
    put(inner, inner_out)
    wo.pump(0)
    block(1 - fh, False, di, gate)
    put(gate, gate_out)
    wo.pump(1)
    wo.pump_pair(0)

    per = width // 128

    for s in range(4):
        for q in range(per):
            ln = slice(s * width + q * 128, s * width + (q + 1) * 128)
            sl = slice(q * 128, (q + 1) * 128)
            v = inner[:, ln]
            w = [sml_out[s, at + k:at + k + 1, sl].astype(jnp.float32) for k in range(4)]
            acc = sml_out[s, at + 4:at + 5, sl].astype(jnp.float32) + w[3] * v
            for j in (1, 2, 3):
                acc = acc + w[3 - j] * (pltpu.roll(v, j, 0) * tap_ref[j - 1])
            conv[:, ln] = acc
            a = acc * jax.nn.sigmoid(acc)
            drive[:, ln] = a
            act[:, ln] = a.astype(low)
        put(conv.at[:, s * width:(s + 1) * width], conv_out.at[:, s * width:(s + 1) * width])
        if s == 0:
            wo.pump(2)
            wo.pump_pair(1)
        elif s == 1:
            wo.pump(3)
            wo.pump_pair(2)
        elif s == 2:
            wo.pump_pair(3)

    pt = jnp.zeros((2 * state, t), jnp.float32)
    dr = jnp.zeros((t, rank), jnp.float32)
    for s in range(4):
        al = act[:, s * width:(s + 1) * width]
        pt = pt + nt(sml_out[s, rank:xw, :], al)
        dr = dr + nt(al, sml_out[s, :rank, :])
    dtr = dr.astype(low)
    dtr_out[...] = dtr
    for tb in range(t // 128):
        for l in range(128):
            col = jnp.broadcast_to(pt[:, tb * 128 + l:tb * 128 + l + 1], (2 * state, 128))
            bx[tb * 128 + l] = col[:state]
            cx[tb * 128 + l] = col[state:]
    put(bx, bx_out)
    put(cx, cx_out)
    for s in range(4):
        cs = slice(s * width, (s + 1) * width)
        p = jnp.dot(dtr, sml_out[s, xw:xw + rank, :], preferred_element_type=jnp.float32) + sml_out[s, at + 5:at + 6, :].astype(jnp.float32)
        pre[:, cs] = p
        put(pre.at[:, cs], pre_out.at[:, cs])
        for q in range(per):
            ln = slice(s * width + q * 128, s * width + (q + 1) * 128)
            v = pre[:, ln]
            st = jnp.maximum(v, 0.0) + jnp.log1p(jnp.exp(-jnp.abs(v)))
            drive[:, ln] = drive[:, ln] * st
            far[:, ln] = jnp.where(keep_ref[...] > 0, st, 1e30)
        put(far.at[:, cs], far_out.at[:, cs])
        put(drive.at[:, cs], drive_out.at[:, cs])
    own_o.wait()
    wo.whole().wait_recv()
    wo.land()
    for s in range(4):
        put(out_vm.at[s], out_out.at[s])
    for g in (sm, wi, wo):
        g.finish()
    for c in outs:
        c.wait()


def front(tokens, tapb, keepb, packed, in_weight, out_weight, dims):
    xw, rank, state, gain_w, width = dims
    t, d = tokens.shape
    di = 4 * width
    low, f32 = jnp.bfloat16, jnp.float32
    vm = pl.BlockSpec(memory_space=pltpu.VMEM)
    hb = pl.BlockSpec(memory_space=pl.ANY)
    sds = jax.ShapeDtypeStruct
    wide = sds((t, di), f32)
    lanes = sds((t, state, 128), f32)
    return pl.pallas_call(
        functools.partial(front_kernel, dims),
        in_specs=[vm, vm, vm, vm, hb, hb],
        out_specs=[hb, hb, vm, vm, hb, hb, hb, hb, hb, hb, hb, hb, vm],
        out_shape=[sds((4,) + in_weight.shape, low), sds((4,) + out_weight.shape, low), sds((4,) + packed.shape, low), sds((t, d), low),
                   wide, wide, wide, wide, wide, wide, lanes, lanes, sds((t, rank), low)],
        scratch_shapes=[pltpu.VMEM((4,) + in_weight.shape, low), pltpu.VMEM((4,) + out_weight.shape, low), pltpu.VMEM((2, t, d // 2), low)]
        + [pltpu.VMEM((t, di), f32)] * 6 + [pltpu.VMEM((t, di), low)] + [pltpu.VMEM((t, state, 128), f32)] * 2
        + [pltpu.SemaphoreType.DMA((42,))] + spread_sems(1) + spread_sems(PARTS) + spread_sems(PARTS),
        compiler_params=pltpu.CompilerParams(collective_id=3, has_side_effects=True, vmem_limit_bytes=63 << 20),
        name="front",
    )(tokens, tapb, keepb, packed, in_weight, out_weight)


LANE = 128
NS = 16
TC = 32
CGF = 1024
CGB = 512


def bcast(ref, i, row):
    v = ref[i, pl.ds(row, 8, stride=0), :]
    return jnp.concatenate([v, v], axis=0)


def stage(src, dst):
    for i in range(dst.shape[0]):
        dst[i] = src[:, i * LANE:(i + 1) * LANE]


def fold(src, i):
    s = [src[i, pl.ds(q, 8, stride=8), :] for q in range(8)]
    return ((s[0] + s[1]) + (s[2] + s[3])) + ((s[4] + s[5]) + (s[6] + s[7]))


def fwd_kernel(dt_ref, dr_ref, b_ref, c_ref, a_ref, y_ref, hs_ref, part, dts, drs, hst):
    cg = dt_ref.shape[1]
    tiles = cg // LANE
    tc = dt_ref.shape[0]

    @pl.when(pl.program_id(1) == 0)
    def _():
        hst[...] = jnp.zeros_like(hst)

    hs_ref[0] = hst[...]
    stage(dt_ref, dts)
    stage(dr_ref, drs)

    def group(g, carry):
        t0 = pl.multiple_of(g * 8, 8)
        hs = list(carry)
        for k in range(8):
            bt = b_ref[t0 + k]
            ct = c_ref[t0 + k]
            for i in range(tiles):
                ln = slice(i * LANE, (i + 1) * LANE)
                d = bcast(dts, i, t0 + k)
                u = bcast(drs, i, t0 + k)
                a = jnp.exp2(d * a_ref[:, ln])
                h = a * hs[i] + bt * u
                hs[i] = h
                p = ct * h
                part[i, k * 8:(k + 1) * 8, :] = p[:8] + p[8:]
        for i in range(tiles):
            ln = slice(i * LANE, (i + 1) * LANE)
            y_ref[pl.ds(t0, 8), ln] = fold(part, i)
        return tuple(hs)

    init = tuple(hst[:, i * LANE:(i + 1) * LANE] for i in range(tiles))
    out = lax.fori_loop(0, tc // 8, group, init)
    for i in range(tiles):
        hst[:, i * LANE:(i + 1) * LANE] = out[i]


def scan_forward(dt, dr, bx, cx, a2, tc=TC, cg=CGF):
    t, c = dt.shape
    nt, nc = t // tc, c // cg
    return pl.pallas_call(
        fwd_kernel,
        grid=(nc, nt),
        in_specs=[
            pl.BlockSpec((tc, cg), lambda j, i: (i, j)),
            pl.BlockSpec((tc, cg), lambda j, i: (i, j)),
            pl.BlockSpec((tc, NS, LANE), lambda j, i: (i, 0, 0)),
            pl.BlockSpec((tc, NS, LANE), lambda j, i: (i, 0, 0)),
            pl.BlockSpec((NS, cg), lambda j, i: (0, j)),
        ],
        out_specs=[
            pl.BlockSpec((tc, cg), lambda j, i: (i, j)),
            pl.BlockSpec((1, NS, cg), lambda j, i: (i, 0, j)),
        ],
        out_shape=[
            jax.ShapeDtypeStruct((t, c), jnp.float32),
            jax.ShapeDtypeStruct((nt, NS, c), jnp.float32),
        ],
        scratch_shapes=[pltpu.VMEM((cg // LANE, 64, LANE), jnp.float32)] + [pltpu.VMEM((cg // LANE, tc, LANE), jnp.float32)] * 2 + [pltpu.VMEM((NS, cg), jnp.float32)],
        name="scan_forward",
    )(dt, dr, bx, cx, a2)


def bwd_kernel(dp, steps, dt_ref, dr_ref, dy_ref, b_ref, c_ref, a_ref, hs_ref, og_ref, gg_ref,
               za_ref, gb_ref, db_ref, dc_ref, rate_ref, os_ref, gs_ref,
               asc, hsc, pz, pg, dts, drs, dys, gst, rst, ores, gres, *comm):
    red = Reducer(dp, (og_ref, gg_ref), (ores, gres), comm, ROWS_B, SLACK_B)
    step = pl.program_id(0) * pl.num_programs(1) + pl.program_id(1)
    for n in range(red.ticks()):
        @pl.when(step == (n * (steps - 1)) // (red.ticks() - 1))
        def _(n=n):
            if n == 0:
                red.entry()
            red.tick(n)

    @pl.when(step == pl.num_programs(0) * pl.num_programs(1) - 1)
    def _():
        red.finish()
        os_ref[...] = ores[...]
        gs_ref[...] = gres[...]

    cg = dt_ref.shape[1]
    tiles = cg // LANE
    tc = dt_ref.shape[0]
    j = pl.program_id(0)
    i_t = pl.program_id(1)
    nt = pl.num_programs(1)

    @pl.when(i_t == 0)
    def _():
        gst[...] = jnp.zeros_like(gst)
        rst[...] = jnp.zeros_like(rst)

    stage(dt_ref, dts)
    stage(dr_ref, drs)
    stage(dy_ref, dys)
    lanes = [slice(i * LANE, (i + 1) * LANE) for i in range(tiles)]

    def fgroup(g, carry):
        t0 = pl.multiple_of(g * 8, 8)
        hs = list(carry)
        for k in range(8):
            bt = b_ref[t0 + k]
            for i in range(tiles):
                ln = lanes[i]
                d = bcast(dts, i, t0 + k)
                u = bcast(drs, i, t0 + k)
                a = jnp.exp2(d * a_ref[:, ln])
                asc[t0 + k, :, ln] = a
                hsc[t0 + k, :, ln] = hs[i]
                hs[i] = a * hs[i] + bt * u
        return tuple(hs)

    out = lax.fori_loop(0, tc // 8, fgroup, tuple(hs_ref[0, :, ln] for ln in lanes))
    for i in range(tiles):
        hsc[tc, :, lanes[i]] = out[i]

    base = pl.multiple_of((nt - 1 - i_t) * tc, tc)
    first = j == 0

    def bgroup(gi, carry):
        g = tc // 8 - 1 - gi
        t0 = pl.multiple_of(g * 8, 8)
        gs = list(carry[0])
        rs = list(carry[1])
        for k in range(7, -1, -1):
            bt = b_ref[t0 + k]
            ct = c_ref[t0 + k]
            accb = None
            for i in range(tiles):
                ln = lanes[i]
                d = bcast(dts, i, t0 + k)
                u = bcast(drs, i, t0 + k)
                w = bcast(dys, i, t0 + k)
                hnow = hsc[t0 + k + 1, :, ln]
                hprev = hsc[t0 + k, :, ln]
                a = asc[t0 + k, :, ln]
                gg = ct * w + gs[i]
                ga = gg * a
                z = ga * hprev
                rs[i] = rs[i] + z * d
                gs[i] = ga
                pa = z * a_ref[:, ln]
                pz[i, k * 8:(k + 1) * 8, :] = pa[:8] + pa[8:]
                pb = gg * bt
                pg[i, k * 8:(k + 1) * 8, :] = pb[:8] + pb[8:]
                vb = gg * u
                vc = w * hnow
                accb = vb if accb is None else accb + vb
                accc = vc if i == 0 else accc + vc
            row = base + t0 + k

            @pl.when(first)
            def _():
                db_ref[row] = accb
                dc_ref[row] = accc

            @pl.when(jnp.logical_not(first))
            def _():
                db_ref[row] = db_ref[row] + accb
                dc_ref[row] = dc_ref[row] + accc
        for i in range(tiles):
            ln = lanes[i]
            za_ref[pl.ds(t0, 8), ln] = fold(pz, i)
            gb_ref[pl.ds(t0, 8), ln] = fold(pg, i)
        return tuple(gs), tuple(rs)

    gs, rs = lax.fori_loop(0, tc // 8, bgroup, (tuple(gst[:, ln] for ln in lanes), tuple(rst[:, ln] for ln in lanes)))
    for i in range(tiles):
        gst[:, lanes[i]] = gs[i]
        rst[:, lanes[i]] = rs[i]

    @pl.when(i_t == nt - 1)
    def _():
        rate_ref[...] = rst[...]


def scan_backward(dp, dt, dr, dy, bx, cx, a2, hs, og, gg, tc=TC, cg=CGB):
    t, c = dt.shape
    nt, nc = t // tc, c // cg
    row = pl.BlockSpec((tc, cg), lambda j, i: (nt - 1 - i, j))
    bc = pl.BlockSpec((tc, NS, LANE), lambda j, i: (nt - 1 - i, 0, 0))
    full = pl.BlockSpec((t, NS, LANE), lambda j, i: (0, 0, 0), pipeline_mode=pl.Buffered(1))
    once = lambda s: pl.BlockSpec(s, lambda j, i: (0,) * len(s), pipeline_mode=pl.Buffered(1))
    og = og.reshape((2, 2) + og.shape[1:])
    gg = gg.reshape((2, 2) + gg.shape[1:])
    parts = [og.shape[2:], gg.shape[2:]]
    return pl.pallas_call(
        functools.partial(bwd_kernel, dp, nc * nt),
        grid=(nc, nt),
        in_specs=[row, row, row, bc, bc, pl.BlockSpec((NS, cg), lambda j, i: (0, j)),
                  pl.BlockSpec((1, NS, cg), lambda j, i: (nt - 1 - i, 0, j)), once(og.shape), once(gg.shape)],
        out_specs=[row, row, full, full, pl.BlockSpec((NS, cg), lambda j, i: (0, j)), once(parts[0]), once(parts[1])],
        out_shape=[
            jax.ShapeDtypeStruct((t, c), jnp.float32),
            jax.ShapeDtypeStruct((t, c), jnp.float32),
            jax.ShapeDtypeStruct((t, NS, LANE), jnp.float32),
            jax.ShapeDtypeStruct((t, NS, LANE), jnp.float32),
            jax.ShapeDtypeStruct((NS, c), jnp.float32),
            jax.ShapeDtypeStruct(parts[0], jnp.bfloat16),
            jax.ShapeDtypeStruct(parts[1], jnp.bfloat16),
        ],
        scratch_shapes=[
            pltpu.VMEM((tc, NS, cg), jnp.float32), pltpu.VMEM((tc + 1, NS, cg), jnp.float32),
            pltpu.VMEM((cg // LANE, 64, LANE), jnp.float32), pltpu.VMEM((cg // LANE, 64, LANE), jnp.float32),
            pltpu.VMEM((cg // LANE, tc, LANE), jnp.float32), pltpu.VMEM((cg // LANE, tc, LANE), jnp.float32), pltpu.VMEM((cg // LANE, tc, LANE), jnp.float32),
            pltpu.VMEM((NS, cg), jnp.float32), pltpu.VMEM((NS, cg), jnp.float32),
            pltpu.VMEM(parts[0], jnp.bfloat16), pltpu.VMEM(parts[1], jnp.bfloat16),
        ] + reducer_scratch(dp, parts, ROWS_B),
        compiler_params=pltpu.CompilerParams(vmem_limit_bytes=60 << 20, collective_id=2, has_side_effects=True),
        name="scan_backward",
    )(dt, dr, dy, bx, cx, a2, hs, og, gg)


def pack_small(gain, conv_w, conv_b, xproj, dt_w, dt_b, alog, skip):
    width = conv_b.shape[-1]
    gain_row = jnp.pad(gain[None], ((0, 0), (0, width - gain.shape[0])))
    return jnp.concatenate(
        [xproj.T, dt_w, alog, conv_w, conv_b[None], dt_b[None], skip[None], gain_row], axis=0
    )


def body(
    tokens,
    cluster_lengths,
    norm_gain,
    in_weight,
    conv_weight,
    conv_bias,
    xproj_weight,
    dt_weight,
    dt_bias,
    a_log,
    skip_gain,
    out_weight,
    cotangent,
):
    low = jnp.bfloat16
    gain_shard = norm_gain.shape[0]
    width = conv_bias.shape[0]
    packed = pack_small(norm_gain, conv_weight, conv_bias, xproj_weight, dt_weight, dt_bias, a_log, skip_gain)
    packed = jnp.pad(packed, ((0, -packed.shape[0] % 32), (0, 0)))
    shards = lax.axis_size("fsdp")
    xw, rank, state = xproj_weight.shape[1], dt_weight.shape[0], a_log.shape[0]
    inner_width = shards * width
    length = tokens.shape[0]
    tap_valid, keep_mask = cluster_masks(cluster_lengths)
    tapb = jnp.broadcast_to(tap_valid.T[1:, :, None], (KCONV - 1, length, LANE))
    keepb = jnp.broadcast_to(keep_mask[:, None], (length, LANE))
    (in_all, out_all, small, normed_low, inner_in, gate_in, conv_out, dt_pre, step_far, drive, bx, cx, dt_rounded) = front(
        tokens, tapb, keepb, packed, in_weight, out_weight, (xw, rank, state, gain_shard, width)
    )
    in_full = in_all.reshape(-1, in_weight.shape[1])
    out_full = out_all.reshape(-1, out_weight.shape[1])
    rows = jnp.moveaxis(small, 0, 1).reshape(small.shape[1], inner_width)
    xproj_t = rows[:xw]
    dt_full = rows[xw : xw + rank]
    at = xw + rank
    decay_rate = -jnp.exp(rows[at : at + state].astype(jnp.float32))
    at += state
    conv_taps = rows[at : at + KCONV].astype(jnp.float32)
    at += KCONV
    skip_value = rows[at + 2].astype(jnp.float32)
    gain_value = small[:, at + 3, :gain_shard].reshape(-1).astype(jnp.float32)
    inputs_full = tokens.astype(jnp.float32)
    mean_square = jnp.mean(inputs_full * inputs_full, axis=-1, keepdims=True)
    inverse_rms = lax.rsqrt(mean_square + epsilon)
    unit_rows = inputs_full * inverse_rms
    padded = jnp.pad(inner_in, ((KCONV - 1, 0), (0, 0)))
    conv_act = silu_of(conv_out)
    act_low = conv_act.astype(low)
    step_size = jax.nn.softplus(dt_pre)
    rate2 = decay_rate * LOG2E
    scanned, starts = scan_forward(step_far, drive, bx, cx, rate2)
    with_skip = scanned + skip_value * conv_act
    gate_act = silu_of(gate_in)
    gated_low = (with_skip * gate_act).astype(low)
    result = inputs_full + matmul(gated_low, out_full)
    output = result.astype(low)
    out_grad = left_inner(gated_low, cotangent)
    gated_grad = right_inner(cotangent, out_full)
    skip_part = gated_grad * gate_act
    gate_grad = gated_grad * with_skip * silu_slope(gate_in)
    gate_low = gate_grad.astype(low)
    gate_in_grad = left_inner(normed_low, gate_low)
    skip_grad = jnp.sum(skip_part * conv_act, axis=0)
    dp = lax.axis_size("dp")
    za, gb, dbx, dcx, rate_grad, out_share, gate_share = scan_backward(
        dp,
        step_far,
        drive,
        skip_part,
        bx,
        cx,
        rate2,
        starts,
        out_grad.astype(low).reshape(shards, -1, out_grad.shape[1]),
        gate_in_grad.astype(low).reshape(shards, -1, inner_width),
    )
    a_log_grad = rate_grad * decay_rate
    step_grad = za * LN2 + gb * conv_act
    act_scan = gb * step_size
    b_grad = jnp.sum(dbx, axis=-1)
    c_grad = jnp.sum(dcx, axis=-1)
    pre_grad = step_grad * jax.nn.sigmoid(dt_pre)
    dt_bias_grad = jnp.sum(pre_grad, axis=0)
    pre_low = pre_grad.astype(low)
    dt_weight_grad = left_inner(dt_rounded, pre_low)
    rank_grad = right_inner(pre_low, dt_full)
    proj_grad = jnp.concatenate([rank_grad, b_grad, c_grad], axis=1).astype(low)
    xproj_grad = left_inner(proj_grad, act_low)
    act_grad = matmul(proj_grad, xproj_t) + skip_part * skip_value + act_scan
    conv_grad = act_grad * silu_slope(conv_out)
    conv_bias_grad = jnp.sum(conv_grad, axis=0)
    inner_grad = jnp.zeros_like(inner_in)
    tap_grads = []
    for offset in range(KCONV):
        lag_now = KCONV - 1 - offset
        masked = conv_grad * tap_valid[:, lag_now : lag_now + 1]
        tap_grads.append(jnp.sum(masked * padded[offset : offset + length], axis=0))
        inner_grad = (
            inner_grad + conv_taps[offset] * jnp.pad(masked, ((0, lag_now), (0, 0)))[lag_now:]
        )
    conv_weight_grad = jnp.stack(tap_grads)
    inner_low = inner_grad.astype(low)
    inner_in_grad = left_inner(normed_low, inner_low)
    normed_grad = right_inner(inner_low, in_full[:, :inner_width]) + right_inner(
        gate_low, in_full[:, inner_width:]
    )
    gain_grad = jnp.sum(normed_grad * unit_rows, axis=0)
    scaled = normed_grad * gain_value
    input_grad = cotangent.astype(jnp.float32) + inverse_rms * (
        scaled - unit_rows * jnp.mean(scaled * unit_rows, axis=-1, keepdims=True)
    )
    gain_rows = jnp.pad(gain_grad.reshape(shards, gain_shard), ((0, 0), (0, width - gain_shard)))
    small_grad = jnp.concatenate(
        [
            xproj_grad,
            dt_weight_grad,
            a_log_grad,
            conv_weight_grad,
            conv_bias_grad[None],
            dt_bias_grad[None],
            skip_grad[None],
            gain_rows.reshape(1, -1),
        ],
        axis=0,
    )
    unit = split_of(dp)[1]
    small_grad = jnp.pad(small_grad, ((0, -small_grad.shape[0] % unit), (0, 0)))
    small_rows = small_grad.shape[0]
    small_grad = jnp.moveaxis(small_grad.reshape(small_rows, shards, width), 1, 0)
    reduced = reduce_all(
        dp,
        [
            inner_in_grad.astype(low).reshape(shards, -1, inner_width),
            small_grad.astype(low),
        ],
        collective_id=1,
    )
    inner_share, small_share = (v.astype(jnp.float32) for v in reduced)
    out_share, gate_share = out_share.astype(jnp.float32), gate_share.astype(jnp.float32)
    at = xw + rank + state
    return (
        output,
        input_grad,
        small_share[at + KCONV + 3, :gain_shard],
        jnp.concatenate([inner_share, gate_share], axis=1),
        small_share[at : at + KCONV],
        small_share[at + KCONV],
        small_share[:xw].T,
        small_share[xw : xw + rank],
        small_share[at + KCONV + 1],
        small_share[xw + rank : at],
        small_share[at + KCONV + 2],
        out_share,
    )


def solution(mesh):
    in_specs = (
        P(("dp", "fsdp"), None),
        P(("dp", "fsdp"), None),
        P("fsdp"),
        P("fsdp", None),
        P(None, "fsdp"),
        P("fsdp"),
        P("fsdp", None),
        P(None, "fsdp"),
        P("fsdp"),
        P(None, "fsdp"),
        P("fsdp"),
        P("fsdp", None),
        P(("dp", "fsdp"), None),
    )
    out_specs = (
        P(("dp", "fsdp"), None),
        P(("dp", "fsdp"), None),
        P("fsdp"),
        P("fsdp", None),
        P(None, "fsdp"),
        P("fsdp"),
        P("fsdp", None),
        P(None, "fsdp"),
        P("fsdp"),
        P(None, "fsdp"),
        P("fsdp"),
        P("fsdp", None),
    )
    return jax.shard_map(body, mesh=mesh, in_specs=in_specs, out_specs=out_specs, check_vma=False)
```

```python
import functools

import jax
import jax.numpy as jnp
import numpy as np
from jax import lax
from jax.experimental import pallas as pl
from jax.experimental.pallas import tpu as pltpu
from jax.sharding import PartitionSpec as P

KCONV = 4
LENGTH = 512
LOG2E = float(np.log2(np.e))
LN2 = float(np.log(2.0))
FAR = 1e30


epsilon = 1e-05


def matmul(former, latter):
    return jnp.dot(former, latter, preferred_element_type=jnp.float32)


def left_inner(former, latter):
    return lax.dot_general(
        former, latter, (((0,), (0,)), ((), ())), preferred_element_type=jnp.float32
    )


def right_inner(former, latter):
    return lax.dot_general(
        former, latter, (((1,), (1,)), ((), ())), preferred_element_type=jnp.float32
    )


def silu_of(values):
    return values * jax.nn.sigmoid(values)


def silu_slope(values):
    logistic = jax.nn.sigmoid(values)
    return logistic * (1.0 + values * (1.0 - logistic))


def cluster_masks(lengths):
    cluster_ends = jnp.cumsum(lengths, axis=-1)
    starts = cluster_ends - lengths
    positions = jnp.arange(LENGTH, dtype=jnp.int32)
    before = starts[:, None, :] <= positions[None, :, None]
    segment_start = jnp.max(jnp.where(before, starts[:, None, :], 0), axis=-1)
    keep_mask = (positions[None, :] > segment_start).astype(jnp.float32)
    lag_index = jnp.arange(KCONV, dtype=jnp.int32)
    tap_valid = (
        positions[None, :, None] - lag_index[None, None, :] >= segment_start[:, :, None]
    ).astype(jnp.float32)
    return (tap_valid[0], keep_mask[0])

MESH = pl.DeviceIdType.MESH
COLS = 1024
ROWS = 32
SLACK = 3
ROWS_B = 64
SLACK_B = 2


class Reducer:

    def __init__(self, dp, sources, targets, scratch, rows=ROWS, slack=SLACK):
        self.slack = slack
        self.nz = dp // 2
        self.sources, self.targets = sources, targets
        (self.rc, self.ry, self.rx, self.rz, self.s_one, self.r_one, self.s_rs, self.r_rs, self.s_ag, self.r_ag) = scratch
        self.me_dp, self.me_f = lax.axis_index("dp"), lax.axis_index("fsdp")
        self.fh, self.fl = self.me_f // 2, self.me_f % 2
        self.z, self.x = self.me_dp // 2, self.me_dp % 2
        self.pieces_c, self.rows = split_of(dp, rows)
        self.pieces_r = self.nz // self.pieces_c
        self.chunks = chunk_list([t.shape for t in targets], self.rows)
        self.core = (self.me_dp, self.fh * 2 + (1 - self.fl))
        self.other = (self.me_dp, (1 - self.fh) * 2 + self.fl)
        self.pair = (self.z * 2 + (1 - self.x), self.me_f)

    def peer(self, o):
        return lax.rem(self.z + o, self.nz)

    def entry(self):
        barrier = pltpu.get_barrier_semaphore()
        ids = [self.core, self.other, self.pair] + [(self.peer(o) * 2 + self.x, self.me_f) for o in range(1, self.nz)]
        for d in ids:
            pl.semaphore_signal(barrier, inc=1, device_id=d, device_id_type=MESH)
        pl.semaphore_wait(barrier, len(ids))

    def copy(self, src, dst, send, recv, device):
        return pltpu.make_async_remote_copy(src_ref=src, dst_ref=dst, send_sem=send, recv_sem=recv, device_id=device, device_id_type=MESH)

    def copies(self, stage, k):
        a, r0, c0, w = self.chunks[k]
        r, hr = self.rows, self.rows // 2
        if stage == 0:
            src = self.sources[a].at[:, 1 - self.fl, r0:r0 + r, c0:c0 + w]
            return [self.copy(src, self.rc.at[k, :, :, :w], self.s_one.at[0, k], self.r_one.at[0, k], self.core)]
        if stage == 1:
            return [self.copy(self.rc.at[k, 1 - self.fh, :, :w], self.ry.at[k, :, :w], self.s_one.at[1, k], self.r_one.at[1, k], self.other)]
        if stage == 2:
            src = self.ry.at[k, pl.ds(pl.multiple_of((1 - self.x) * hr, hr), hr), :w]
            return [self.copy(src, self.rx.at[k, :, :w], self.s_one.at[2, k], self.r_one.at[2, k], self.pair)]
        out = []
        if stage == 5:
            rows = pl.ds(pl.multiple_of(r0 + self.x * hr, hr), hr)
            t = self.targets[a].at[rows, c0:c0 + w]
            return [self.copy(t, t, self.s_one.at[3, k], self.r_one.at[3, k], self.pair)]
        for o in range(1, self.nz):
            j = self.peer(o)
            device = (j * 2 + self.x, self.me_f)
            if stage == 3:
                pr, pc = self.place(j, w)
                out.append(self.copy(self.rx.at[k, pr, pc], self.rz.at[k, o - 1, :, :w // self.pieces_c], self.s_rs.at[k, o - 1], self.r_rs.at[k, o - 1], device))
            else:
                t = self.own(k)
                out.append(self.copy(t, t, self.s_ag.at[k, o - 1], self.r_ag.at[k, o - 1], device))
        return out

    def place(self, j, w, r0=0, c0=0):
        pr, pw = self.rows // 2 // self.pieces_r, w // self.pieces_c
        return (pl.ds(pl.multiple_of(r0 + (j // self.pieces_c) * pr, 16), pr), pl.ds(pl.multiple_of(c0 + lax.rem(j, self.pieces_c) * pw, 128), pw))

    def own(self, k):
        a, r0, c0, w = self.chunks[k]
        pr, pc = self.place(self.z, w, r0 + self.x * (self.rows // 2), c0)
        return self.targets[a].at[pr, pc]

    def absorb(self, stage, k):
        a, r0, c0, w = self.chunks[k]
        r, hr = self.rows, self.rows // 2
        for c in self.copies(stage, k):
            c.wait_recv()
        if stage == 0:
            for h in range(2):
                self.rc[k, h, :, :w] = self.rc[k, h, :, :w] + self.sources[a][h, self.fl, r0:r0 + r, c0:c0 + w]
        elif stage == 1:
            self.ry[k, :, :w] = self.ry[k, :, :w] + self.rc[k, self.fh, :, :w]
        elif stage == 2:
            mine = self.ry[k, pl.ds(pl.multiple_of(self.x * hr, hr), hr), :w]
            self.rx[k, :, :w] = self.rx[k, :, :w] + mine
        elif stage == 3:
            pr, pc = self.place(self.z, w)
            total = self.rx[k, pr, pc].astype(jnp.float32)
            for o in range(1, self.nz):
                total = total + self.rz[k, o - 1, :, :w // self.pieces_c].astype(jnp.float32)
            self.own(k)[...] = total.astype(jnp.bfloat16)

    def ticks(self):
        return len(self.chunks) + 6 * self.slack

    def tick(self, n):
        live = [(s, n - self.slack * s) for s in range(7) if 0 <= n - self.slack * s < len(self.chunks)]
        for s, k in reversed(live):
            if s > 0:
                self.absorb(s - 1, k)
        for s, k in reversed(live):
            if s < 6:
                for c in self.copies(s, k):
                    c.start()

    def finish(self):
        for k in range(len(self.chunks)):
            for s in range(6):
                for c in self.copies(s, k):
                    c.wait_send()


def split_of(dp, rows=ROWS):
    nz = dp // 2
    pieces_c = min(nz, COLS // 128, 4)
    return pieces_c, max(rows, 32 * (nz // pieces_c))


def chunk_list(shapes, rows):
    out = []
    for a, (r, c) in enumerate(shapes):
        w = min(c, COLS)
        for c0 in range(0, c, w):
            for r0 in range(0, r, rows):
                out.append((a, r0, c0, w))
    return out


def reducer_scratch(dp, shapes, rows=ROWS):
    nz = dp // 2
    pieces_c, rows = split_of(dp, rows)
    n = len(chunk_list(shapes, rows))
    low = jnp.bfloat16
    return [
        pltpu.VMEM((n, 2, rows, COLS), low),
        pltpu.VMEM((n, rows, COLS), low),
        pltpu.VMEM((n, rows // 2, COLS), low),
        pltpu.VMEM((n, nz - 1, rows // 2 // (nz // pieces_c), COLS // pieces_c), low),
        pltpu.SemaphoreType.DMA((4, n)),
        pltpu.SemaphoreType.DMA((4, n)),
        pltpu.SemaphoreType.DMA((n, nz - 1)),
        pltpu.SemaphoreType.DMA((n, nz - 1)),
        pltpu.SemaphoreType.DMA((n, nz - 1)),
        pltpu.SemaphoreType.DMA((n, nz - 1)),
    ]


PARTS = 4


class Spread:

    def __init__(self, shard, full, s_one, r_one, s_part, r_part, parts):
        dp, f = lax.axis_index("dp"), lax.axis_index("fsdp")
        fh, fl = f // 2, f % 2
        self.f, self.x = f, dp % 2
        self.far = (1 - fh) * 2 + fl
        self.core = (dp, fh * 2 + (1 - fl))
        self.other = (dp, self.far)
        self.pair = ((dp // 2) * 2 + (1 - self.x), f)
        self.shard, self.full, self.parts = shard, full, parts
        self.s_one, self.r_one, self.s_part, self.r_part = s_one, r_one, s_part, r_part
        self.half = shard.shape[0] // 2
        self.rows = self.half // parts

    def span(self, half, i):
        return pl.ds(pl.multiple_of(half * self.half + i * self.rows, self.rows), self.rows)

    def send(self, src, dst, s, r, device):
        return pltpu.make_async_remote_copy(src_ref=src, dst_ref=dst, send_sem=s, recv_sem=r, device_id=device, device_id_type=pl.DeviceIdType.MESH)

    def whole(self):
        return self.send(self.shard, self.full.at[self.f], self.s_one, self.r_one, self.core)

    def across(self, i):
        rows = self.span(self.x, i)
        return self.send(self.shard.at[rows], self.full.at[self.f, rows], self.s_part.at[0, i], self.r_part.at[0, i], self.other)

    def onward(self, kind, i):
        rows = self.span(self.x if kind < 3 else 1 - self.x, i)
        ref = self.full.at[self.far, rows]
        return self.send(ref, ref, self.s_part.at[kind, i], self.r_part.at[kind, i], self.pair if kind == 1 else self.core)

    def begin(self):
        self.whole().start()
        for i in range(self.parts):
            self.across(i).start()

    def pump(self, i):
        self.across(i).wait_recv()
        self.onward(1, i).start()
        self.onward(2, i).start()

    def pump_pair(self, i):
        self.onward(1, i).wait_recv()
        self.onward(3, i).start()

    def land(self):
        for i in range(self.parts):
            self.onward(2, i).wait_recv()
            self.onward(3, i).wait_recv()

    def finish(self):
        self.whole().wait_send()
        for i in range(self.parts):
            self.across(i).wait_send()
            for kind in (1, 2, 3):
                self.onward(kind, i).wait_send()


def spread_sems(parts):
    return [pltpu.SemaphoreType.DMA, pltpu.SemaphoreType.DMA, pltpu.SemaphoreType.DMA((4, parts)), pltpu.SemaphoreType.DMA((4, parts))]


def enter_square():
    dp, f = lax.axis_index("dp"), lax.axis_index("fsdp")
    fh, fl = f // 2, f % 2
    barrier = pltpu.get_barrier_semaphore()
    for d in ((dp, fh * 2 + (1 - fl)), (dp, (1 - fh) * 2 + fl), ((dp // 2) * 2 + (1 - dp % 2), f)):
        pl.semaphore_signal(barrier, inc=1, device_id=d, device_id_type=pl.DeviceIdType.MESH)
    pl.semaphore_wait(barrier, 3)


def nt(a, b):
    return lax.dot_general(a, b, (((1,), (1,)), ((), ())), preferred_element_type=jnp.float32)


def front_kernel(dims, tok_ref, tap_ref, keep_ref, sml_ref, inw_ref, outw_ref,
                 in_out, out_out, sml_out, norm_out, inner_out, gate_out, conv_out, pre_out, far_out, drive_out, bx_out, cx_out, dtr_out,
                 in_vm, out_vm, norm_vm, inner, gate, conv, pre, far, drive, act, bx, cx, osem,
                 a0, a1, a2, a3, b0, b1, b2, b3, c0, c1, c2, c3):
    xw, rank, state, gain_w, width = dims
    t = tok_ref.shape[0]
    low = jnp.bfloat16
    f = lax.axis_index("fsdp")
    fh = f // 2
    outs = []

    def put(src, dst):
        c = pltpu.make_async_copy(src, dst, osem.at[len(outs)])
        c.start()
        outs.append(c)

    enter_square()
    sm = Spread(sml_ref, sml_out, a0, a1, a2, a3, 1)
    wi = Spread(inw_ref, in_vm, b0, b1, b2, b3, PARTS)
    wo = Spread(outw_ref, out_vm, c0, c1, c2, c3, PARTS)
    own_i = pltpu.make_async_copy(inw_ref, in_vm.at[f], osem.at[40])
    own_o = pltpu.make_async_copy(outw_ref, out_vm.at[f], osem.at[41])
    sm.begin()
    wi.begin()
    wo.begin()
    own_i.start()
    own_o.start()
    sml_out[f] = sml_ref[...]

    x = tok_ref[...].astype(jnp.float32)
    unit = (x * lax.rsqrt(jnp.mean(x * x, axis=-1, keepdims=True) + 1e-05))
    conv[:, :x.shape[1]] = unit

    sm.pump(0)
    sm.pump_pair(0)
    sm.whole().wait_recv()
    sm.land()
    at = xw + rank + state
    for s in range(4):
        g = sml_out[s, at + 7:at + 8, :gain_w].astype(jnp.float32)
        norm_vm[s // 2, :, (s % 2) * gain_w:(s % 2 + 1) * gain_w] = (conv[:, s * gain_w:(s + 1) * gain_w] * g).astype(low)
        norm_out[:, s * gain_w:(s + 1) * gain_w] = norm_vm[s // 2, :, (s % 2) * gain_w:(s % 2 + 1) * gain_w]

    own_i.wait()
    wi.whole().wait_recv()
    tile = 256

    def block(h, first, base, dst):
        def go(n, _):
            cols = pl.ds(pl.multiple_of(base + n * tile, tile), tile)
            here = pl.ds(pl.multiple_of(n * tile, tile), tile)
            acc = jnp.dot(norm_vm[h], jnp.concatenate([in_vm[2 * h, :, cols], in_vm[2 * h + 1, :, cols]], axis=0), preferred_element_type=jnp.float32)
            dst[:, here] = acc if first else dst[:, here] + acc
            return 0
        lax.fori_loop(0, dst.shape[1] // tile, go, 0)

    di = inner.shape[1]
    block(fh, True, 0, inner)
    block(fh, True, di, gate)
    for i in range(PARTS):
        wi.pump(i)
        if i > 0:
            wi.pump_pair(i - 1)
    wi.pump_pair(PARTS - 1)
    wi.land()
    for s in range(4):
        put(in_vm.at[s], in_out.at[s])
    block(1 - fh, False, 0, inner)
    put(inner, inner_out)
    wo.pump(0)
    block(1 - fh, False, di, gate)
    put(gate, gate_out)
    wo.pump(1)
    wo.pump_pair(0)

    per = width // 128

    for s in range(4):
        for q in range(per):
            ln = slice(s * width + q * 128, s * width + (q + 1) * 128)
            sl = slice(q * 128, (q + 1) * 128)
            v = inner[:, ln]
            w = [sml_out[s, at + k:at + k + 1, sl].astype(jnp.float32) for k in range(4)]
            acc = sml_out[s, at + 4:at + 5, sl].astype(jnp.float32) + w[3] * v
            for j in (1, 2, 3):
                acc = acc + w[3 - j] * (pltpu.roll(v, j, 0) * tap_ref[j - 1])
            conv[:, ln] = acc
            a = acc * jax.nn.sigmoid(acc)
            drive[:, ln] = a
            act[:, ln] = a.astype(low)
        put(conv.at[:, s * width:(s + 1) * width], conv_out.at[:, s * width:(s + 1) * width])
        if s == 0:
            wo.pump(2)
            wo.pump_pair(1)
        elif s == 1:
            wo.pump(3)
            wo.pump_pair(2)
        elif s == 2:
            wo.pump_pair(3)

    pt = jnp.zeros((2 * state, t), jnp.float32)
    dr = jnp.zeros((t, rank), jnp.float32)
    for s in range(4):
        al = act[:, s * width:(s + 1) * width]
        pt = pt + nt(sml_out[s, rank:xw, :], al)
        dr = dr + nt(al, sml_out[s, :rank, :])
    dtr = dr.astype(low)
    dtr_out[...] = dtr
    for tb in range(t // 128):
        for l in range(128):
            col = jnp.broadcast_to(pt[:, tb * 128 + l:tb * 128 + l + 1], (2 * state, 128))
            bx[tb * 128 + l] = col[:state]
            cx[tb * 128 + l] = col[state:]
    put(bx, bx_out)
    put(cx, cx_out)
    for s in range(4):
        cs = slice(s * width, (s + 1) * width)
        p = jnp.dot(dtr, sml_out[s, xw:xw + rank, :], preferred_element_type=jnp.float32) + sml_out[s, at + 5:at + 6, :].astype(jnp.float32)
        pre[:, cs] = p
        put(pre.at[:, cs], pre_out.at[:, cs])
        for q in range(per):
            ln = slice(s * width + q * 128, s * width + (q + 1) * 128)
            v = pre[:, ln]
            st = jnp.maximum(v, 0.0) + jnp.log1p(jnp.exp(-jnp.abs(v)))
            drive[:, ln] = drive[:, ln] * st
            far[:, ln] = jnp.where(keep_ref[...] > 0, st, 1e30)
        put(far.at[:, cs], far_out.at[:, cs])
        put(drive.at[:, cs], drive_out.at[:, cs])
    own_o.wait()
    wo.whole().wait_recv()
    wo.land()
    for s in range(4):
        put(out_vm.at[s], out_out.at[s])
    for g in (sm, wi, wo):
        g.finish()
    for c in outs:
        c.wait()


def front(tokens, tapb, keepb, packed, in_weight, out_weight, dims):
    xw, rank, state, gain_w, width = dims
    t, d = tokens.shape
    di = 4 * width
    low, f32 = jnp.bfloat16, jnp.float32
    vm = pl.BlockSpec(memory_space=pltpu.VMEM)
    hb = pl.BlockSpec(memory_space=pl.ANY)
    sds = jax.ShapeDtypeStruct
    wide = sds((t, di), f32)
    lanes = sds((t, state, 128), f32)
    return pl.pallas_call(
        functools.partial(front_kernel, dims),
        in_specs=[vm, vm, vm, vm, hb, hb],
        out_specs=[hb, hb, vm, vm, hb, hb, hb, hb, hb, hb, hb, hb, vm],
        out_shape=[sds((4,) + in_weight.shape, low), sds((4,) + out_weight.shape, low), sds((4,) + packed.shape, low), sds((t, d), low),
                   wide, wide, wide, wide, wide, wide, lanes, lanes, sds((t, rank), low)],
        scratch_shapes=[pltpu.VMEM((4,) + in_weight.shape, low), pltpu.VMEM((4,) + out_weight.shape, low), pltpu.VMEM((2, t, d // 2), low)]
        + [pltpu.VMEM((t, di), f32)] * 6 + [pltpu.VMEM((t, di), low)] + [pltpu.VMEM((t, state, 128), f32)] * 2
        + [pltpu.SemaphoreType.DMA((42,))] + spread_sems(1) + spread_sems(PARTS) + spread_sems(PARTS),
        compiler_params=pltpu.CompilerParams(collective_id=3, has_side_effects=True, vmem_limit_bytes=63 << 20),
        name="front",
    )(tokens, tapb, keepb, packed, in_weight, out_weight)


def tn(a, b):
    return lax.dot_general(a, b, (((0,), (0,)), ((), ())), preferred_element_type=jnp.float32)


def sum8(v):
    return jnp.sum(v.reshape(v.shape[0] // 8, 8, v.shape[1]), axis=0)


def back_kernel(dp, dims, za_h, gb_h, pre_h, dys_h, conv_h, inner_h, inw_h, gl_h, nt_h, tok_ref, cot_ref, sml_ref, dtrt_ref, dbt_ref, rate_ref, tap_ref,
                ish_ref, ssh_ref, ig_ref,
                za, gb, pre, dys, conv, inner, inw, gl, normt, prelow, actlow, pt, agv, misc, gainv, ng, isrc, ssrc, csem, *comm):
    xw, rank, state, gain_w, width = dims
    t = tok_ref.shape[0]
    low = jnp.bfloat16
    at = xw + rank + state
    per = width // 128

    def fetch(k, src, dst):
        c = pltpu.make_async_copy(src, dst, csem.at[k])
        c.start()
        return c

    waits = []
    for s in range(4):
        cs = slice(s * width, (s + 1) * width)
        waits.append([fetch(s * 8 + k, h.at[:, cs], v.at[:, cs]) for k, (h, v) in enumerate(((conv_h, conv), (gb_h, gb), (pre_h, pre), (dys_h, dys), (za_h, za)))])
    late = [fetch(32, inner_h, inner), fetch(33, nt_h, normt), fetch(34, inw_h, inw), fetch(35, gl_h, gl)]
    red = Reducer(dp, (isrc, ssrc), (ish_ref, ssh_ref), comm)
    red.entry()
    misc[...] = jnp.zeros_like(misc)
    rankt = jnp.zeros((rank, t), jnp.float32)
    for s in range(4):
        for c in waits[s]:
            c.wait()

        def tile(q, _, s=s):
            ln = pl.ds(pl.multiple_of(s * width + q * 128, 128), 128)
            lq = pl.ds(pl.multiple_of(q * 128, 128), 128)
            skip = sml_ref[s, at + 6:at + 7, lq].astype(jnp.float32)

            def rows(r, sums):
                rs = pl.ds(pl.multiple_of(r * 64, 64), 64)
                cv = conv[rs, ln]
                sg = jax.nn.sigmoid(cv)
                ac = cv * sg
                gv = gb[rs, ln]
                pv = pre[rs, ln]
                dy = dys[rs, ln]
                st = jnp.maximum(pv, 0.0) + jnp.log1p(jnp.exp(-jnp.abs(pv)))
                pg = (za[rs, ln] * LN2 + gv * ac) * jax.nn.sigmoid(pv)
                prelow[rs, lq] = pg.astype(low)
                actlow[rs, ln] = ac.astype(low)
                dys[rs, ln] = dy * skip + gv * st
                conv[rs, ln] = sg * (1.0 + cv * (1.0 - sg))
                return sums[0] + sum8(pg), sums[1] + sum8(dy * ac)

            zero = jnp.zeros((8, 128), jnp.float32)
            bias, skips = lax.fori_loop(0, t // 64, rows, (zero, zero))
            misc[5:6, ln] = jnp.sum(bias, axis=0, keepdims=True)
            misc[6:7, ln] = jnp.sum(skips, axis=0, keepdims=True)
            return 0

        lax.fori_loop(0, per, tile, 0)
        p = prelow[...]
        ssrc[s // 2, s % 2, xw:xw + rank, :] = jnp.dot(dtrt_ref[...], p, preferred_element_type=jnp.float32).astype(low)
        rankt = rankt + nt(sml_ref[s, xw:xw + rank, :], p)
    pt[:rank] = rankt.astype(low)
    pt[rank:] = dbt_ref[...].astype(low)
    for c in late[:2]:
        c.wait()
    done = 0
    for s in range(4):
        cs = slice(s * width, (s + 1) * width)
        agv[...] = tn(pt[...], sml_ref[s, :xw, :])
        ssrc[s // 2, s % 2, :xw, :] = jnp.dot(pt[...], actlow[:, cs], preferred_element_type=jnp.float32).astype(low)
        ssrc[s // 2, s % 2, xw + rank:at, :] = rate_ref[:, cs].astype(low)

        def tile2(q, _, s=s):
            ln = pl.ds(pl.multiple_of(s * width + q * 128, 128), 128)
            lq = pl.ds(pl.multiple_of(q * 128, 128), 128)
            cg = (agv[:, lq] + dys[:, ln]) * conv[:, ln]
            v = inner[:, ln]
            ig = sml_ref[s, at + 3:at + 4, lq].astype(jnp.float32) * cg
            misc[3:4, ln] = jnp.sum(sum8(cg * v), axis=0, keepdims=True)
            misc[4:5, ln] = jnp.sum(sum8(cg), axis=0, keepdims=True)
            for j in (1, 2, 3):
                m = cg * tap_ref[j - 1]
                misc[3 - j:4 - j, ln] = jnp.sum(sum8(m * pltpu.roll(v, j, 0)), axis=0, keepdims=True)
                ig = ig + sml_ref[s, at + 3 - j:at + 4 - j, lq].astype(jnp.float32) * pltpu.roll(m, t - j, 0)
            actlow[:, ln] = ig.astype(low)
            return 0

        lax.fori_loop(0, per, tile2, 0)
        for k in range(4):
            rows = slice(k * gain_w, (k + 1) * gain_w)
            isrc[k // 2, k % 2, :, cs] = jnp.dot(normt[rows, :], actlow[:, cs], preferred_element_type=jnp.float32).astype(low)
        ready = len([c for c in red.chunks if c[0] == 0 and c[2] + c[3] <= (s + 1) * width])
        if s == 2:
            half = ready // 2
            while done < half:
                red.tick(done)
                done += 1
    for c in late[2:]:
        c.wait()
    small0 = len([c for c in red.chunks if c[0] == 0])
    for blk in range(8):
        if done < small0:
            red.tick(done)
            done += 1
        src = gl if blk < 4 else actlow
        base = (blk % 4) * width
        wcol = (4 * width if blk < 4 else 0) + base
        for k in range(4):
            rows = slice(k * gain_w, (k + 1) * gain_w)
            part = nt(src[:, base:base + width], inw[k, :, wcol:wcol + width])
            ng[:, rows] = part if blk == 0 else ng[:, rows] + part
    for k in range(4):
        gainv[0:1, k * gain_w:(k + 1) * gain_w] = sml_ref[k, at + 7:at + 8, :gain_w].astype(jnp.float32)

    def fin(r, acc):
        rs = pl.ds(pl.multiple_of(r * 32, 32), 32)
        x = tok_ref[rs, :].astype(jnp.float32)
        inv = lax.rsqrt(jnp.mean(x * x, axis=-1, keepdims=True) + 1e-05)
        u = x * inv
        d = ng[rs, :]
        e = d * gainv[0:1, :]
        ig_ref[rs, :] = cot_ref[rs, :].astype(jnp.float32) + inv * (e - u * jnp.mean(e * u, axis=-1, keepdims=True))
        return acc + sum8(d * u)

    gsum = lax.fori_loop(0, t // 32, fin, jnp.zeros((8, ng.shape[1]), jnp.float32))
    gsum = jnp.sum(gsum, axis=0, keepdims=True)
    for k in range(4):
        misc[7:8, k * width:k * width + gain_w] = gsum[:, k * gain_w:(k + 1) * gain_w]
    for k in range(4):
        ssrc[k // 2, k % 2, at:at + 16, :] = misc[:, k * width:(k + 1) * width].astype(low)
        if ssrc.shape[2] > at + 16:
            ssrc[k // 2, k % 2, at + 16:, :] = jnp.zeros((ssrc.shape[2] - at - 16, width), low)
    while done < red.ticks():
        red.tick(done)
        done += 1
    red.finish()


def back(dp, dims, za, gb, pre, dys, conv, inner, in_all, gate_low, normt, tokens, cot, small, dtrt, dbt, rate, tapb):
    xw, rank, state, gain_w, width = dims
    t, d = tokens.shape
    di = 4 * width
    low, f32 = jnp.bfloat16, jnp.float32
    unit = split_of(dp)[1]
    srows = -(-(xw + rank + state + 16) // unit) * unit
    shapes = [(gain_w, di), (srows, width)]
    vm = pl.BlockSpec(memory_space=pltpu.VMEM)
    hb = pl.BlockSpec(memory_space=pl.ANY)
    sds = jax.ShapeDtypeStruct
    return pl.pallas_call(
        functools.partial(back_kernel, dp, dims),
        in_specs=[hb] * 9 + [vm] * 7,
        out_specs=[vm] * 3,
        out_shape=[sds(shapes[0], low), sds(shapes[1], low), sds((t, d), f32)],
        scratch_shapes=[pltpu.VMEM((t, di), f32)] * 6
        + [pltpu.VMEM(in_all.shape, low), pltpu.VMEM((t, di), low), pltpu.VMEM((d, t), low), pltpu.VMEM((t, width), low), pltpu.VMEM((t, di), low),
           pltpu.VMEM((xw, t), low), pltpu.VMEM((t, width), f32), pltpu.VMEM((16, di), f32), pltpu.VMEM((8, d), f32), pltpu.VMEM((t, d), f32),
           pltpu.VMEM((2, 2) + shapes[0], low), pltpu.VMEM((2, 2) + shapes[1], low), pltpu.SemaphoreType.DMA((36,))]
        + reducer_scratch(dp, shapes),
        compiler_params=pltpu.CompilerParams(collective_id=1, has_side_effects=True, vmem_limit_bytes=63 << 20),
        name="back",
    )(za, gb, pre, dys, conv, inner, in_all, gate_low, normt, tokens, cot, small, dtrt, dbt, rate, tapb)


LANE = 128
NS = 16
TC = 32
CGF = 1024
CGB = 512


def bcast(ref, i, row):
    v = ref[i, pl.ds(row, 8, stride=0), :]
    return jnp.concatenate([v, v], axis=0)


def stage(src, dst):
    for i in range(dst.shape[0]):
        dst[i] = src[:, i * LANE:(i + 1) * LANE]


def fold(src, i):
    s = [src[i, pl.ds(q, 8, stride=8), :] for q in range(8)]
    return ((s[0] + s[1]) + (s[2] + s[3])) + ((s[4] + s[5]) + (s[6] + s[7]))


def fwd_kernel(dt_ref, dr_ref, b_ref, c_ref, a_ref, y_ref, hs_ref, part, dts, drs, hst):
    cg = dt_ref.shape[1]
    tiles = cg // LANE
    tc = dt_ref.shape[0]

    @pl.when(pl.program_id(1) == 0)
    def _():
        hst[...] = jnp.zeros_like(hst)

    hs_ref[0] = hst[...]
    stage(dt_ref, dts)
    stage(dr_ref, drs)

    def group(g, carry):
        t0 = pl.multiple_of(g * 8, 8)
        hs = list(carry)
        for k in range(8):
            bt = b_ref[t0 + k]
            ct = c_ref[t0 + k]
            for i in range(tiles):
                ln = slice(i * LANE, (i + 1) * LANE)
                d = bcast(dts, i, t0 + k)
                u = bcast(drs, i, t0 + k)
                a = jnp.exp2(d * a_ref[:, ln])
                h = a * hs[i] + bt * u
                hs[i] = h
                p = ct * h
                part[i, k * 8:(k + 1) * 8, :] = p[:8] + p[8:]
        for i in range(tiles):
            ln = slice(i * LANE, (i + 1) * LANE)
            y_ref[pl.ds(t0, 8), ln] = fold(part, i)
        return tuple(hs)

    init = tuple(hst[:, i * LANE:(i + 1) * LANE] for i in range(tiles))
    out = lax.fori_loop(0, tc // 8, group, init)
    for i in range(tiles):
        hst[:, i * LANE:(i + 1) * LANE] = out[i]


def scan_forward(dt, dr, bx, cx, a2, tc=TC, cg=CGF):
    t, c = dt.shape
    nt, nc = t // tc, c // cg
    return pl.pallas_call(
        fwd_kernel,
        grid=(nc, nt),
        in_specs=[
            pl.BlockSpec((tc, cg), lambda j, i: (i, j)),
            pl.BlockSpec((tc, cg), lambda j, i: (i, j)),
            pl.BlockSpec((tc, NS, LANE), lambda j, i: (i, 0, 0)),
            pl.BlockSpec((tc, NS, LANE), lambda j, i: (i, 0, 0)),
            pl.BlockSpec((NS, cg), lambda j, i: (0, j)),
        ],
        out_specs=[
            pl.BlockSpec((tc, cg), lambda j, i: (i, j)),
            pl.BlockSpec((1, NS, cg), lambda j, i: (i, 0, j)),
        ],
        out_shape=[
            jax.ShapeDtypeStruct((t, c), jnp.float32),
            jax.ShapeDtypeStruct((nt, NS, c), jnp.float32),
        ],
        scratch_shapes=[pltpu.VMEM((cg // LANE, 64, LANE), jnp.float32)] + [pltpu.VMEM((cg // LANE, tc, LANE), jnp.float32)] * 2 + [pltpu.VMEM((NS, cg), jnp.float32)],
        name="scan_forward",
    )(dt, dr, bx, cx, a2)


def bwd_kernel(dp, steps, dt_ref, dr_ref, dy_ref, b_ref, c_ref, a_ref, hs_ref, og_ref, gg_ref,
               za_ref, gb_ref, dbt_ref, rate_ref, os_ref, gs_ref,
               db_ref, dc_ref, asc, hsc, pz, pg, dts, drs, dys, gst, rst, ores, gres, *comm):
    red = Reducer(dp, (og_ref, gg_ref), (ores, gres), comm, ROWS_B, SLACK_B)
    step = pl.program_id(0) * pl.num_programs(1) + pl.program_id(1)
    for n in range(red.ticks()):
        @pl.when(step == (n * (steps - 1)) // (red.ticks() - 1))
        def _(n=n):
            if n == 0:
                red.entry()
            red.tick(n)

    @pl.when(step == pl.num_programs(0) * pl.num_programs(1) - 1)
    def _():
        red.finish()
        os_ref[...] = ores[...]
        gs_ref[...] = gres[...]

    cg = dt_ref.shape[1]
    tiles = cg // LANE
    tc = dt_ref.shape[0]
    j = pl.program_id(0)
    i_t = pl.program_id(1)
    nt = pl.num_programs(1)

    @pl.when(i_t == 0)
    def _():
        gst[...] = jnp.zeros_like(gst)
        rst[...] = jnp.zeros_like(rst)

    stage(dt_ref, dts)
    stage(dr_ref, drs)
    stage(dy_ref, dys)
    lanes = [slice(i * LANE, (i + 1) * LANE) for i in range(tiles)]

    def fgroup(g, carry):
        t0 = pl.multiple_of(g * 8, 8)
        hs = list(carry)
        for k in range(8):
            bt = b_ref[t0 + k]
            for i in range(tiles):
                ln = lanes[i]
                d = bcast(dts, i, t0 + k)
                u = bcast(drs, i, t0 + k)
                a = jnp.exp2(d * a_ref[:, ln])
                asc[t0 + k, :, ln] = a
                hsc[t0 + k, :, ln] = hs[i]
                hs[i] = a * hs[i] + bt * u
        return tuple(hs)

    out = lax.fori_loop(0, tc // 8, fgroup, tuple(hs_ref[0, :, ln] for ln in lanes))
    for i in range(tiles):
        hsc[tc, :, lanes[i]] = out[i]

    base = pl.multiple_of((nt - 1 - i_t) * tc, tc)
    first = j == 0

    def bgroup(gi, carry):
        g = tc // 8 - 1 - gi
        t0 = pl.multiple_of(g * 8, 8)
        gs = list(carry[0])
        rs = list(carry[1])
        for k in range(7, -1, -1):
            bt = b_ref[t0 + k]
            ct = c_ref[t0 + k]
            accb = None
            for i in range(tiles):
                ln = lanes[i]
                d = bcast(dts, i, t0 + k)
                u = bcast(drs, i, t0 + k)
                w = bcast(dys, i, t0 + k)
                hnow = hsc[t0 + k + 1, :, ln]
                hprev = hsc[t0 + k, :, ln]
                a = asc[t0 + k, :, ln]
                gg = ct * w + gs[i]
                ga = gg * a
                z = ga * hprev
                rs[i] = rs[i] + z * d
                gs[i] = ga
                pa = z * a_ref[:, ln]
                pz[i, k * 8:(k + 1) * 8, :] = pa[:8] + pa[8:]
                pb = gg * bt
                pg[i, k * 8:(k + 1) * 8, :] = pb[:8] + pb[8:]
                vb = gg * u
                vc = w * hnow
                accb = vb if accb is None else accb + vb
                accc = vc if i == 0 else accc + vc
            row = base + t0 + k

            @pl.when(first)
            def _():
                db_ref[row] = accb
                dc_ref[row] = accc

            @pl.when(jnp.logical_not(first))
            def _():
                db_ref[row] = db_ref[row] + accb
                dc_ref[row] = dc_ref[row] + accc
        for i in range(tiles):
            ln = lanes[i]
            za_ref[pl.ds(t0, 8), ln] = fold(pz, i)
            gb_ref[pl.ds(t0, 8), ln] = fold(pg, i)
        return tuple(gs), tuple(rs)

    gs, rs = lax.fori_loop(0, tc // 8, bgroup, (tuple(gst[:, ln] for ln in lanes), tuple(rst[:, ln] for ln in lanes)))
    for i in range(tiles):
        gst[:, lanes[i]] = gs[i]
        rst[:, lanes[i]] = rs[i]

    @pl.when(i_t == nt - 1)
    def _():
        rate_ref[...] = rst[...]

    @pl.when(j == pl.num_programs(0) - 1)
    def _():
        block = pl.ds(pl.multiple_of((base // LANE) * LANE, LANE), LANE)
        lane = lax.broadcasted_iota(jnp.int32, (NS, LANE), 1)
        at = base % LANE

        def put(k, accs):
            row = base + k
            hit = lane == at + k
            return (jnp.where(hit, jnp.sum(db_ref[row], axis=-1, keepdims=True), accs[0]),
                    jnp.where(hit, jnp.sum(dc_ref[row], axis=-1, keepdims=True), accs[1]))

        got = lax.fori_loop(0, tc, put, (dbt_ref[:NS, block], dbt_ref[NS:, block]), unroll=8)
        dbt_ref[:NS, block] = got[0]
        dbt_ref[NS:, block] = got[1]


def scan_backward(dp, dt, dr, dy, bx, cx, a2, hs, og, gg, tc=TC, cg=CGB):
    t, c = dt.shape
    nt, nc = t // tc, c // cg
    row = pl.BlockSpec((tc, cg), lambda j, i: (nt - 1 - i, j))
    bc = pl.BlockSpec((tc, NS, LANE), lambda j, i: (nt - 1 - i, 0, 0))
    once = lambda s: pl.BlockSpec(s, lambda j, i: (0,) * len(s), pipeline_mode=pl.Buffered(1))
    og = og.reshape((2, 2) + og.shape[1:])
    gg = gg.reshape((2, 2) + gg.shape[1:])
    parts = [og.shape[2:], gg.shape[2:]]
    return pl.pallas_call(
        functools.partial(bwd_kernel, dp, nc * nt),
        grid=(nc, nt),
        in_specs=[row, row, row, bc, bc, pl.BlockSpec((NS, cg), lambda j, i: (0, j)),
                  pl.BlockSpec((1, NS, cg), lambda j, i: (nt - 1 - i, 0, j)), once(og.shape), once(gg.shape)],
        out_specs=[row, row, once((2 * NS, t)), pl.BlockSpec((NS, cg), lambda j, i: (0, j)), once(parts[0]), once(parts[1])],
        out_shape=[
            jax.ShapeDtypeStruct((t, c), jnp.float32),
            jax.ShapeDtypeStruct((t, c), jnp.float32),
            jax.ShapeDtypeStruct((2 * NS, t), jnp.float32),
            jax.ShapeDtypeStruct((NS, c), jnp.float32),
            jax.ShapeDtypeStruct(parts[0], jnp.bfloat16),
            jax.ShapeDtypeStruct(parts[1], jnp.bfloat16),
        ],
        scratch_shapes=[
            pltpu.VMEM((t, NS, LANE), jnp.float32), pltpu.VMEM((t, NS, LANE), jnp.float32),
            pltpu.VMEM((tc, NS, cg), jnp.float32), pltpu.VMEM((tc + 1, NS, cg), jnp.float32),
            pltpu.VMEM((cg // LANE, 64, LANE), jnp.float32), pltpu.VMEM((cg // LANE, 64, LANE), jnp.float32),
            pltpu.VMEM((cg // LANE, tc, LANE), jnp.float32), pltpu.VMEM((cg // LANE, tc, LANE), jnp.float32), pltpu.VMEM((cg // LANE, tc, LANE), jnp.float32),
            pltpu.VMEM((NS, cg), jnp.float32), pltpu.VMEM((NS, cg), jnp.float32),
            pltpu.VMEM(parts[0], jnp.bfloat16), pltpu.VMEM(parts[1], jnp.bfloat16),
        ] + reducer_scratch(dp, parts, ROWS_B),
        compiler_params=pltpu.CompilerParams(vmem_limit_bytes=60 << 20, collective_id=2, has_side_effects=True),
        name="scan_backward",
    )(dt, dr, dy, bx, cx, a2, hs, og, gg)


def pack_small(gain, conv_w, conv_b, xproj, dt_w, dt_b, alog, skip):
    width = conv_b.shape[-1]
    gain_row = jnp.pad(gain[None], ((0, 0), (0, width - gain.shape[0])))
    return jnp.concatenate(
        [xproj.T, dt_w, alog, conv_w, conv_b[None], dt_b[None], skip[None], gain_row], axis=0
    )


def body(
    tokens,
    cluster_lengths,
    norm_gain,
    in_weight,
    conv_weight,
    conv_bias,
    xproj_weight,
    dt_weight,
    dt_bias,
    a_log,
    skip_gain,
    out_weight,
    cotangent,
):
    low = jnp.bfloat16
    gain_shard = norm_gain.shape[0]
    width = conv_bias.shape[0]
    packed = pack_small(norm_gain, conv_weight, conv_bias, xproj_weight, dt_weight, dt_bias, a_log, skip_gain)
    packed = jnp.pad(packed, ((0, -packed.shape[0] % 32), (0, 0)))
    shards = lax.axis_size("fsdp")
    xw, rank, state = xproj_weight.shape[1], dt_weight.shape[0], a_log.shape[0]
    inner_width = shards * width
    length = tokens.shape[0]
    tap_valid, keep_mask = cluster_masks(cluster_lengths)
    tapb = jnp.broadcast_to(tap_valid.T[1:, :, None], (KCONV - 1, length, LANE))
    keepb = jnp.broadcast_to(keep_mask[:, None], (length, LANE))
    (in_all, out_all, small, normed_low, inner_in, gate_in, conv_out, dt_pre, step_far, drive, bx, cx, dt_rounded) = front(
        tokens, tapb, keepb, packed, in_weight, out_weight, (xw, rank, state, gain_shard, width)
    )
    out_full = out_all.reshape(-1, out_weight.shape[1])
    rows = jnp.moveaxis(small, 0, 1).reshape(small.shape[1], inner_width)
    at = xw + rank
    decay_rate = -jnp.exp(rows[at : at + state].astype(jnp.float32))
    at += state
    at += KCONV
    skip_value = rows[at + 2].astype(jnp.float32)
    inputs_full = tokens.astype(jnp.float32)
    conv_act = silu_of(conv_out)
    rate2 = decay_rate * LOG2E
    scanned, starts = scan_forward(step_far, drive, bx, cx, rate2)
    with_skip = scanned + skip_value * conv_act
    gate_act = silu_of(gate_in)
    gated_low = (with_skip * gate_act).astype(low)
    result = inputs_full + matmul(gated_low, out_full)
    output = result.astype(low)
    out_grad = left_inner(gated_low, cotangent)
    gated_grad = right_inner(cotangent, out_full)
    skip_part = gated_grad * gate_act
    gate_grad = gated_grad * with_skip * silu_slope(gate_in)
    gate_low = gate_grad.astype(low)
    gate_in_grad = left_inner(normed_low, gate_low)
    dp = lax.axis_size("dp")
    za, gb, dbt, rate_grad, out_share, gate_share = scan_backward(
        dp,
        step_far,
        drive,
        skip_part,
        bx,
        cx,
        rate2,
        starts,
        out_grad.astype(low).reshape(shards, -1, out_grad.shape[1]),
        gate_in_grad.astype(low).reshape(shards, -1, inner_width),
    )
    inner_share, small_share, input_grad = back(
        dp, (xw, rank, state, gain_shard, width), za, gb, dt_pre, skip_part, conv_out, inner_in, in_all, gate_low,
        normed_low.T, tokens, cotangent, small, dt_rounded.T, dbt, rate_grad * decay_rate, tapb,
    )
    out_share, gate_share, inner_share, small_share = (
        v.astype(jnp.float32) for v in (out_share, gate_share, inner_share, small_share)
    )
    at = xw + rank + state
    return (
        output,
        input_grad,
        small_share[at + KCONV + 3, :gain_shard],
        jnp.concatenate([inner_share, gate_share], axis=1),
        small_share[at : at + KCONV],
        small_share[at + KCONV],
        small_share[:xw].T,
        small_share[xw : xw + rank],
        small_share[at + KCONV + 1],
        small_share[xw + rank : at],
        small_share[at + KCONV + 2],
        out_share,
    )


def solution(mesh):
    in_specs = (
        P(("dp", "fsdp"), None),
        P(("dp", "fsdp"), None),
        P("fsdp"),
        P("fsdp", None),
        P(None, "fsdp"),
        P("fsdp"),
        P("fsdp", None),
        P(None, "fsdp"),
        P("fsdp"),
        P(None, "fsdp"),
        P("fsdp"),
        P("fsdp", None),
        P(("dp", "fsdp"), None),
    )
    out_specs = (
        P(("dp", "fsdp"), None),
        P(("dp", "fsdp"), None),
        P("fsdp"),
        P("fsdp", None),
        P(None, "fsdp"),
        P("fsdp"),
        P("fsdp", None),
        P(None, "fsdp"),
        P("fsdp"),
        P(None, "fsdp"),
        P("fsdp"),
        P("fsdp", None),
    )
    return jax.shard_map(body, mesh=mesh, in_specs=in_specs, out_specs=out_specs, check_vma=False)
```

```python
import functools

import jax
import jax.numpy as jnp
import numpy as np
from jax import lax
from jax.experimental import pallas as pl
from jax.experimental.pallas import tpu as pltpu
from jax.sharding import PartitionSpec as P

KCONV = 4
LENGTH = 512
LOG2E = float(np.log2(np.e))
LN2 = float(np.log(2.0))
FAR = 1e30


epsilon = 1e-05


def matmul(former, latter):
    return jnp.dot(former, latter, preferred_element_type=jnp.float32)


def left_inner(former, latter):
    return lax.dot_general(
        former, latter, (((0,), (0,)), ((), ())), preferred_element_type=jnp.float32
    )


def right_inner(former, latter):
    return lax.dot_general(
        former, latter, (((1,), (1,)), ((), ())), preferred_element_type=jnp.float32
    )


def silu_of(values):
    return values * jax.nn.sigmoid(values)


def silu_slope(values):
    logistic = jax.nn.sigmoid(values)
    return logistic * (1.0 + values * (1.0 - logistic))

MESH = pl.DeviceIdType.MESH
COLS = 1024
ROWS = 32
SLACK = 3
ROWS_B = 64
SLACK_B = 2
STRIDE_B = 1


class Reducer:

    def __init__(self, dp, sources, targets, scratch, rows=ROWS, slack=SLACK, cols=COLS):
        self.slack = slack
        self.nz = dp // 2
        self.sources, self.targets = sources, targets
        (self.rc, self.ry, self.rx, self.rz, self.s_one, self.r_one, self.s_rs, self.r_rs, self.s_ag, self.r_ag) = scratch
        self.me_dp, self.me_f = lax.axis_index("dp"), lax.axis_index("fsdp")
        self.fh, self.fl = self.me_f // 2, self.me_f % 2
        self.z, self.x = self.me_dp // 2, self.me_dp % 2
        self.pieces_c, self.rows = split_of(dp, rows)
        self.pieces_r = self.nz // self.pieces_c
        self.chunks = chunk_list([t.shape for t in targets], self.rows, cols)
        self.core = (self.me_dp, self.fh * 2 + (1 - self.fl))
        self.other = (self.me_dp, (1 - self.fh) * 2 + self.fl)
        self.pair = (self.z * 2 + (1 - self.x), self.me_f)

    def peer(self, o):
        return lax.rem(self.z + o, self.nz)

    def entry(self):
        barrier = pltpu.get_barrier_semaphore()
        ids = [self.core, self.other, self.pair] + [(self.peer(o) * 2 + self.x, self.me_f) for o in range(1, self.nz)]
        for d in ids:
            pl.semaphore_signal(barrier, inc=1, device_id=d, device_id_type=MESH)
        pl.semaphore_wait(barrier, len(ids))

    def copy(self, src, dst, send, recv, device):
        return pltpu.make_async_remote_copy(src_ref=src, dst_ref=dst, send_sem=send, recv_sem=recv, device_id=device, device_id_type=MESH)

    def copies(self, stage, k):
        a, r0, c0, w = self.chunks[k]
        r, hr = self.rows, self.rows // 2
        if stage == 0:
            src = self.sources[a].at[:, 1 - self.fl, r0:r0 + r, c0:c0 + w]
            return [self.copy(src, self.rc.at[k, :, :, :w], self.s_one.at[0, k], self.r_one.at[0, k], self.core)]
        if stage == 1:
            return [self.copy(self.rc.at[k, 1 - self.fh, :, :w], self.ry.at[k, :, :w], self.s_one.at[1, k], self.r_one.at[1, k], self.other)]
        if stage == 2:
            src = self.ry.at[k, pl.ds(pl.multiple_of((1 - self.x) * hr, hr), hr), :w]
            return [self.copy(src, self.rx.at[k, :, :w], self.s_one.at[2, k], self.r_one.at[2, k], self.pair)]
        out = []
        if stage == 5:
            rows = pl.ds(pl.multiple_of(r0 + self.x * hr, hr), hr)
            t = self.targets[a].at[rows, c0:c0 + w]
            return [self.copy(t, t, self.s_one.at[3, k], self.r_one.at[3, k], self.pair)]
        for o in range(1, self.nz):
            j = self.peer(o)
            device = (j * 2 + self.x, self.me_f)
            if stage == 3:
                pr, pc = self.place(j, w)
                out.append(self.copy(self.rx.at[k, pr, pc], self.rz.at[k, o - 1, :, :w // self.pieces_c], self.s_rs.at[k, o - 1], self.r_rs.at[k, o - 1], device))
            else:
                t = self.own(k)
                out.append(self.copy(t, t, self.s_ag.at[k, o - 1], self.r_ag.at[k, o - 1], device))
        return out

    def place(self, j, w, r0=0, c0=0):
        pr, pw = self.rows // 2 // self.pieces_r, w // self.pieces_c
        return (pl.ds(pl.multiple_of(r0 + (j // self.pieces_c) * pr, 16), pr), pl.ds(pl.multiple_of(c0 + lax.rem(j, self.pieces_c) * pw, 128), pw))

    def own(self, k):
        a, r0, c0, w = self.chunks[k]
        pr, pc = self.place(self.z, w, r0 + self.x * (self.rows // 2), c0)
        return self.targets[a].at[pr, pc]

    def absorb(self, stage, k):
        a, r0, c0, w = self.chunks[k]
        r, hr = self.rows, self.rows // 2
        for c in self.copies(stage, k):
            c.wait_recv()
        if stage == 0:
            for h in range(2):
                self.rc[k, h, :, :w] = self.rc[k, h, :, :w] + self.sources[a][h, self.fl, r0:r0 + r, c0:c0 + w]
        elif stage == 1:
            self.ry[k, :, :w] = self.ry[k, :, :w] + self.rc[k, self.fh, :, :w]
        elif stage == 2:
            mine = self.ry[k, pl.ds(pl.multiple_of(self.x * hr, hr), hr), :w]
            self.rx[k, :, :w] = self.rx[k, :, :w] + mine
        elif stage == 3:
            pr, pc = self.place(self.z, w)
            total = self.rx[k, pr, pc].astype(jnp.float32)
            for o in range(1, self.nz):
                total = total + self.rz[k, o - 1, :, :w // self.pieces_c].astype(jnp.float32)
            self.own(k)[...] = total.astype(jnp.bfloat16)

    def ticks(self):
        return len(self.chunks) + 6 * self.slack

    def tick(self, n):
        live = [(s, n - self.slack * s) for s in range(7) if 0 <= n - self.slack * s < len(self.chunks)]
        for s, k in reversed(live):
            if s > 0:
                self.absorb(s - 1, k)
        for s, k in reversed(live):
            if s < 6:
                for c in self.copies(s, k):
                    c.start()

    def finish(self):
        for k in range(len(self.chunks)):
            for s in range(6):
                for c in self.copies(s, k):
                    c.wait_send()


def split_of(dp, rows=ROWS):
    nz = dp // 2
    pieces_c = min(nz, COLS // 128, 4)
    return pieces_c, max(rows, 32 * (nz // pieces_c))


def chunk_list(shapes, rows, cols=COLS):
    out = []
    for a, (r, c) in enumerate(shapes):
        w = min(c, cols)
        for c0 in range(0, c, w):
            for r0 in range(0, r, rows):
                out.append((a, r0, c0, w))
    return out


def reducer_scratch(dp, shapes, rows=ROWS, cols=COLS):
    nz = dp // 2
    pieces_c, rows = split_of(dp, rows)
    n = len(chunk_list(shapes, rows, cols))
    low = jnp.bfloat16
    return [
        pltpu.VMEM((n, 2, rows, cols), low),
        pltpu.VMEM((n, rows, cols), low),
        pltpu.VMEM((n, rows // 2, cols), low),
        pltpu.VMEM((n, nz - 1, rows // 2 // (nz // pieces_c), cols // pieces_c), low),
        pltpu.SemaphoreType.DMA((4, n)),
        pltpu.SemaphoreType.DMA((4, n)),
        pltpu.SemaphoreType.DMA((n, nz - 1)),
        pltpu.SemaphoreType.DMA((n, nz - 1)),
        pltpu.SemaphoreType.DMA((n, nz - 1)),
        pltpu.SemaphoreType.DMA((n, nz - 1)),
    ]


PARTS = 4


class Spread:

    def __init__(self, shard, full, s_one, r_one, s_part, r_part, parts):
        dp, f = lax.axis_index("dp"), lax.axis_index("fsdp")
        fh, fl = f // 2, f % 2
        self.f, self.x = f, dp % 2
        self.far = (1 - fh) * 2 + fl
        self.core = (dp, fh * 2 + (1 - fl))
        self.other = (dp, self.far)
        self.pair = ((dp // 2) * 2 + (1 - self.x), f)
        self.shard, self.full, self.parts = shard, full, parts
        self.s_one, self.r_one, self.s_part, self.r_part = s_one, r_one, s_part, r_part
        self.half = shard.shape[0] // 2
        self.rows = self.half // parts

    def span(self, half, i):
        return pl.ds(pl.multiple_of(half * self.half + i * self.rows, self.rows), self.rows)

    def send(self, src, dst, s, r, device):
        return pltpu.make_async_remote_copy(src_ref=src, dst_ref=dst, send_sem=s, recv_sem=r, device_id=device, device_id_type=pl.DeviceIdType.MESH)

    def whole(self):
        return self.send(self.shard, self.full.at[self.f], self.s_one, self.r_one, self.core)

    def across(self, i):
        rows = self.span(self.x, i)
        return self.send(self.shard.at[rows], self.full.at[self.f, rows], self.s_part.at[0, i], self.r_part.at[0, i], self.other)

    def onward(self, kind, i):
        rows = self.span(self.x if kind < 3 else 1 - self.x, i)
        ref = self.full.at[self.far, rows]
        return self.send(ref, ref, self.s_part.at[kind, i], self.r_part.at[kind, i], self.pair if kind == 1 else self.core)

    def begin(self):
        self.whole().start()
        for i in range(self.parts):
            self.across(i).start()

    def pump(self, i):
        self.across(i).wait_recv()
        self.onward(1, i).start()
        self.onward(2, i).start()

    def pump_pair(self, i):
        self.onward(1, i).wait_recv()
        self.onward(3, i).start()

    def land(self):
        for i in range(self.parts):
            self.onward(2, i).wait_recv()
            self.onward(3, i).wait_recv()

    def finish(self):
        self.whole().wait_send()
        for i in range(self.parts):
            self.across(i).wait_send()
            for kind in (1, 2, 3):
                self.onward(kind, i).wait_send()


def spread_sems(parts):
    return [pltpu.SemaphoreType.DMA, pltpu.SemaphoreType.DMA, pltpu.SemaphoreType.DMA((4, parts)), pltpu.SemaphoreType.DMA((4, parts))]


def enter_square():
    dp, f = lax.axis_index("dp"), lax.axis_index("fsdp")
    fh, fl = f // 2, f % 2
    barrier = pltpu.get_barrier_semaphore()
    for d in ((dp, fh * 2 + (1 - fl)), (dp, (1 - fh) * 2 + fl), ((dp // 2) * 2 + (1 - dp % 2), f)):
        pl.semaphore_signal(barrier, inc=1, device_id=d, device_id_type=pl.DeviceIdType.MESH)
    pl.semaphore_wait(barrier, 3)


def nt(a, b):
    return lax.dot_general(a, b, (((1,), (1,)), ((), ())), preferred_element_type=jnp.float32)


def front_kernel(dims, len_ref, tok_ref, sml_ref, inw_ref,
                 in_out, sml_out, norm_out, inner_out, conv_out, pre_out, far_out, drive_out, bx_out, cx_out, dtr_out, tap_ref,
                 in_vm, norm_vm, inner, conv, pre, far, drive, act, bx, cx, keep_ref, osem,
                 a0, a1, a2, a3, b0, b1, b2, b3):
    xw, rank, state, gain_w, width = dims
    t = tok_ref.shape[0]
    low = jnp.bfloat16
    f = lax.axis_index("fsdp")
    fh = f // 2
    outs = []

    def put(src, dst):
        c = pltpu.make_async_copy(src, dst, osem.at[len(outs)])
        c.start()
        outs.append(c)

    enter_square()
    sm = Spread(sml_ref, sml_out, a0, a1, a2, a3, 1)
    di = inner.shape[1]
    wi = Spread(inw_ref.at[:, :di], in_vm, b0, b1, b2, b3, PARTS)
    own_i = pltpu.make_async_copy(inw_ref.at[:, :di], in_vm.at[f], osem.at[40])
    sm.begin()
    wi.begin()
    own_i.start()
    sml_out[f] = sml_ref[...]
    spot = lax.broadcasted_iota(jnp.int32, keep_ref.shape, 0)
    start = jnp.zeros_like(spot)
    run = 0
    for c in range(len_ref.shape[1] - 1):
        run = run + len_ref[0, c]
        start = jnp.where(spot >= run, run, start)
    keep_ref[...] = (spot > start).astype(jnp.float32)
    for j in (1, 2, 3):
        tap_ref[j - 1] = (spot - j >= start).astype(jnp.float32)

    x = tok_ref[...].astype(jnp.float32)
    unit = (x * lax.rsqrt(jnp.mean(x * x, axis=-1, keepdims=True) + 1e-05))
    conv[:, :x.shape[1]] = unit

    sm.pump(0)
    sm.pump_pair(0)
    sm.whole().wait_recv()
    sm.land()
    at = xw + rank + state
    for s in range(4):
        g = sml_out[s, at + 7:at + 8, :gain_w].astype(jnp.float32)
        norm_vm[s // 2, :, (s % 2) * gain_w:(s % 2 + 1) * gain_w] = (conv[:, s * gain_w:(s + 1) * gain_w] * g).astype(low)
        norm_out[:, s * gain_w:(s + 1) * gain_w] = norm_vm[s // 2, :, (s % 2) * gain_w:(s % 2 + 1) * gain_w]

    own_i.wait()
    wi.whole().wait_recv()
    tile = 256

    def block(h, first, base, dst):
        def go(n, _):
            cols = pl.ds(pl.multiple_of(base + n * tile, tile), tile)
            here = pl.ds(pl.multiple_of(n * tile, tile), tile)
            acc = jnp.dot(norm_vm[h], jnp.concatenate([in_vm[2 * h, :, cols], in_vm[2 * h + 1, :, cols]], axis=0), preferred_element_type=jnp.float32)
            dst[:, here] = acc if first else dst[:, here] + acc
            return 0
        lax.fori_loop(0, dst.shape[1] // tile, go, 0)

    block(fh, True, 0, inner)
    for i in range(PARTS):
        wi.pump(i)
        if i > 0:
            wi.pump_pair(i - 1)
    wi.pump_pair(PARTS - 1)
    wi.land()
    for s in range(4):
        put(in_vm.at[s], in_out.at[s])
    block(1 - fh, False, 0, inner)
    put(inner, inner_out)

    per = width // 128

    for s in range(4):
        for q in range(per):
            ln = slice(s * width + q * 128, s * width + (q + 1) * 128)
            sl = slice(q * 128, (q + 1) * 128)
            v = inner[:, ln]
            w = [sml_out[s, at + k:at + k + 1, sl].astype(jnp.float32) for k in range(4)]
            acc = sml_out[s, at + 4:at + 5, sl].astype(jnp.float32) + w[3] * v
            for j in (1, 2, 3):
                acc = acc + w[3 - j] * (pltpu.roll(v, j, 0) * tap_ref[j - 1])
            conv[:, ln] = acc
            a = acc * jax.nn.sigmoid(acc)
            drive[:, ln] = a
            act[:, ln] = a.astype(low)
        put(conv.at[:, s * width:(s + 1) * width], conv_out.at[:, s * width:(s + 1) * width])

    pt = jnp.zeros((2 * state, t), jnp.float32)
    dr = jnp.zeros((t, rank), jnp.float32)
    for s in range(4):
        al = act[:, s * width:(s + 1) * width]
        pt = pt + nt(sml_out[s, rank:xw, :], al)
        dr = dr + nt(al, sml_out[s, :rank, :])
    dtr = dr.astype(low)
    dtr_out[...] = dtr
    for tb in range(t // 128):
        for l in range(128):
            col = jnp.broadcast_to(pt[:, tb * 128 + l:tb * 128 + l + 1], (2 * state, 128))
            bx[tb * 128 + l] = col[:state]
            cx[tb * 128 + l] = col[state:]
    put(bx, bx_out)
    put(cx, cx_out)
    for s in range(4):
        cs = slice(s * width, (s + 1) * width)
        p = jnp.dot(dtr, sml_out[s, xw:xw + rank, :], preferred_element_type=jnp.float32) + sml_out[s, at + 5:at + 6, :].astype(jnp.float32)
        pre[:, cs] = p
        put(pre.at[:, cs], pre_out.at[:, cs])
        for q in range(per):
            ln = slice(s * width + q * 128, s * width + (q + 1) * 128)
            v = pre[:, ln]
            st = jnp.maximum(v, 0.0) + jnp.log1p(jnp.exp(-jnp.abs(v)))
            drive[:, ln] = drive[:, ln] * st
            far[:, ln] = jnp.where(keep_ref[...] > 0, st, 1e30)
        put(far.at[:, cs], far_out.at[:, cs])
        put(drive.at[:, cs], drive_out.at[:, cs])
    for g in (sm, wi):
        g.finish()
    for c in outs:
        c.wait()


def front(lengths, tokens, packed, in_weight, dims):
    xw, rank, state, gain_w, width = dims
    t, d = tokens.shape
    di = 4 * width
    low, f32 = jnp.bfloat16, jnp.float32
    vm = pl.BlockSpec(memory_space=pltpu.VMEM)
    hb = pl.BlockSpec(memory_space=pl.ANY)
    sds = jax.ShapeDtypeStruct
    wide = sds((t, di), f32)
    lanes = sds((t, state, 128), f32)
    return pl.pallas_call(
        functools.partial(front_kernel, dims),
        in_specs=[pl.BlockSpec(memory_space=pltpu.SMEM), vm, vm, hb],
        out_specs=[hb, vm, vm, hb, hb, hb, hb, hb, hb, hb, vm, vm],
        out_shape=[sds((4, gain_w, di), low), sds((4,) + packed.shape, low), sds((t, d), low),
                   wide, wide, wide, wide, wide, lanes, lanes, sds((t, rank), low), sds((3, t, 128), f32)],
        scratch_shapes=[pltpu.VMEM((4, gain_w, di), low), pltpu.VMEM((2, t, d // 2), low)]
        + [pltpu.VMEM((t, di), f32)] * 5 + [pltpu.VMEM((t, di), low)] + [pltpu.VMEM((t, state, 128), f32)] * 2
        + [pltpu.VMEM((t, 128), f32), pltpu.SemaphoreType.DMA((42,))] + spread_sems(1) + spread_sems(PARTS),
        compiler_params=pltpu.CompilerParams(collective_id=3, has_side_effects=True, vmem_limit_bytes=63 << 20),
        name="front",
    )(lengths, tokens, packed, in_weight)


BACK_ROWS = 64
BACK_COLS = 512


def tn(a, b):
    return lax.dot_general(a, b, (((0,), (0,)), ((), ())), preferred_element_type=jnp.float32)


def sum8(v):
    return jnp.sum(v.reshape(v.shape[0] // 8, 8, v.shape[1]), axis=0)


def back_kernel(dp, dims, za_h, gb_h, pre_h, dys_h, conv_h, inner_h, ina_h, inb_h, gl_h, nt_h, gg_ref, tok_ref, cot_ref, sml_ref, dtrt_ref, dbt_ref, rate_ref, tap_ref,
                gsh_ref, ish_ref, ssh_ref, ig_ref,
                za, gb, pre, dys, conv, inner, ina, inb, gl, normt, prelow, actlow, pt, agv, misc, gainv, ng, isrc, ssrc, csem, *comm):
    xw, rank, state, gain_w, width = dims
    t = tok_ref.shape[0]
    low = jnp.bfloat16
    at = xw + rank + state
    per = width // 128

    def fetch(k, src, dst):
        c = pltpu.make_async_copy(src, dst, csem.at[k])
        c.start()
        return c

    def slab(s):
        cs = slice(s * width, (s + 1) * width)
        return [fetch(s * 8 + k, h.at[:, cs], v) for k, (h, v) in enumerate(((conv_h, conv.at[:, cs]), (gb_h, gb.at[s % 2]), (pre_h, pre.at[s % 2]), (dys_h, dys.at[:, cs]), (za_h, za.at[s % 2])))]

    waits = [slab(0), slab(1)]
    late = [fetch(32, inner_h, inner), fetch(33, nt_h, normt), fetch(34, ina_h, ina), fetch(35, gl_h, gl), fetch(36, inb_h, inb)]
    red = Reducer(dp, (gg_ref, isrc, ssrc), (gsh_ref, ish_ref, ssh_ref), comm, BACK_ROWS, SLACK, BACK_COLS)
    red.entry()
    misc[...] = jnp.zeros_like(misc)
    gates = len([c for c in red.chunks if c[0] == 0])
    small0 = len([c for c in red.chunks if c[0] < 2])
    done = 0
    rankt = jnp.zeros((rank, t), jnp.float32)
    for s in range(4):
        for c in waits[s]:
            c.wait()

        def tile(q, _, s=s):
            ln = pl.ds(pl.multiple_of(s * width + q * 128, 128), 128)
            lq = pl.ds(pl.multiple_of(q * 128, 128), 128)
            skip = sml_ref[s, at + 6:at + 7, lq].astype(jnp.float32)

            def rows(r, sums):
                rs = pl.ds(pl.multiple_of(r * 64, 64), 64)
                cv = conv[rs, ln]
                sg = jax.nn.sigmoid(cv)
                ac = cv * sg
                gv = gb[s % 2, rs, lq]
                pv = pre[s % 2, rs, lq]
                dy = dys[rs, ln]
                st = jnp.maximum(pv, 0.0) + jnp.log1p(jnp.exp(-jnp.abs(pv)))
                pg = (za[s % 2, rs, lq] * LN2 + gv * ac) * jax.nn.sigmoid(pv)
                prelow[rs, lq] = pg.astype(low)
                actlow[rs, ln] = ac.astype(low)
                dys[rs, ln] = dy * skip + gv * st
                conv[rs, ln] = sg * (1.0 + cv * (1.0 - sg))
                return sums[0] + sum8(pg), sums[1] + sum8(dy * ac)

            zero = jnp.zeros((8, 128), jnp.float32)
            bias, skips = lax.fori_loop(0, t // 64, rows, (zero, zero))
            misc[5:6, ln] = jnp.sum(bias, axis=0, keepdims=True)
            misc[6:7, ln] = jnp.sum(skips, axis=0, keepdims=True)
            return 0

        for q in range(per):
            tile(q, 0)
            if done < gates:
                red.tick(done)
                done += 1
        if s < 2:
            waits.append(slab(s + 2))
        p = prelow[...]
        ssrc[s // 2, s % 2, xw:xw + rank, :] = jnp.dot(dtrt_ref[...], p, preferred_element_type=jnp.float32).astype(low)
        rankt = rankt + nt(sml_ref[s, xw:xw + rank, :], p)
    pt[:rank] = rankt.astype(low)
    pt[rank:] = dbt_ref[...].astype(low)
    for c in late[:2]:
        c.wait()
    while done < gates:
        red.tick(done)
        done += 1
    for s in range(4):
        cs = slice(s * width, (s + 1) * width)
        agv[...] = tn(pt[...], sml_ref[s, :xw, :])
        ssrc[s // 2, s % 2, :xw, :] = jnp.dot(pt[...], actlow[:, cs], preferred_element_type=jnp.float32).astype(low)
        ssrc[s // 2, s % 2, xw + rank:at, :] = rate_ref[:, cs].astype(low)

        def tile2(q, _, s=s):
            ln = pl.ds(pl.multiple_of(s * width + q * 128, 128), 128)
            lq = pl.ds(pl.multiple_of(q * 128, 128), 128)
            cg = (agv[:, lq] + dys[:, ln]) * conv[:, ln]
            v = inner[:, ln]
            ig = sml_ref[s, at + 3:at + 4, lq].astype(jnp.float32) * cg
            misc[3:4, ln] = jnp.sum(sum8(cg * v), axis=0, keepdims=True)
            misc[4:5, ln] = jnp.sum(sum8(cg), axis=0, keepdims=True)
            for j in (1, 2, 3):
                m = cg * tap_ref[j - 1]
                misc[3 - j:4 - j, ln] = jnp.sum(sum8(m * pltpu.roll(v, j, 0)), axis=0, keepdims=True)
                ig = ig + sml_ref[s, at + 3 - j:at + 4 - j, lq].astype(jnp.float32) * pltpu.roll(m, t - j, 0)
            actlow[:, ln] = ig.astype(low)
            return 0

        for half in range(2):
            lax.fori_loop(half * (per // 2), (half + 1) * (per // 2), tile2, 0)
            while s > 0 and done < gates + ((small0 - gates) * (2 * s + half - 1)) // 8:
                red.tick(done)
                done += 1
        for k in range(4):
            rows = slice(k * gain_w, (k + 1) * gain_w)
            isrc[k // 2, k % 2, :, cs] = jnp.dot(normt[rows, :], actlow[:, cs], preferred_element_type=jnp.float32).astype(low)
    for c in late[2:]:
        c.wait()
    for blk in range(8):
        if done < small0:
            red.tick(done)
            done += 1
        src = gl if blk < 4 else actlow
        base = (blk % 4) * width
        wsrc = inb if blk < 4 else ina
        for k in range(4):
            rows = slice(k * gain_w, (k + 1) * gain_w)
            part = nt(src[:, base:base + width], wsrc[k, :, base:base + width])
            ng[:, rows] = part if blk == 0 else ng[:, rows] + part
    for k in range(4):
        gainv[0:1, k * gain_w:(k + 1) * gain_w] = sml_ref[k, at + 7:at + 8, :gain_w].astype(jnp.float32)

    def fin(r, acc):
        rs = pl.ds(pl.multiple_of(r * 32, 32), 32)
        x = tok_ref[rs, :].astype(jnp.float32)
        inv = lax.rsqrt(jnp.mean(x * x, axis=-1, keepdims=True) + 1e-05)
        u = x * inv
        d = ng[rs, :]
        e = d * gainv[0:1, :]
        ig_ref[rs, :] = cot_ref[rs, :].astype(jnp.float32) + inv * (e - u * jnp.mean(e * u, axis=-1, keepdims=True))
        return acc + sum8(d * u)

    gsum = lax.fori_loop(0, t // 32, fin, jnp.zeros((8, ng.shape[1]), jnp.float32))
    gsum = jnp.sum(gsum, axis=0, keepdims=True)
    for k in range(4):
        misc[7:8, k * width:k * width + gain_w] = gsum[:, k * gain_w:(k + 1) * gain_w]
    for k in range(4):
        ssrc[k // 2, k % 2, at:at + 16, :] = misc[:, k * width:(k + 1) * width].astype(low)
        if ssrc.shape[2] > at + 16:
            ssrc[k // 2, k % 2, at + 16:, :] = jnp.zeros((ssrc.shape[2] - at - 16, width), low)
    while done < red.ticks():
        red.tick(done)
        done += 1
    red.finish()


def back(dp, dims, za, gb, pre, dys, conv, inner, in_a, in_b, gate_low, normt, gg, tokens, cot, small, dtrt, dbt, rate, tapb):
    xw, rank, state, gain_w, width = dims
    t, d = tokens.shape
    di = 4 * width
    low, f32 = jnp.bfloat16, jnp.float32
    unit = split_of(dp, BACK_ROWS)[1]
    srows = -(-(xw + rank + state + 16) // unit) * unit
    shapes = [(gain_w, di), (gain_w, di), (srows, width)]
    vm = pl.BlockSpec(memory_space=pltpu.VMEM)
    hb = pl.BlockSpec(memory_space=pl.ANY)
    sds = jax.ShapeDtypeStruct
    return pl.pallas_call(
        functools.partial(back_kernel, dp, dims),
        in_specs=[hb] * 10 + [vm] * 8,
        out_specs=[vm] * 4,
        out_shape=[sds(shapes[0], low), sds(shapes[1], low), sds(shapes[2], low), sds((t, d), f32)],
        scratch_shapes=[pltpu.VMEM((2, t, width), f32)] * 3 + [pltpu.VMEM((t, di), f32)] * 3
        + [pltpu.VMEM(in_a.shape, low), pltpu.VMEM(in_b.shape, low), pltpu.VMEM((t, di), low), pltpu.VMEM((d, t), low), pltpu.VMEM((t, width), low), pltpu.VMEM((t, di), low),
           pltpu.VMEM((xw, t), low), pltpu.VMEM((t, width), f32), pltpu.VMEM((16, di), f32), pltpu.VMEM((8, d), f32), pltpu.VMEM((t, d), f32),
           pltpu.VMEM((2, 2) + shapes[1], low), pltpu.VMEM((2, 2) + shapes[2], low), pltpu.SemaphoreType.DMA((37,))]
        + reducer_scratch(dp, shapes, BACK_ROWS, BACK_COLS),
        compiler_params=pltpu.CompilerParams(collective_id=1, has_side_effects=True, vmem_limit_bytes=63 << 20),
        name="back",
    )(za, gb, pre, dys, conv, inner, in_a, in_b, gate_low, normt, gg.reshape((2, 2) + shapes[0]), tokens, cot, small, dtrt, dbt, rate, tapb)


def last_kernel(dims, i_ref, g_ref, o_ref, s_ref, in_ref, og_ref, gain_ref, cw_ref, cb_ref, xp_ref, dw_ref, db_ref, al_ref, sk_ref):
    xw, rank, state, gain_w, width = dims
    f32 = jnp.float32
    half = i_ref.shape[1]
    in_ref[:, :half] = i_ref[...].astype(f32)
    in_ref[:, half:] = g_ref[...].astype(f32)
    og_ref[...] = o_ref[...].astype(f32)
    at = xw + rank + state
    xp_ref[...] = s_ref[:xw, :].astype(f32).T
    dw_ref[...] = s_ref[xw:xw + rank, :].astype(f32)
    al_ref[...] = s_ref[xw + rank:at, :].astype(f32)
    tail = s_ref[at:at + 16, :].astype(f32)
    cw_ref[...] = tail[:4]
    cb_ref[...] = tail[4:5]
    db_ref[...] = tail[5:6]
    sk_ref[...] = tail[6:7]
    gain_ref[...] = tail[7:8, :gain_w]


def last(dims, ish, gsh, osh, ssh):
    xw, rank, state, gain_w, width = dims
    f32 = jnp.float32
    sds = jax.ShapeDtypeStruct
    vm = pl.BlockSpec(memory_space=pltpu.VMEM)
    return pl.pallas_call(
        functools.partial(last_kernel, dims),
        in_specs=[vm] * 4,
        out_specs=[vm] * 10,
        out_shape=[sds((ish.shape[0], 2 * ish.shape[1]), f32), sds(osh.shape, f32), sds((1, gain_w), f32), sds((4, width), f32), sds((1, width), f32),
                   sds((width, xw), f32), sds((rank, width), f32), sds((1, width), f32), sds((state, width), f32), sds((1, width), f32)],
        compiler_params=pltpu.CompilerParams(vmem_limit_bytes=63 << 20),
        name="last",
    )(ish, gsh, osh, ssh)


LANE = 128
NS = 16
TC = 64
CGF = 1024
CGB = 512


def bcast(ref, i, row):
    v = ref[i, pl.ds(row, 8, stride=0), :]
    return jnp.concatenate([v, v], axis=0)


def stage(src, dst):
    for i in range(dst.shape[0]):
        dst[i] = src[:, i * LANE:(i + 1) * LANE]


def fold(src, i):
    s = [src[i, pl.ds(q, 8, stride=8), :] for q in range(8)]
    return ((s[0] + s[1]) + (s[2] + s[3])) + ((s[4] + s[5]) + (s[6] + s[7]))


def fwd_kernel(dt_ref, dr_ref, b_ref, c_ref, a_ref, inw_ref, outw_ref, y_ref, hs_ref, inb_ref, all_ref,
               part, dts, drs, hst, bi, bo, lsem, b0, b1, b2, b3, c0, c1, c2, c3):
    step = pl.program_id(0) * pl.num_programs(1) + pl.program_id(1)
    di = inb_ref.shape[2]
    f = lax.axis_index("fsdp")
    wb = Spread(inw_ref.at[:, di:], inb_ref, b0, b1, b2, b3, PARTS)
    wo = Spread(outw_ref, all_ref, c0, c1, c2, c3, PARTS)
    into = [pltpu.make_async_copy(inw_ref.at[:, di:], bi, lsem.at[0]), pltpu.make_async_copy(outw_ref, bo, lsem.at[1])]
    away = [pltpu.make_async_copy(bi, inb_ref.at[f], lsem.at[2]), pltpu.make_async_copy(bo, all_ref.at[f], lsem.at[3])]

    @pl.when(step == 0)
    def _():
        enter_square()
        wb.begin()
        wo.begin()
        for c in into:
            c.start()

    @pl.when(step == 1)
    def _():
        for c in into:
            c.wait()
        for c in away:
            c.start()

    for i in range(2 * PARTS):
        @pl.when(step == PUMPS[i])
        def _(i=i):
            (wb if i < PARTS else wo).pump(i % PARTS)
            if i > 0:
                (wb if i - 1 < PARTS else wo).pump_pair((i - 1) % PARTS)

    @pl.when(step == pl.num_programs(0) * pl.num_programs(1) - 1)
    def _():
        wo.pump_pair(PARTS - 1)
        for w in (wb, wo):
            w.whole().wait_recv()
            w.land()
            w.finish()
        for c in away:
            c.wait()

    cg = dt_ref.shape[1]
    tiles = cg // LANE
    tc = dt_ref.shape[0]

    @pl.when(pl.program_id(1) == 0)
    def _():
        hst[...] = jnp.zeros_like(hst)

    stage(dt_ref, dts)
    stage(dr_ref, drs)

    def group(g, carry):
        t0 = pl.multiple_of(g * 8, 8)
        hs = list(carry)
        for k in range(8):
            bt = b_ref[t0 + k]
            ct = c_ref[t0 + k]
            for i in range(tiles):
                ln = slice(i * LANE, (i + 1) * LANE)
                d = bcast(dts, i, t0 + k)
                u = bcast(drs, i, t0 + k)
                a = jnp.exp2(d * a_ref[:, ln])
                hs_ref[0, t0 + k, :, ln] = hs[i]
                h = a * hs[i] + bt * u
                hs[i] = h
                p = ct * h
                part[i, k * 8:(k + 1) * 8, :] = p[:8] + p[8:]
        for i in range(tiles):
            ln = slice(i * LANE, (i + 1) * LANE)
            y_ref[pl.ds(t0, 8), ln] = fold(part, i)
        return tuple(hs)

    init = tuple(hst[:, i * LANE:(i + 1) * LANE] for i in range(tiles))
    out = lax.fori_loop(0, tc // 8, group, init, unroll=2)
    for i in range(tiles):
        hst[:, i * LANE:(i + 1) * LANE] = out[i]
        hs_ref[0, tc, :, i * LANE:(i + 1) * LANE] = out[i]


PUMPS = (2, 4, 6, 8, 10, 12, 13, 14)


def scan_forward(dt, dr, bx, cx, a2, in_weight, out_weight, tc=TC, cg=CGF):
    t, c = dt.shape
    nt, nc = t // tc, c // cg
    assert nt * nc > PUMPS[-1] + 1
    return pl.pallas_call(
        fwd_kernel,
        grid=(nc, nt),
        in_specs=[
            pl.BlockSpec((tc, cg), lambda j, i: (i, j)),
            pl.BlockSpec((tc, cg), lambda j, i: (i, j)),
            pl.BlockSpec((tc, NS, LANE), lambda j, i: (i, 0, 0)),
            pl.BlockSpec((tc, NS, LANE), lambda j, i: (i, 0, 0)),
            pl.BlockSpec((NS, cg), lambda j, i: (0, j)),
            pl.BlockSpec(memory_space=pl.ANY),
            pl.BlockSpec(memory_space=pl.ANY),
        ],
        out_specs=[
            pl.BlockSpec((tc, cg), lambda j, i: (i, j)),
            pl.BlockSpec((1, tc + 1, NS, cg), lambda j, i: (i, 0, 0, j)),
            pl.BlockSpec(memory_space=pl.ANY),
            pl.BlockSpec(memory_space=pl.ANY),
        ],
        out_shape=[
            jax.ShapeDtypeStruct((t, c), jnp.float32),
            jax.ShapeDtypeStruct((nt, tc + 1, NS, c), jnp.float32),
            jax.ShapeDtypeStruct((4, in_weight.shape[0], c), jnp.bfloat16),
            jax.ShapeDtypeStruct((4,) + out_weight.shape, jnp.bfloat16),
        ],
        scratch_shapes=[pltpu.VMEM((cg // LANE, 64, LANE), jnp.float32)] + [pltpu.VMEM((cg // LANE, tc, LANE), jnp.float32)] * 2 + [pltpu.VMEM((NS, cg), jnp.float32), pltpu.VMEM((in_weight.shape[0], c), jnp.bfloat16), pltpu.VMEM(out_weight.shape, jnp.bfloat16), pltpu.SemaphoreType.DMA((4,))] + spread_sems(PARTS) * 2,
        compiler_params=pltpu.CompilerParams(vmem_limit_bytes=63 << 20, collective_id=4, has_side_effects=True),
        name="scan_forward",
    )(dt, dr, bx, cx, a2, in_weight, out_weight)


def bwd_kernel(dp, steps, dt_ref, dr_ref, dy_ref, b_ref, c_ref, a_ref, hs_ref, og_ref,
               za_ref, gb_ref, dbt_ref, rate_ref, os_ref,
               db_ref, dc_ref, pz, pg, dts, drs, dys, gst, rst, ores, *comm):
    red = Reducer(dp, (og_ref,), (ores,), comm, ROWS_B, SLACK_B)
    step = pl.program_id(0) * pl.num_programs(1) + pl.program_id(1)
    def tree(lo, hi):
        if hi - lo == 1:
            @pl.when(step == lo * STRIDE_B)
            def _():
                if lo == 0:
                    red.entry()
                red.tick(lo)
            return
        mid = (lo + hi) // 2
        lax.cond(step < mid * STRIDE_B, lambda: tree(lo, mid), lambda: tree(mid, hi))

    assert (red.ticks() - 1) * STRIDE_B < steps
    tree(0, red.ticks())

    @pl.when(step == pl.num_programs(0) * pl.num_programs(1) - 1)
    def _():
        red.finish()
        os_ref[...] = ores[...]

    cg = dt_ref.shape[1]
    tiles = cg // LANE
    tc = dt_ref.shape[0]
    j = pl.program_id(0)
    i_t = pl.program_id(1)
    nt = pl.num_programs(1)

    @pl.when(i_t == 0)
    def _():
        gst[...] = jnp.zeros_like(gst)
        rst[...] = jnp.zeros_like(rst)

    @pl.when(step == 0)
    def _():
        db_ref[...] = jnp.zeros_like(db_ref)
        dc_ref[...] = jnp.zeros_like(dc_ref)

    stage(dt_ref, dts)
    stage(dr_ref, drs)
    stage(dy_ref, dys)
    lanes = [slice(i * LANE, (i + 1) * LANE) for i in range(tiles)]

    base = pl.multiple_of((nt - 1 - i_t) * tc, tc)

    def bgroup(gi, carry):
        g = tc // 8 - 1 - gi
        t0 = pl.multiple_of(g * 8, 8)
        gs = list(carry[0])
        rs = list(carry[1])
        for k in range(7, -1, -1):
            bt = b_ref[t0 + k]
            ct = c_ref[t0 + k]
            accb = None
            for i in range(tiles):
                ln = lanes[i]
                d = bcast(dts, i, t0 + k)
                u = bcast(drs, i, t0 + k)
                w = bcast(dys, i, t0 + k)
                hnow = hs_ref[0, t0 + k + 1, :, ln]
                hprev = hs_ref[0, t0 + k, :, ln]
                a = jnp.exp2(d * a_ref[:, ln])
                gg = ct * w + gs[i]
                ga = gg * a
                z = ga * hprev
                rs[i] = rs[i] + z * d
                gs[i] = ga
                pa = z * a_ref[:, ln]
                pz[i, k * 8:(k + 1) * 8, :] = pa[:8] + pa[8:]
                pb = gg * bt
                pg[i, k * 8:(k + 1) * 8, :] = pb[:8] + pb[8:]
                vb = gg * u
                vc = w * hnow
                accb = vb if accb is None else accb + vb
                accc = vc if i == 0 else accc + vc
            row = base + t0 + k

            db_ref[row] = db_ref[row] + accb
            dc_ref[row] = dc_ref[row] + accc
        for i in range(tiles):
            ln = lanes[i]
            za_ref[pl.ds(t0, 8), ln] = fold(pz, i)
            gb_ref[pl.ds(t0, 8), ln] = fold(pg, i)
        return tuple(gs), tuple(rs)

    gs, rs = lax.fori_loop(0, tc // 8, bgroup, (tuple(gst[:, ln] for ln in lanes), tuple(rst[:, ln] for ln in lanes)), unroll=2)
    for i in range(tiles):
        gst[:, lanes[i]] = gs[i]
        rst[:, lanes[i]] = rs[i]

    @pl.when(i_t == nt - 1)
    def _():
        rate_ref[...] = rst[...]

    @pl.when(j == pl.num_programs(0) - 1)
    def _():
        block = pl.ds(pl.multiple_of((base // LANE) * LANE, LANE), LANE)
        lane = lax.broadcasted_iota(jnp.int32, (NS, LANE), 1)
        at = base % LANE

        def put(k, accs):
            row = base + k
            hit = lane == at + k
            return (jnp.where(hit, jnp.sum(db_ref[row], axis=-1, keepdims=True), accs[0]),
                    jnp.where(hit, jnp.sum(dc_ref[row], axis=-1, keepdims=True), accs[1]))

        got = lax.fori_loop(0, tc, put, (dbt_ref[:NS, block], dbt_ref[NS:, block]), unroll=8)
        dbt_ref[:NS, block] = got[0]
        dbt_ref[NS:, block] = got[1]


def scan_backward(dp, dt, dr, dy, bx, cx, a2, hs, og, tc=TC, cg=CGB):
    t, c = dt.shape
    nt, nc = t // tc, c // cg
    row = pl.BlockSpec((tc, cg), lambda j, i: (nt - 1 - i, j))
    bc = pl.BlockSpec((tc, NS, LANE), lambda j, i: (nt - 1 - i, 0, 0))
    once = lambda s: pl.BlockSpec(s, lambda j, i: (0,) * len(s), pipeline_mode=pl.Buffered(1))
    og = og.reshape((2, 2) + og.shape[1:])
    parts = [og.shape[2:]]
    return pl.pallas_call(
        functools.partial(bwd_kernel, dp, nc * nt),
        grid=(nc, nt),
        in_specs=[row, row, row, bc, bc, pl.BlockSpec((NS, cg), lambda j, i: (0, j)),
                  pl.BlockSpec((1, tc + 1, NS, cg), lambda j, i: (nt - 1 - i, 0, 0, j)), once(og.shape)],
        out_specs=[row, row, once((2 * NS, t)), pl.BlockSpec((NS, cg), lambda j, i: (0, j)), once(parts[0])],
        out_shape=[
            jax.ShapeDtypeStruct((t, c), jnp.float32),
            jax.ShapeDtypeStruct((t, c), jnp.float32),
            jax.ShapeDtypeStruct((2 * NS, t), jnp.float32),
            jax.ShapeDtypeStruct((NS, c), jnp.float32),
            jax.ShapeDtypeStruct(parts[0], jnp.bfloat16),
        ],
        scratch_shapes=[
            pltpu.VMEM((t, NS, LANE), jnp.float32), pltpu.VMEM((t, NS, LANE), jnp.float32),
            pltpu.VMEM((cg // LANE, 64, LANE), jnp.float32), pltpu.VMEM((cg // LANE, 64, LANE), jnp.float32),
            pltpu.VMEM((cg // LANE, tc, LANE), jnp.float32), pltpu.VMEM((cg // LANE, tc, LANE), jnp.float32), pltpu.VMEM((cg // LANE, tc, LANE), jnp.float32),
            pltpu.VMEM((NS, cg), jnp.float32), pltpu.VMEM((NS, cg), jnp.float32),
            pltpu.VMEM(parts[0], jnp.bfloat16),
        ] + reducer_scratch(dp, parts, ROWS_B),
        compiler_params=pltpu.CompilerParams(vmem_limit_bytes=60 << 20, collective_id=2, has_side_effects=True),
        name="scan_backward",
    )(dt, dr, dy, bx, cx, a2, hs, og)


def pack_small(gain, conv_w, conv_b, xproj, dt_w, dt_b, alog, skip):
    width = conv_b.shape[-1]
    gain_row = jnp.pad(gain[None], ((0, 0), (0, width - gain.shape[0])))
    return jnp.concatenate(
        [xproj.T, dt_w, alog, conv_w, conv_b[None], dt_b[None], skip[None], gain_row], axis=0
    )


def body(
    tokens,
    cluster_lengths,
    norm_gain,
    in_weight,
    conv_weight,
    conv_bias,
    xproj_weight,
    dt_weight,
    dt_bias,
    a_log,
    skip_gain,
    out_weight,
    cotangent,
):
    low = jnp.bfloat16
    gain_shard = norm_gain.shape[0]
    width = conv_bias.shape[0]
    packed = pack_small(norm_gain, conv_weight, conv_bias, xproj_weight, dt_weight, dt_bias, a_log, skip_gain)
    packed = jnp.pad(packed, ((0, -packed.shape[0] % 32), (0, 0)))
    shards = lax.axis_size("fsdp")
    xw, rank, state = xproj_weight.shape[1], dt_weight.shape[0], a_log.shape[0]
    inner_width = shards * width
    (in_a, small, normed_low, inner_in, conv_out, dt_pre, step_far, drive, bx, cx, dt_rounded, tapb) = front(
        cluster_lengths, tokens, packed, in_weight, (xw, rank, state, gain_shard, width)
    )
    rows = jnp.moveaxis(small, 0, 1).reshape(small.shape[1], inner_width)
    at = xw + rank
    decay_rate = -jnp.exp(rows[at : at + state].astype(jnp.float32))
    at += state
    at += KCONV
    skip_value = rows[at + 2].astype(jnp.float32)
    inputs_full = tokens.astype(jnp.float32)
    conv_act = silu_of(conv_out)
    rate2 = decay_rate * LOG2E
    scanned, starts, in_b, out_all = scan_forward(step_far, drive, bx, cx, rate2, in_weight, out_weight)
    out_full = out_all.reshape(-1, out_weight.shape[1])
    gate_in = matmul(normed_low, in_b.reshape(-1, inner_width))
    with_skip = scanned + skip_value * conv_act
    gate_act = silu_of(gate_in)
    gated_low = (with_skip * gate_act).astype(low)
    result = inputs_full + matmul(gated_low, out_full)
    output = result.astype(low)
    out_grad = left_inner(gated_low, cotangent)
    gated_grad = right_inner(cotangent, out_full)
    skip_part = gated_grad * gate_act
    gate_grad = gated_grad * with_skip * silu_slope(gate_in)
    gate_low = gate_grad.astype(low)
    gate_in_grad = left_inner(normed_low, gate_low)
    dp = lax.axis_size("dp")
    za, gb, dbt, rate_grad, out_share = scan_backward(
        dp,
        step_far,
        drive,
        skip_part,
        bx,
        cx,
        rate2,
        starts,
        out_grad.astype(low).reshape(shards, -1, out_grad.shape[1]),
    )
    gate_share, inner_share, small_share, input_grad = back(
        dp, (xw, rank, state, gain_shard, width), za, gb, dt_pre, skip_part, conv_out, inner_in, in_a, in_b, gate_low,
        normed_low.T, gate_in_grad.astype(low), tokens, cotangent, small, dt_rounded.T, dbt, rate_grad * decay_rate, tapb,
    )
    in_grad, out_weight_grad, gain_g, conv_g, conv_b, xproj_g, dt_g, dt_b, alog_g, skip_g = last(
        (xw, rank, state, gain_shard, width), inner_share, gate_share, out_share, small_share
    )
    return (
        output, input_grad, gain_g[0], in_grad, conv_g, conv_b[0], xproj_g, dt_g, dt_b[0], alog_g, skip_g[0], out_weight_grad
    )


def solution(mesh):
    in_specs = (
        P(("dp", "fsdp"), None),
        P(("dp", "fsdp"), None),
        P("fsdp"),
        P("fsdp", None),
        P(None, "fsdp"),
        P("fsdp"),
        P("fsdp", None),
        P(None, "fsdp"),
        P("fsdp"),
        P(None, "fsdp"),
        P("fsdp"),
        P("fsdp", None),
        P(("dp", "fsdp"), None),
    )
    out_specs = (
        P(("dp", "fsdp"), None),
        P(("dp", "fsdp"), None),
        P("fsdp"),
        P("fsdp", None),
        P(None, "fsdp"),
        P("fsdp"),
        P("fsdp", None),
        P(None, "fsdp"),
        P("fsdp"),
        P(None, "fsdp"),
        P("fsdp"),
        P("fsdp", None),
    )
    return jax.shard_map(body, mesh=mesh, in_specs=in_specs, out_specs=out_specs, check_vma=False)
```

```python
import functools

import jax
import jax.numpy as jnp
import numpy as np
from jax import lax
from jax.experimental import pallas as pl
from jax.experimental.pallas import tpu as pltpu
from jax.sharding import PartitionSpec as P

KCONV = 4
LENGTH = 512
LOG2E = float(np.log2(np.e))
LN2 = float(np.log(2.0))
FAR = 1e30


epsilon = 1e-05


def matmul(former, latter):
    return jnp.dot(former, latter, preferred_element_type=jnp.float32)


def left_inner(former, latter):
    return lax.dot_general(
        former, latter, (((0,), (0,)), ((), ())), preferred_element_type=jnp.float32
    )


def right_inner(former, latter):
    return lax.dot_general(
        former, latter, (((1,), (1,)), ((), ())), preferred_element_type=jnp.float32
    )


def silu_of(values):
    return values * jax.nn.sigmoid(values)


def silu_slope(values):
    logistic = jax.nn.sigmoid(values)
    return logistic * (1.0 + values * (1.0 - logistic))

MESH = pl.DeviceIdType.MESH
COLS = 1024
ROWS = 32
SCAN_ROWS, SCAN_RATE, SCAN_FIRST, SCAN_DELAY = 32, 0.65, 1.0, 3.0


class Reducer:

    def __init__(self, dp, sources, targets, scratch, rows=ROWS, cols=COLS, cuts=None):
        self.nz = dp // 2
        self.sources, self.targets = sources, targets
        (self.rc, self.ry, self.rx, self.rz, self.s_one, self.r_one, self.s_rs, self.r_rs, self.s_ag, self.r_ag) = scratch
        self.me_dp, self.me_f = lax.axis_index("dp"), lax.axis_index("fsdp")
        self.fh, self.fl = self.me_f // 2, self.me_f % 2
        self.z, self.x = self.me_dp // 2, self.me_dp % 2
        self.pieces_c, self.rows = split_of(dp, rows)
        self.pieces_r = self.nz // self.pieces_c
        self.cuts = cuts or [0] * len(targets)
        self.chunks = chunk_list([t.shape for t in targets], self.rows, cols)
        self.core = (self.me_dp, self.fh * 2 + (1 - self.fl))
        self.other = (self.me_dp, (1 - self.fh) * 2 + self.fl)
        self.pair = (self.z * 2 + (1 - self.x), self.me_f)

    def peer(self, o):
        return lax.rem(self.z + o, self.nz)

    def entry(self):
        barrier = pltpu.get_barrier_semaphore()
        ids = [self.core, self.other, self.pair] + [(self.peer(o) * 2 + self.x, self.me_f) for o in range(1, self.nz)]
        for d in ids:
            pl.semaphore_signal(barrier, inc=1, device_id=d, device_id_type=MESH)
        pl.semaphore_wait(barrier, len(ids))

    def copy(self, src, dst, send, recv, device):
        return pltpu.make_async_remote_copy(src_ref=src, dst_ref=dst, send_sem=send, recv_sem=recv, device_id=device, device_id_type=MESH)

    def copies(self, stage, k):
        a, r0, c0, w = self.chunks[k]
        r, hr = self.rows, self.rows // 2
        if stage == 0:
            src = self.sources[a].at[:, 1 - self.fl, r0:r0 + r, self.cuts[a] + c0:self.cuts[a] + c0 + w]
            return [self.copy(src, self.rc.at[k, :, :, :w], self.s_one.at[0, k], self.r_one.at[0, k], self.core)]
        if stage == 1:
            return [self.copy(self.rc.at[k, 1 - self.fh, :, :w], self.ry.at[k, :, :w], self.s_one.at[1, k], self.r_one.at[1, k], self.other)]
        if stage == 2:
            src = self.ry.at[k, pl.ds(pl.multiple_of((1 - self.x) * hr, hr), hr), :w]
            return [self.copy(src, self.rx.at[k, :, :w], self.s_one.at[2, k], self.r_one.at[2, k], self.pair)]
        out = []
        if stage == 5:
            rows = pl.ds(pl.multiple_of(r0 + self.x * hr, hr), hr)
            t = self.targets[a].at[rows, c0:c0 + w]
            return [self.copy(t, t, self.s_one.at[3, k], self.r_one.at[3, k], self.pair)]
        for o in range(1, self.nz):
            j = self.peer(o)
            device = (j * 2 + self.x, self.me_f)
            if stage == 3:
                pr, pc = self.place(j, w)
                out.append(self.copy(self.rx.at[k, pr, pc], self.rz.at[k, o - 1, :, :w // self.pieces_c], self.s_rs.at[k, o - 1], self.r_rs.at[k, o - 1], device))
            else:
                t = self.own(k)
                out.append(self.copy(t, t, self.s_ag.at[k, o - 1], self.r_ag.at[k, o - 1], device))
        return out

    def place(self, j, w, r0=0, c0=0):
        pr, pw = self.rows // 2 // self.pieces_r, w // self.pieces_c
        return (pl.ds(pl.multiple_of(r0 + (j // self.pieces_c) * pr, 16), pr), pl.ds(pl.multiple_of(c0 + lax.rem(j, self.pieces_c) * pw, 128), pw))

    def own(self, k):
        a, r0, c0, w = self.chunks[k]
        pr, pc = self.place(self.z, w, r0 + self.x * (self.rows // 2), c0)
        return self.targets[a].at[pr, pc]

    def absorb(self, stage, k):
        a, r0, c0, w = self.chunks[k]
        r, hr = self.rows, self.rows // 2
        for c in self.copies(stage, k):
            c.wait_recv()
        if stage == 0:
            for h in range(2):
                self.rc[k, h, :, :w] = self.rc[k, h, :, :w] + self.sources[a][h, self.fl, r0:r0 + r, self.cuts[a] + c0:self.cuts[a] + c0 + w]
        elif stage == 1:
            self.ry[k, :, :w] = self.ry[k, :, :w] + self.rc[k, self.fh, :, :w]
        elif stage == 2:
            mine = self.ry[k, pl.ds(pl.multiple_of(self.x * hr, hr), hr), :w]
            self.rx[k, :, :w] = self.rx[k, :, :w] + mine
        elif stage == 3:
            pr, pc = self.place(self.z, w)
            total = self.rx[k, pr, pc].astype(jnp.float32)
            for o in range(1, self.nz):
                total = total + self.rz[k, o - 1, :, :w // self.pieces_c].astype(jnp.float32)
            self.own(k)[...] = total.astype(jnp.bfloat16)

    def plan(self, entries, points, first, delay):
        lists = [[] for _ in points]
        for k in range(len(self.chunks)):
            for s in range(7):
                n = next(i for i, p in enumerate(points) if p >= entries[k] + (first + (s - 1) * delay if s else 0))
                lists[n].append((s, k))
        return lists

    def tick(self, live):
        for s, k in sorted(live, reverse=True):
            if s > 0:
                self.absorb(s - 1, k)
        for s, k in sorted(live, reverse=True):
            if s < 6:
                for c in self.copies(s, k):
                    c.start()

    def finish(self):
        for k in range(len(self.chunks)):
            for s in range(6):
                for c in self.copies(s, k):
                    c.wait_send()


def split_of(dp, rows=ROWS):
    nz = dp // 2
    pieces_c = min(nz, COLS // 128, 4)
    return pieces_c, max(rows, 32 * (nz // pieces_c))


def chunk_list(shapes, rows, cols=COLS):
    out = []
    for a, (r, c) in enumerate(shapes):
        w = min(c, cols)
        for c0 in range(0, c, w):
            for r0 in range(0, r, rows):
                out.append((a, r0, c0, w))
    return out


def reducer_scratch(dp, shapes, rows=ROWS, cols=COLS):
    nz = dp // 2
    pieces_c, rows = split_of(dp, rows)
    n = len(chunk_list(shapes, rows, cols))
    low = jnp.bfloat16
    return [
        pltpu.VMEM((n, 2, rows, cols), low),
        pltpu.VMEM((n, rows, cols), low),
        pltpu.VMEM((n, rows // 2, cols), low),
        pltpu.VMEM((n, nz - 1, rows // 2 // (nz // pieces_c), cols // pieces_c), low),
        pltpu.SemaphoreType.DMA((4, n)),
        pltpu.SemaphoreType.DMA((4, n)),
        pltpu.SemaphoreType.DMA((n, nz - 1)),
        pltpu.SemaphoreType.DMA((n, nz - 1)),
        pltpu.SemaphoreType.DMA((n, nz - 1)),
        pltpu.SemaphoreType.DMA((n, nz - 1)),
    ]


PARTS = 4


class Spread:

    def __init__(self, shard, full, s_one, r_one, s_part, r_part, parts):
        dp, f = lax.axis_index("dp"), lax.axis_index("fsdp")
        fh, fl = f // 2, f % 2
        self.f, self.x = f, dp % 2
        self.far = (1 - fh) * 2 + fl
        self.core = (dp, fh * 2 + (1 - fl))
        self.other = (dp, self.far)
        self.pair = ((dp // 2) * 2 + (1 - self.x), f)
        self.shard, self.full, self.parts = shard, full, parts
        self.s_one, self.r_one, self.s_part, self.r_part = s_one, r_one, s_part, r_part
        self.half = shard.shape[0] // 2
        self.rows = self.half // parts

    def span(self, half, i):
        return pl.ds(pl.multiple_of(half * self.half + i * self.rows, self.rows), self.rows)

    def send(self, src, dst, s, r, device):
        return pltpu.make_async_remote_copy(src_ref=src, dst_ref=dst, send_sem=s, recv_sem=r, device_id=device, device_id_type=pl.DeviceIdType.MESH)

    def whole(self):
        return self.send(self.shard, self.full.at[self.f], self.s_one, self.r_one, self.core)

    def across(self, i):
        rows = self.span(self.x, i)
        return self.send(self.shard.at[rows], self.full.at[self.f, rows], self.s_part.at[0, i], self.r_part.at[0, i], self.other)

    def onward(self, kind, i):
        rows = self.span(self.x if kind < 3 else 1 - self.x, i)
        ref = self.full.at[self.far, rows]
        return self.send(ref, ref, self.s_part.at[kind, i], self.r_part.at[kind, i], self.pair if kind == 1 else self.core)

    def begin(self):
        self.whole().start()
        for i in range(self.parts):
            self.across(i).start()

    def pump(self, i):
        self.across(i).wait_recv()
        self.onward(1, i).start()
        self.onward(2, i).start()

    def pump_pair(self, i):
        self.onward(1, i).wait_recv()
        self.onward(3, i).start()

    def land(self):
        for i in range(self.parts):
            self.onward(2, i).wait_recv()
            self.onward(3, i).wait_recv()

    def finish(self):
        self.whole().wait_send()
        for i in range(self.parts):
            self.across(i).wait_send()
            for kind in (1, 2, 3):
                self.onward(kind, i).wait_send()


def spread_sems(parts):
    return [pltpu.SemaphoreType.DMA, pltpu.SemaphoreType.DMA, pltpu.SemaphoreType.DMA((4, parts)), pltpu.SemaphoreType.DMA((4, parts))]


def enter_square():
    dp, f = lax.axis_index("dp"), lax.axis_index("fsdp")
    fh, fl = f // 2, f % 2
    barrier = pltpu.get_barrier_semaphore()
    for d in ((dp, fh * 2 + (1 - fl)), (dp, (1 - fh) * 2 + fl), ((dp // 2) * 2 + (1 - dp % 2), f)):
        pl.semaphore_signal(barrier, inc=1, device_id=d, device_id_type=pl.DeviceIdType.MESH)
    pl.semaphore_wait(barrier, 3)


def nt(a, b):
    return lax.dot_general(a, b, (((1,), (1,)), ((), ())), preferred_element_type=jnp.float32)


def front_kernel(dims, len_ref, tok_ref, sml_ref, inw_ref,
                 in_out, sml_out, norm_out, normt_out, inner_out, conv_out, pre_out, far_out, drive_out, bx_out, cx_out, dtrt_out, tap_ref,
                 in_vm, norm_vm, inner, conv, pre, far, drive, act, bx, cx, keep_ref, ptv, osem,
                 a0, a1, a2, a3, b0, b1, b2, b3):
    xw, rank, state, gain_w, width = dims
    t = tok_ref.shape[0]
    low = jnp.bfloat16
    f = lax.axis_index("fsdp")
    fh = f // 2
    outs = []

    def put(src, dst):
        c = pltpu.make_async_copy(src, dst, osem.at[len(outs)])
        c.start()
        outs.append(c)

    enter_square()
    sm = Spread(sml_ref, sml_out, a0, a1, a2, a3, 1)
    di = inner.shape[1]
    wi = Spread(inw_ref.at[:, :di], in_vm, b0, b1, b2, b3, PARTS)
    own_i = pltpu.make_async_copy(inw_ref.at[:, :di], in_vm.at[f], osem.at[40])
    sm.begin()
    wi.begin()
    own_i.start()
    sml_out[f] = sml_ref[...]
    spot = lax.broadcasted_iota(jnp.int32, keep_ref.shape, 0)
    start = jnp.zeros_like(spot)
    run = 0
    for c in range(len_ref.shape[1] - 1):
        run = run + len_ref[0, c]
        start = jnp.where(spot >= run, run, start)
    keep_ref[...] = (spot > start).astype(jnp.float32)
    for j in (1, 2, 3):
        tap_ref[j - 1] = (spot - j >= start).astype(jnp.float32)

    def units(r, _):
        rs = pl.ds(pl.multiple_of(r * 32, 32), 32)
        x = tok_ref[rs, :].astype(jnp.float32)
        conv[rs, :x.shape[1]] = x * lax.rsqrt(jnp.mean(x * x, axis=-1, keepdims=True) + 1e-05)
        return 0

    lax.fori_loop(0, t // 32, units, 0)

    sm.pump(0)
    sm.pump_pair(0)
    sm.whole().wait_recv()
    sm.land()
    at = xw + rank + state
    def gains(r, _):
        rs = pl.ds(pl.multiple_of(r * 64, 64), 64)
        for s in range(4):
            ks, half = slice(s * gain_w, (s + 1) * gain_w), slice((s % 2) * gain_w, (s % 2 + 1) * gain_w)
            v = (conv[rs, ks] * sml_out[s, at + 7:at + 8, :gain_w].astype(jnp.float32)).astype(low)
            norm_vm[s // 2, rs, half] = v
            norm_out[rs, ks] = v
        return 0

    lax.fori_loop(0, t // 64, gains, 0)
    for s in range(4):
        normt_out[s * gain_w:(s + 1) * gain_w, :] = norm_vm[s // 2, :, (s % 2) * gain_w:(s % 2 + 1) * gain_w].T
    own_i.wait()
    wi.whole().wait_recv()
    tile = 256

    def block(h, first, base, dst):
        def go(n, _):
            cols = pl.ds(pl.multiple_of(base + n * tile, tile), tile)
            here = pl.ds(pl.multiple_of(n * tile, tile), tile)
            acc = jnp.dot(norm_vm[h], jnp.concatenate([in_vm[2 * h, :, cols], in_vm[2 * h + 1, :, cols]], axis=0), preferred_element_type=jnp.float32)
            dst[:, here] = acc if first else dst[:, here] + acc
            return 0
        lax.fori_loop(0, dst.shape[1] // tile, go, 0)

    block(fh, True, 0, inner)
    for i in range(PARTS):
        wi.pump(i)
        if i > 0:
            wi.pump_pair(i - 1)
    wi.pump_pair(PARTS - 1)
    wi.land()
    for s in range(4):
        put(in_vm.at[s], in_out.at[s])
    block(1 - fh, False, 0, inner)
    put(inner, inner_out)

    per = width // 128

    for s in range(4):
        def taps(q, _, s=s):
            ln = pl.ds(pl.multiple_of(s * width + q * 128, 128), 128)
            sl = pl.ds(pl.multiple_of(q * 128, 128), 128)
            v = inner[:, ln]
            w = [sml_out[s, at + k:at + k + 1, sl].astype(jnp.float32) for k in range(4)]
            acc = sml_out[s, at + 4:at + 5, sl].astype(jnp.float32) + w[3] * v
            for j in (1, 2, 3):
                acc = acc + w[3 - j] * (pltpu.roll(v, j, 0) * tap_ref[j - 1])
            conv[:, ln] = acc
            a = acc * jax.nn.sigmoid(acc)
            drive[:, ln] = a
            act[:, ln] = a.astype(low)
            return 0

        lax.fori_loop(0, per, taps, 0)
        put(conv.at[:, s * width:(s + 1) * width], conv_out.at[:, s * width:(s + 1) * width])

    pt = jnp.zeros((2 * state, t), jnp.float32)
    dr = jnp.zeros((t, rank), jnp.float32)
    drt = jnp.zeros((rank, t), jnp.float32)
    for s in range(4):
        al = act[:, s * width:(s + 1) * width]
        pt = pt + nt(sml_out[s, rank:xw, :], al)
        dr = dr + nt(al, sml_out[s, :rank, :])
        drt = drt + nt(sml_out[s, :rank, :], al)
    dtr = dr.astype(low)
    dtrt_out[...] = drt.astype(low)
    ptv[...] = pt

    def wide(tb, _):
        part = ptv[:, pl.ds(pl.multiple_of(tb * 128, 128), 128)]
        for l in range(128):
            col = jnp.broadcast_to(part[:, l:l + 1], (2 * state, 128))
            bx[tb * 128 + l] = col[:state]
            cx[tb * 128 + l] = col[state:]
        return 0

    lax.fori_loop(0, t // 128, wide, 0)
    put(bx, bx_out)
    put(cx, cx_out)
    for s in range(4):
        cs = slice(s * width, (s + 1) * width)
        p = jnp.dot(dtr, sml_out[s, xw:xw + rank, :], preferred_element_type=jnp.float32) + sml_out[s, at + 5:at + 6, :].astype(jnp.float32)
        pre[:, cs] = p
        put(pre.at[:, cs], pre_out.at[:, cs])

        def steps(q, _, s=s):
            ln = pl.ds(pl.multiple_of(s * width + q * 128, 128), 128)

            def rows(r, _):
                rs = pl.ds(pl.multiple_of(r * 128, 128), 128)
                v = pre[rs, ln]
                st = jnp.maximum(v, 0.0) + jnp.log1p(jnp.exp(-jnp.abs(v)))
                drive[rs, ln] = drive[rs, ln] * st
                far[rs, ln] = jnp.where(keep_ref[rs, :] > 0, st, 1e30)
                return 0

            return lax.fori_loop(0, t // 128, rows, 0)

        lax.fori_loop(0, per, steps, 0)
        put(far.at[:, cs], far_out.at[:, cs])
        put(drive.at[:, cs], drive_out.at[:, cs])
    for g in (sm, wi):
        g.finish()
    for c in outs:
        c.wait()


def front(lengths, tokens, packed, in_weight, dims):
    xw, rank, state, gain_w, width = dims
    t, d = tokens.shape
    di = 4 * width
    low, f32 = jnp.bfloat16, jnp.float32
    vm = pl.BlockSpec(memory_space=pltpu.VMEM)
    hb = pl.BlockSpec(memory_space=pl.ANY)
    sds = jax.ShapeDtypeStruct
    wide = sds((t, di), f32)
    lanes = sds((t, state, 128), f32)
    return pl.pallas_call(
        functools.partial(front_kernel, dims),
        in_specs=[pl.BlockSpec(memory_space=pltpu.SMEM), vm, vm, hb],
        out_specs=[hb, vm, vm, vm, hb, hb, hb, hb, hb, hb, hb, vm, vm],
        out_shape=[sds((4, gain_w, di), low), sds((4,) + packed.shape, low), sds((t, d), low), sds((d, t), low),
                   wide, wide, wide, wide, wide, lanes, lanes, sds((rank, t), low), sds((3, t, 128), f32)],
        scratch_shapes=[pltpu.VMEM((4, gain_w, di), low), pltpu.VMEM((2, t, d // 2), low)]
        + [pltpu.VMEM((t, di), f32)] * 5 + [pltpu.VMEM((t, di), low)] + [pltpu.VMEM((t, state, 128), f32)] * 2
        + [pltpu.VMEM((t, 128), f32), pltpu.VMEM((2 * state, t), f32), pltpu.SemaphoreType.DMA((42,))] + spread_sems(1) + spread_sems(PARTS),
        compiler_params=pltpu.CompilerParams(collective_id=3, has_side_effects=True, vmem_limit_bytes=63 << 20),
        name="front",
    )(lengths, tokens, packed, in_weight)


BACK_ROWS = 64
BACK_COLS = 512
BACK_FIRST, BACK_DELAY, BACK_GATE, BACK_NEXT = 2.0, 6.5, 2.4, 1.6


def tn(a, b):
    return lax.dot_general(a, b, (((0,), (0,)), ((), ())), preferred_element_type=jnp.float32)


def sum8(v):
    return jnp.sum(v.reshape(v.shape[0] // 8, 8, v.shape[1]), axis=0)


def back_kernel(dp, dims, za_h, gb_h, pre_h, dys_h, conv_h, inner_h, ina_h, inb_h, gl_h, nt_h, gg_ref, tok_ref, cot_ref, sml_ref, dtrt_ref, dbt_ref, rate_ref, tap_ref,
                gsh_ref, ish_ref, ssh_ref, ig_ref,
                za, gb, pre, dys, conv, inner, ina, inb, gl, normt, prelow, actlow, pt, agv, misc, gainv, ng, isrc, ssrc, csem, *comm):
    xw, rank, state, gain_w, width = dims
    t = tok_ref.shape[0]
    low = jnp.bfloat16
    at = xw + rank + state
    per = width // 128

    def fetch(k, src, dst):
        c = pltpu.make_async_copy(src, dst, csem.at[k])
        c.start()
        return c

    def slab(s):
        cs = slice(s * width, (s + 1) * width)
        return [fetch(s * 8 + k, h.at[:, cs], v) for k, (h, v) in enumerate(((conv_h, conv.at[:, cs]), (gb_h, gb.at[s % 2]), (pre_h, pre.at[s % 2]), (dys_h, dys.at[:, cs]), (za_h, za.at[s % 2])))]

    waits = [slab(0), slab(1)]
    late = [fetch(32, inner_h, inner), fetch(33, nt_h, normt), fetch(34, ina_h, ina), fetch(35, gl_h, gl), fetch(36, inb_h, inb)]
    red = Reducer(dp, (gg_ref, isrc, ssrc), (gsh_ref, ish_ref, ssh_ref), comm, BACK_ROWS, BACK_COLS, [gg_ref.shape[3] // 2, 0, 0])
    red.entry()
    misc[...] = jnp.zeros_like(misc)
    points = [1.3 * (i + 1) for i in range(4 * per)] + [22.0 + 3.6 * s + 1.7 * (h + 1) for s in range(4) for h in range(2)]
    points += [36.5 + i for i in range(8)] + [46.0 + 0.8 * i for i in range(120)]
    entries, seen = [], [0, 0, 0]
    for a, r0, c0, w in red.chunks:
        here = 1.3 + seen[0] * BACK_GATE if a == 0 else 46.0 if a == 2 else 22.01 + 3.6 * (c0 // width + 1)
        entries.append(max(here, entries[-1] + BACK_NEXT if entries and a else here))
        seen[a] += 1
    plan = red.plan(entries, points, BACK_FIRST, BACK_DELAY)
    pos = [0]

    def tick():
        red.tick(plan[pos[0]])
        pos[0] += 1

    rankt = jnp.zeros((rank, t), jnp.float32)
    for s in range(4):
        for c in waits[s]:
            c.wait()

        def tile(q, _, s=s):
            ln = pl.ds(pl.multiple_of(s * width + q * 128, 128), 128)
            lq = pl.ds(pl.multiple_of(q * 128, 128), 128)
            skip = sml_ref[s, at + 6:at + 7, lq].astype(jnp.float32)

            def rows(r, sums):
                rs = pl.ds(pl.multiple_of(r * 64, 64), 64)
                cv = conv[rs, ln]
                sg = jax.nn.sigmoid(cv)
                ac = cv * sg
                gv = gb[s % 2, rs, lq]
                pv = pre[s % 2, rs, lq]
                dy = dys[rs, ln]
                st = jnp.maximum(pv, 0.0) + jnp.log1p(jnp.exp(-jnp.abs(pv)))
                pg = (za[s % 2, rs, lq] * LN2 + gv * ac) * jax.nn.sigmoid(pv)
                prelow[rs, lq] = pg.astype(low)
                actlow[rs, ln] = ac.astype(low)
                dys[rs, ln] = dy * skip + gv * st
                conv[rs, ln] = sg * (1.0 + cv * (1.0 - sg))
                return sums[0] + sum8(pg), sums[1] + sum8(dy * ac)

            zero = jnp.zeros((8, 128), jnp.float32)
            bias, skips = lax.fori_loop(0, t // 64, rows, (zero, zero))
            misc[5:6, ln] = jnp.sum(bias, axis=0, keepdims=True)
            misc[6:7, ln] = jnp.sum(skips, axis=0, keepdims=True)
            return 0

        for half in range(2):
            lax.fori_loop(half * (per // 2), (half + 1) * (per // 2), tile, 0)
            for _ in range(per // 2):
                tick()
        if s < 2:
            waits.append(slab(s + 2))
        p = prelow[...]
        ssrc[s // 2, s % 2, xw:xw + rank, :] = jnp.dot(dtrt_ref[...], p, preferred_element_type=jnp.float32).astype(low)
        rankt = rankt + nt(sml_ref[s, xw:xw + rank, :], p)
    pt[:rank] = rankt.astype(low)
    pt[rank:] = dbt_ref[...].astype(low)
    for c in late[:2]:
        c.wait()
    for s in range(4):
        cs = slice(s * width, (s + 1) * width)
        agv[...] = tn(pt[...], sml_ref[s, :xw, :])
        ssrc[s // 2, s % 2, :xw, :] = jnp.dot(pt[...], actlow[:, cs], preferred_element_type=jnp.float32).astype(low)
        ssrc[s // 2, s % 2, xw + rank:at, :] = (-rate_ref[:, cs] * jnp.exp(sml_ref[s, xw + rank:at, :].astype(jnp.float32))).astype(low)

        def tile2(q, _, s=s):
            ln = pl.ds(pl.multiple_of(s * width + q * 128, 128), 128)
            lq = pl.ds(pl.multiple_of(q * 128, 128), 128)
            cg = (agv[:, lq] + dys[:, ln]) * conv[:, ln]
            v = inner[:, ln]
            ig = sml_ref[s, at + 3:at + 4, lq].astype(jnp.float32) * cg
            misc[3:4, ln] = jnp.sum(sum8(cg * v), axis=0, keepdims=True)
            misc[4:5, ln] = jnp.sum(sum8(cg), axis=0, keepdims=True)
            for j in (1, 2, 3):
                m = cg * tap_ref[j - 1]
                misc[3 - j:4 - j, ln] = jnp.sum(sum8(m * pltpu.roll(v, j, 0)), axis=0, keepdims=True)
                ig = ig + sml_ref[s, at + 3 - j:at + 4 - j, lq].astype(jnp.float32) * pltpu.roll(m, t - j, 0)
            actlow[:, ln] = ig.astype(low)
            return 0

        for half in range(2):
            lax.fori_loop(half * (per // 2), (half + 1) * (per // 2), tile2, 0)
            tick()

        def grads(k, _, cs=cs):
            rows = pl.ds(pl.multiple_of(k * gain_w, gain_w), gain_w)
            isrc[k // 2, k % 2, :, cs] = jnp.dot(normt[rows, :], actlow[:, cs], preferred_element_type=jnp.float32).astype(low)
            return 0

        lax.fori_loop(0, 4, grads, 0)
    for c in late[2:]:
        c.wait()
    for blk in range(8):
        tick()
        src = gl if blk < 4 else actlow
        base = (blk % 4) * width
        wsrc = inb if blk < 4 else ina

        def back_in(k, _, blk=blk, src=src, wsrc=wsrc, base=base):
            rows = pl.ds(pl.multiple_of(k * gain_w, gain_w), gain_w)
            part = nt(src[:, base:base + width], wsrc[k, :, base:base + width])
            ng[:, rows] = part if blk == 0 else ng[:, rows] + part
            return 0

        lax.fori_loop(0, 4, back_in, 0)
    for k in range(4):
        gainv[0:1, k * gain_w:(k + 1) * gain_w] = sml_ref[k, at + 7:at + 8, :gain_w].astype(jnp.float32)

    def fin(r, acc):
        rs = pl.ds(pl.multiple_of(r * 32, 32), 32)
        x = tok_ref[rs, :].astype(jnp.float32)
        inv = lax.rsqrt(jnp.mean(x * x, axis=-1, keepdims=True) + 1e-05)
        u = x * inv
        d = ng[rs, :]
        e = d * gainv[0:1, :]
        ig_ref[rs, :] = cot_ref[rs, :].astype(jnp.float32) + inv * (e - u * jnp.mean(e * u, axis=-1, keepdims=True))
        return acc + sum8(d * u)

    gsum = lax.fori_loop(0, t // 32, fin, jnp.zeros((8, ng.shape[1]), jnp.float32))
    gsum = jnp.sum(gsum, axis=0, keepdims=True)
    for k in range(4):
        misc[7:8, k * width:k * width + gain_w] = gsum[:, k * gain_w:(k + 1) * gain_w]
    for k in range(4):
        ssrc[k // 2, k % 2, at:at + 16, :] = misc[:, k * width:(k + 1) * width].astype(low)
        if ssrc.shape[2] > at + 16:
            ssrc[k // 2, k % 2, at + 16:, :] = jnp.zeros((ssrc.shape[2] - at - 16, width), low)
    while pos[0] < len(plan):
        tick()
    red.finish()


def back(dp, dims, za, gb, pre, dys, conv, inner, in_a, in_b, gate_low, normt, gg, tokens, cot, small, dtrt, dbt, rate, tapb):
    xw, rank, state, gain_w, width = dims
    t, d = tokens.shape
    di = 4 * width
    low, f32 = jnp.bfloat16, jnp.float32
    unit = split_of(dp, BACK_ROWS)[1]
    srows = -(-(xw + rank + state + 16) // unit) * unit
    shapes = [(gain_w, di // 2), (gain_w, di), (srows, width)]
    vm = pl.BlockSpec(memory_space=pltpu.VMEM)
    hb = pl.BlockSpec(memory_space=pl.ANY)
    sds = jax.ShapeDtypeStruct
    return pl.pallas_call(
        functools.partial(back_kernel, dp, dims),
        in_specs=[hb] * 10 + [vm] * 8,
        out_specs=[vm] * 4,
        out_shape=[sds(shapes[0], low), sds(shapes[1], low), sds(shapes[2], low), sds((t, d), f32)],
        scratch_shapes=[pltpu.VMEM((2, t, width), f32)] * 3 + [pltpu.VMEM((t, di), f32)] * 3
        + [pltpu.VMEM(in_a.shape, low), pltpu.VMEM(in_b.shape, low), pltpu.VMEM((t, di), low), pltpu.VMEM((d, t), low), pltpu.VMEM((t, width), low), pltpu.VMEM((t, di), low),
           pltpu.VMEM((xw, t), low), pltpu.VMEM((t, width), f32), pltpu.VMEM((16, di), f32), pltpu.VMEM((8, d), f32), pltpu.VMEM((t, d), f32),
           pltpu.VMEM((2, 2) + shapes[1], low), pltpu.VMEM((2, 2) + shapes[2], low), pltpu.SemaphoreType.DMA((37,))]
        + reducer_scratch(dp, shapes, BACK_ROWS, BACK_COLS),
        compiler_params=pltpu.CompilerParams(collective_id=1, has_side_effects=True, vmem_limit_bytes=63 << 20),
        name="back",
    )(za, gb, pre, dys, conv, inner, in_a, in_b, gate_low, normt, gg.reshape((2, 2, gain_w, di)), tokens, cot, small, dtrt, dbt, rate, tapb)


def last_kernel(dims, i_ref, ga_ref, gb_ref, o_ref, s_ref, x_ref, xo_ref, in_ref, og_ref, gain_ref, cw_ref, cb_ref, xp_ref, dw_ref, db_ref, al_ref, sk_ref):
    xw, rank, state, gain_w, width = dims
    f32 = jnp.float32
    half = i_ref.shape[1]
    n = 16
    step_i, step_o, step_x = i_ref.shape[0] // n, o_ref.shape[0] // n, x_ref.shape[0] // n

    def rows(r, _):
        ri, ro, rx = (pl.ds(pl.multiple_of(r * v, v), v) for v in (step_i, step_o, step_x))
        xo_ref[rx, :] = x_ref[rx, :]
        in_ref[ri, :half] = i_ref[ri, :].astype(f32)
        in_ref[ri, half:half + half // 2] = ga_ref[ri, :].astype(f32)
        in_ref[ri, half + half // 2:] = gb_ref[ri, :].astype(f32)
        og_ref[ro, :] = o_ref[ro, :].astype(f32)
        return 0

    lax.fori_loop(0, n, rows, 0)
    at = xw + rank + state
    xp_ref[...] = s_ref[:xw, :].astype(f32)
    dw_ref[...] = s_ref[xw:xw + rank, :].astype(f32)
    al_ref[...] = s_ref[xw + rank:at, :].astype(f32)
    tail = s_ref[at:at + 16, :].astype(f32)
    cw_ref[...] = tail[:4]
    cb_ref[...] = tail[4:5]
    db_ref[...] = tail[5:6]
    sk_ref[...] = tail[6:7]
    gain_ref[...] = tail[7:8, :gain_w]


def last(dims, ish, gsa, gsb, osh, ssh, grad):
    xw, rank, state, gain_w, width = dims
    f32 = jnp.float32
    sds = jax.ShapeDtypeStruct
    vm = pl.BlockSpec(memory_space=pltpu.VMEM)
    return pl.pallas_call(
        functools.partial(last_kernel, dims),
        in_specs=[vm] * 6,
        out_specs=[vm] * 11,
        out_shape=[sds(grad.shape, f32), sds((ish.shape[0], 2 * ish.shape[1]), f32), sds(osh.shape, f32), sds((1, gain_w), f32), sds((4, width), f32), sds((1, width), f32),
                   sds((xw, width), f32), sds((rank, width), f32), sds((1, width), f32), sds((state, width), f32), sds((1, width), f32)],
        compiler_params=pltpu.CompilerParams(vmem_limit_bytes=63 << 20),
        name="last",
    )(ish, gsa, gsb, osh, ssh, grad)


LANE = 128
NS = 16
TC = 64
CGF = 1024
CGB = 512


def bcast(ref, i, row):
    v = ref[i, pl.ds(row, 8, stride=0), :]
    return jnp.concatenate([v, v], axis=0)


def stage(src, dst):
    for i in range(dst.shape[0]):
        dst[i] = src[:, i * LANE:(i + 1) * LANE]


def fold(src, i):
    s = [src[i, pl.ds(q, 8, stride=8), :] for q in range(8)]
    return ((s[0] + s[1]) + (s[2] + s[3])) + ((s[4] + s[5]) + (s[6] + s[7]))


def fwd_kernel(dt_ref, dr_ref, b_ref, c_ref, a_ref, inw_ref, outw_ref, y_ref, hs_ref, inb_ref, all_ref,
               part, dts, drs, hst, bi, bo, lsem, b0, b1, b2, b3, c0, c1, c2, c3):
    step = pl.program_id(0) * pl.num_programs(1) + pl.program_id(1)
    di = inb_ref.shape[2]
    f = lax.axis_index("fsdp")
    wb = Spread(inw_ref.at[:, di:], inb_ref, b0, b1, b2, b3, PARTS)
    wo = Spread(outw_ref, all_ref, c0, c1, c2, c3, PARTS)
    into = [pltpu.make_async_copy(inw_ref.at[:, di:], bi, lsem.at[0]), pltpu.make_async_copy(outw_ref, bo, lsem.at[1])]
    away = [pltpu.make_async_copy(bi, inb_ref.at[f], lsem.at[2]), pltpu.make_async_copy(bo, all_ref.at[f], lsem.at[3])]

    @pl.when(step == 0)
    def _():
        enter_square()
        wb.begin()
        wo.begin()
        for c in into:
            c.start()

    @pl.when(step == 1)
    def _():
        for c in into:
            c.wait()
        for c in away:
            c.start()

    for i in range(2 * PARTS):
        @pl.when(step == PUMPS[i])
        def _(i=i):
            (wb if i < PARTS else wo).pump(i % PARTS)
            if i > 0:
                (wb if i - 1 < PARTS else wo).pump_pair((i - 1) % PARTS)

    @pl.when(step == pl.num_programs(0) * pl.num_programs(1) - 1)
    def _():
        wo.pump_pair(PARTS - 1)
        for w in (wb, wo):
            w.whole().wait_recv()
            w.land()
            w.finish()
        for c in away:
            c.wait()

    cg = dt_ref.shape[1]
    tiles = cg // LANE
    tc = dt_ref.shape[0]

    @pl.when(pl.program_id(1) == 0)
    def _():
        hst[...] = jnp.zeros_like(hst)

    stage(dt_ref, dts)
    stage(dr_ref, drs)

    def group(g, carry):
        t0 = pl.multiple_of(g * 8, 8)
        hs = list(carry)
        for k in range(8):
            bt = b_ref[t0 + k]
            ct = c_ref[t0 + k]
            for i in range(tiles):
                ln = slice(i * LANE, (i + 1) * LANE)
                d = bcast(dts, i, t0 + k)
                u = bcast(drs, i, t0 + k)
                a = jnp.exp2(d * a_ref[:, ln])
                hs_ref[0, t0 + k, :, ln] = hs[i]
                h = a * hs[i] + bt * u
                hs[i] = h
                p = ct * h
                part[i, k * 8:(k + 1) * 8, :] = p[:8] + p[8:]
        for i in range(tiles):
            ln = slice(i * LANE, (i + 1) * LANE)
            y_ref[pl.ds(t0, 8), ln] = fold(part, i)
        return tuple(hs)

    init = tuple(hst[:, i * LANE:(i + 1) * LANE] for i in range(tiles))
    out = lax.fori_loop(0, tc // 8, group, init, unroll=2)
    for i in range(tiles):
        hst[:, i * LANE:(i + 1) * LANE] = out[i]
        hs_ref[0, tc, :, i * LANE:(i + 1) * LANE] = out[i]


PUMPS = (2, 4, 6, 8, 10, 12, 13, 14)


def scan_forward(dt, dr, bx, cx, a2, in_weight, out_weight, tc=TC, cg=CGF):
    t, c = dt.shape
    nt, nc = t // tc, c // cg
    assert nt * nc > PUMPS[-1] + 1
    return pl.pallas_call(
        fwd_kernel,
        grid=(nc, nt),
        in_specs=[
            pl.BlockSpec((tc, cg), lambda j, i: (i, j)),
            pl.BlockSpec((tc, cg), lambda j, i: (i, j)),
            pl.BlockSpec((tc, NS, LANE), lambda j, i: (i, 0, 0)),
            pl.BlockSpec((tc, NS, LANE), lambda j, i: (i, 0, 0)),
            pl.BlockSpec((NS, cg), lambda j, i: (0, j)),
            pl.BlockSpec(memory_space=pl.ANY),
            pl.BlockSpec(memory_space=pl.ANY),
        ],
        out_specs=[
            pl.BlockSpec((tc, cg), lambda j, i: (i, j)),
            pl.BlockSpec((1, tc + 1, NS, cg), lambda j, i: (i, 0, 0, j)),
            pl.BlockSpec(memory_space=pl.ANY),
            pl.BlockSpec(memory_space=pl.ANY),
        ],
        out_shape=[
            jax.ShapeDtypeStruct((t, c), jnp.float32),
            jax.ShapeDtypeStruct((nt, tc + 1, NS, c), jnp.float32),
            jax.ShapeDtypeStruct((4, in_weight.shape[0], c), jnp.bfloat16),
            jax.ShapeDtypeStruct((4,) + out_weight.shape, jnp.bfloat16),
        ],
        scratch_shapes=[pltpu.VMEM((cg // LANE, 64, LANE), jnp.float32)] + [pltpu.VMEM((cg // LANE, tc, LANE), jnp.float32)] * 2 + [pltpu.VMEM((NS, cg), jnp.float32), pltpu.VMEM((in_weight.shape[0], c), jnp.bfloat16), pltpu.VMEM(out_weight.shape, jnp.bfloat16), pltpu.SemaphoreType.DMA((4,))] + spread_sems(PARTS) * 2,
        compiler_params=pltpu.CompilerParams(vmem_limit_bytes=63 << 20, collective_id=4, has_side_effects=True),
        name="scan_forward",
    )(dt, dr, bx, cx, a2, in_weight, out_weight)


def bwd_kernel(dp, steps, dt_ref, dr_ref, dy_ref, b_ref, c_ref, a_ref, hs_ref, og_ref, gg_ref,
               za_ref, gb_ref, dbt_ref, rate_ref, os_ref, gs_ref,
               db_ref, dc_ref, pz, pg, dts, drs, dys, gst, rst, ores, gres, *comm):
    red = Reducer(dp, (og_ref, gg_ref), (ores, gres), comm, SCAN_ROWS)
    step = pl.program_id(0) * pl.num_programs(1) + pl.program_id(1)
    count = len(red.chunks)
    plan = red.plan([k * SCAN_RATE * 24 / max(count, 24) for k in range(count)], range(steps), SCAN_FIRST, SCAN_DELAY)

    def tree(lo, hi):
        if hi - lo == 1:
            if lo == 0:
                red.entry()
            red.tick(plan[lo])
            return
        mid = (lo + hi) // 2
        lax.cond(step < mid, lambda: tree(lo, mid), lambda: tree(mid, hi))

    tree(0, steps)

    @pl.when(step == pl.num_programs(0) * pl.num_programs(1) - 1)
    def _():
        red.finish()
        os_ref[...] = ores[...]
        gs_ref[...] = gres[...]

    cg = dt_ref.shape[1]
    tiles = cg // LANE
    tc = dt_ref.shape[0]
    j = pl.program_id(0)
    i_t = pl.program_id(1)
    nt = pl.num_programs(1)

    @pl.when(i_t == 0)
    def _():
        gst[...] = jnp.zeros_like(gst)
        rst[...] = jnp.zeros_like(rst)

    @pl.when(step == 0)
    def _():
        db_ref[...] = jnp.zeros_like(db_ref)
        dc_ref[...] = jnp.zeros_like(dc_ref)

    stage(dt_ref, dts)
    stage(dr_ref, drs)
    stage(dy_ref, dys)
    lanes = [slice(i * LANE, (i + 1) * LANE) for i in range(tiles)]

    base = pl.multiple_of((nt - 1 - i_t) * tc, tc)

    def bgroup(gi, carry):
        g = tc // 8 - 1 - gi
        t0 = pl.multiple_of(g * 8, 8)
        gs = list(carry[0])
        rs = list(carry[1])
        for k in range(7, -1, -1):
            bt = b_ref[t0 + k]
            ct = c_ref[t0 + k]
            accb = None
            for i in range(tiles):
                ln = lanes[i]
                d = bcast(dts, i, t0 + k)
                u = bcast(drs, i, t0 + k)
                w = bcast(dys, i, t0 + k)
                hnow = hs_ref[0, t0 + k + 1, :, ln]
                hprev = hs_ref[0, t0 + k, :, ln]
                a = jnp.exp2(d * a_ref[:, ln])
                gg = ct * w + gs[i]
                ga = gg * a
                z = ga * hprev
                rs[i] = rs[i] + z * d
                gs[i] = ga
                pa = z * a_ref[:, ln]
                pz[i, k * 8:(k + 1) * 8, :] = pa[:8] + pa[8:]
                pb = gg * bt
                pg[i, k * 8:(k + 1) * 8, :] = pb[:8] + pb[8:]
                vb = gg * u
                vc = w * hnow
                accb = vb if accb is None else accb + vb
                accc = vc if i == 0 else accc + vc
            row = base + t0 + k

            db_ref[row] = db_ref[row] + accb
            dc_ref[row] = dc_ref[row] + accc
        for i in range(tiles):
            ln = lanes[i]
            za_ref[pl.ds(t0, 8), ln] = fold(pz, i)
            gb_ref[pl.ds(t0, 8), ln] = fold(pg, i)
        return tuple(gs), tuple(rs)

    gs, rs = lax.fori_loop(0, tc // 8, bgroup, (tuple(gst[:, ln] for ln in lanes), tuple(rst[:, ln] for ln in lanes)), unroll=2)
    for i in range(tiles):
        gst[:, lanes[i]] = gs[i]
        rst[:, lanes[i]] = rs[i]

    @pl.when(i_t == nt - 1)
    def _():
        rate_ref[...] = rst[...]

    @pl.when(j == pl.num_programs(0) - 1)
    def _():
        block = pl.ds(pl.multiple_of((base // LANE) * LANE, LANE), LANE)
        lane = lax.broadcasted_iota(jnp.int32, (NS, LANE), 1)
        at = base % LANE

        def put(k, accs):
            row = base + k
            hit = lane == at + k
            return (jnp.where(hit, jnp.sum(db_ref[row], axis=-1, keepdims=True), accs[0]),
                    jnp.where(hit, jnp.sum(dc_ref[row], axis=-1, keepdims=True), accs[1]))

        got = lax.fori_loop(0, tc, put, (dbt_ref[:NS, block], dbt_ref[NS:, block]), unroll=8)
        dbt_ref[:NS, block] = got[0]
        dbt_ref[NS:, block] = got[1]


def scan_backward(dp, dt, dr, dy, bx, cx, a2, hs, og, gg, tc=TC, cg=CGB):
    t, c = dt.shape
    nt, nc = t // tc, c // cg
    row = pl.BlockSpec((tc, cg), lambda j, i: (nt - 1 - i, j))
    bc = pl.BlockSpec((tc, NS, LANE), lambda j, i: (nt - 1 - i, 0, 0))
    once = lambda s: pl.BlockSpec(s, lambda j, i: (0,) * len(s), pipeline_mode=pl.Buffered(1))
    og = og.reshape((2, 2) + og.shape[1:])
    gg = gg.reshape((2, 2) + gg.shape[1:])
    parts = [og.shape[2:], (gg.shape[2], gg.shape[3] // 2)]
    return pl.pallas_call(
        functools.partial(bwd_kernel, dp, nc * nt),
        grid=(nc, nt),
        in_specs=[row, row, row, bc, bc, pl.BlockSpec((NS, cg), lambda j, i: (0, j)),
                  pl.BlockSpec((1, tc + 1, NS, cg), lambda j, i: (nt - 1 - i, 0, 0, j)), once(og.shape), once((2, 2) + parts[1])],
        out_specs=[row, row, once((2 * NS, t)), pl.BlockSpec((NS, cg), lambda j, i: (0, j)), once(parts[0]), once(parts[1])],
        out_shape=[
            jax.ShapeDtypeStruct((t, c), jnp.float32),
            jax.ShapeDtypeStruct((t, c), jnp.float32),
            jax.ShapeDtypeStruct((2 * NS, t), jnp.float32),
            jax.ShapeDtypeStruct((NS, c), jnp.float32),
            jax.ShapeDtypeStruct(parts[0], jnp.bfloat16),
            jax.ShapeDtypeStruct(parts[1], jnp.bfloat16),
        ],
        scratch_shapes=[
            pltpu.VMEM((t, NS, LANE), jnp.float32), pltpu.VMEM((t, NS, LANE), jnp.float32),
            pltpu.VMEM((cg // LANE, 64, LANE), jnp.float32), pltpu.VMEM((cg // LANE, 64, LANE), jnp.float32),
            pltpu.VMEM((cg // LANE, tc, LANE), jnp.float32), pltpu.VMEM((cg // LANE, tc, LANE), jnp.float32), pltpu.VMEM((cg // LANE, tc, LANE), jnp.float32),
            pltpu.VMEM((NS, cg), jnp.float32), pltpu.VMEM((NS, cg), jnp.float32),
            pltpu.VMEM(parts[0], jnp.bfloat16), pltpu.VMEM(parts[1], jnp.bfloat16),
        ] + reducer_scratch(dp, parts, SCAN_ROWS),
        compiler_params=pltpu.CompilerParams(vmem_limit_bytes=60 << 20, collective_id=2, has_side_effects=True),
        name="scan_backward",
    )(dt, dr, dy, bx, cx, a2, hs, og, gg)


def pack_small(gain, conv_w, conv_b, xproj, dt_w, dt_b, alog, skip):
    width = conv_b.shape[-1]
    gain_row = jnp.pad(gain[None], ((0, 0), (0, width - gain.shape[0])))
    return jnp.concatenate(
        [xproj.T, dt_w, alog, conv_w, conv_b[None], dt_b[None], skip[None], gain_row], axis=0
    )


def body(
    tokens,
    cluster_lengths,
    norm_gain,
    in_weight,
    conv_weight,
    conv_bias,
    xproj_weight,
    dt_weight,
    dt_bias,
    a_log,
    skip_gain,
    out_weight,
    cotangent,
):
    low = jnp.bfloat16
    gain_shard = norm_gain.shape[0]
    width = conv_bias.shape[0]
    packed = pack_small(norm_gain, conv_weight, conv_bias, xproj_weight, dt_weight, dt_bias, a_log, skip_gain)
    packed = jnp.pad(packed, ((0, -packed.shape[0] % 32), (0, 0)))
    shards = lax.axis_size("fsdp")
    xw, rank, state = xproj_weight.shape[1], dt_weight.shape[0], a_log.shape[0]
    inner_width = shards * width
    (in_a, small, normed_low, normed_t, inner_in, conv_out, dt_pre, step_far, drive, bx, cx, dt_t, tapb) = front(
        cluster_lengths, tokens, packed, in_weight, (xw, rank, state, gain_shard, width)
    )
    rows = jnp.moveaxis(small, 0, 1).reshape(small.shape[1], inner_width)
    at = xw + rank
    decay_rate = -jnp.exp(rows[at : at + state].astype(jnp.float32))
    at += state
    at += KCONV
    skip_value = rows[at + 2].astype(jnp.float32)
    inputs_full = tokens.astype(jnp.float32)
    conv_act = silu_of(conv_out)
    rate2 = decay_rate * LOG2E
    scanned, starts, in_b, out_all = scan_forward(step_far, drive, bx, cx, rate2, in_weight, out_weight)
    out_full = out_all.reshape(-1, out_weight.shape[1])
    gate_in = matmul(normed_low, in_b.reshape(-1, inner_width))
    with_skip = scanned + skip_value * conv_act
    gate_act = silu_of(gate_in)
    gated_low = (with_skip * gate_act).astype(low)
    result = inputs_full + matmul(gated_low, out_full)
    output = result.astype(low)
    out_grad = left_inner(gated_low, cotangent)
    gated_grad = right_inner(cotangent, out_full)
    skip_part = gated_grad * gate_act
    gate_grad = gated_grad * with_skip * silu_slope(gate_in)
    gate_low = gate_grad.astype(low)
    gate_low_grad = left_inner(normed_low, gate_low).astype(low).reshape(shards, -1, inner_width)
    dp = lax.axis_size("dp")
    za, gb, dbt, rate_grad, out_share, gate_share_a = scan_backward(
        dp,
        step_far,
        drive,
        skip_part,
        bx,
        cx,
        rate2,
        starts,
        out_grad.astype(low).reshape(shards, -1, out_grad.shape[1]),
        gate_low_grad,
    )
    gate_share, inner_share, small_share, input_grad = back(
        dp, (xw, rank, state, gain_shard, width), za, gb, dt_pre, skip_part, conv_out, inner_in, in_a, in_b, gate_low,
        normed_t, gate_low_grad, tokens, cotangent, small, dt_t, dbt, rate_grad, tapb,
    )
    input_grad, in_grad, out_weight_grad, gain_g, conv_g, conv_b, xproj_g, dt_g, dt_b, alog_g, skip_g = last(
        (xw, rank, state, gain_shard, width), inner_share, gate_share_a, gate_share, out_share, small_share, input_grad
    )
    return (
        output, input_grad, gain_g[0], in_grad, conv_g, conv_b[0], xproj_g.T, dt_g, dt_b[0], alog_g, skip_g[0], out_weight_grad
    )


def solution(mesh):
    in_specs = (
        P(("dp", "fsdp"), None),
        P(("dp", "fsdp"), None),
        P("fsdp"),
        P("fsdp", None),
        P(None, "fsdp"),
        P("fsdp"),
        P("fsdp", None),
        P(None, "fsdp"),
        P("fsdp"),
        P(None, "fsdp"),
        P("fsdp"),
        P("fsdp", None),
        P(("dp", "fsdp"), None),
    )
    out_specs = (
        P(("dp", "fsdp"), None),
        P(("dp", "fsdp"), None),
        P("fsdp"),
        P("fsdp", None),
        P(None, "fsdp"),
        P("fsdp"),
        P("fsdp", None),
        P(None, "fsdp"),
        P("fsdp"),
        P(None, "fsdp"),
        P("fsdp"),
        P("fsdp", None),
    )
    return jax.shard_map(body, mesh=mesh, in_specs=in_specs, out_specs=out_specs, check_vma=False)
```

```python
import functools

import jax
import jax.numpy as jnp
import numpy as np
from jax import lax
from jax.experimental import pallas as pl
from jax.experimental.pallas import tpu as pltpu
from jax.sharding import PartitionSpec as P

KCONV = 4
LENGTH = 512
LOG2E = float(np.log2(np.e))
LN2 = float(np.log(2.0))
FAR = 1e30


epsilon = 1e-05


def matmul(former, latter):
    return jnp.dot(former, latter, preferred_element_type=jnp.float32)


def left_inner(former, latter):
    return lax.dot_general(
        former, latter, (((0,), (0,)), ((), ())), preferred_element_type=jnp.float32
    )


def right_inner(former, latter):
    return lax.dot_general(
        former, latter, (((1,), (1,)), ((), ())), preferred_element_type=jnp.float32
    )


def silu_of(values):
    return values * jax.nn.sigmoid(values)


def silu_slope(values):
    logistic = jax.nn.sigmoid(values)
    return logistic * (1.0 + values * (1.0 - logistic))

MESH = pl.DeviceIdType.MESH
COLS = 1024
ROWS = 32
SCAN_ROWS, SCAN_RATE, SCAN_FIRST, SCAN_DELAY = 64, 1.3, 1.0, 2.9


class Reducer:

    def __init__(self, dp, sources, targets, scratch, rows=ROWS, cols=COLS, cuts=None):
        self.nz = dp // 2
        self.sources, self.targets = sources, targets
        (self.rc, self.ry, self.rx, self.rz, self.s_one, self.r_one, self.s_rs, self.r_rs, self.s_ag, self.r_ag) = scratch
        self.me_dp, self.me_f = lax.axis_index("dp"), lax.axis_index("fsdp")
        self.fh, self.fl = self.me_f // 2, self.me_f % 2
        self.z, self.x = self.me_dp // 2, self.me_dp % 2
        self.pieces_c, self.rows = split_of(dp, rows)
        self.pieces_r = self.nz // self.pieces_c
        self.cuts = cuts or [0] * len(targets)
        self.chunks = chunk_list([t.shape for t in targets], self.rows, cols)
        self.core = (self.me_dp, self.fh * 2 + (1 - self.fl))
        self.other = (self.me_dp, (1 - self.fh) * 2 + self.fl)
        self.pair = (self.z * 2 + (1 - self.x), self.me_f)

    def peer(self, o):
        return lax.rem(self.z + o, self.nz)

    def entry(self):
        barrier = pltpu.get_barrier_semaphore()
        ids = [self.core, self.other, self.pair] + [(self.peer(o) * 2 + self.x, self.me_f) for o in range(1, self.nz)]
        for d in ids:
            pl.semaphore_signal(barrier, inc=1, device_id=d, device_id_type=MESH)
        pl.semaphore_wait(barrier, len(ids))

    def copy(self, src, dst, send, recv, device):
        return pltpu.make_async_remote_copy(src_ref=src, dst_ref=dst, send_sem=send, recv_sem=recv, device_id=device, device_id_type=MESH)

    def copies(self, stage, k):
        a, r0, c0, w = self.chunks[k]
        r, hr = self.rows, self.rows // 2
        if stage == 0:
            src = self.sources[a].at[:, 1 - self.fl, r0:r0 + r, self.cuts[a] + c0:self.cuts[a] + c0 + w]
            return [self.copy(src, self.rc.at[k, :, :, :w], self.s_one.at[0, k], self.r_one.at[0, k], self.core)]
        if stage == 1:
            return [self.copy(self.rc.at[k, 1 - self.fh, :, :w], self.ry.at[k, :, :w], self.s_one.at[1, k], self.r_one.at[1, k], self.other)]
        if stage == 2:
            src = self.ry.at[k, pl.ds(pl.multiple_of((1 - self.x) * hr, hr), hr), :w]
            return [self.copy(src, self.rx.at[k, :, :w], self.s_one.at[2, k], self.r_one.at[2, k], self.pair)]
        out = []
        if stage == 5:
            rows = pl.ds(pl.multiple_of(r0 + self.x * hr, hr), hr)
            t = self.targets[a].at[rows, c0:c0 + w]
            return [self.copy(t, t, self.s_one.at[3, k], self.r_one.at[3, k], self.pair)]
        for o in range(1, self.nz):
            j = self.peer(o)
            device = (j * 2 + self.x, self.me_f)
            if stage == 3:
                pr, pc = self.place(j, w)
                out.append(self.copy(self.rx.at[k, pr, pc], self.rz.at[k, o - 1, :, :w // self.pieces_c], self.s_rs.at[k, o - 1], self.r_rs.at[k, o - 1], device))
            else:
                t = self.own(k)
                out.append(self.copy(t, t, self.s_ag.at[k, o - 1], self.r_ag.at[k, o - 1], device))
        return out

    def place(self, j, w, r0=0, c0=0):
        pr, pw = self.rows // 2 // self.pieces_r, w // self.pieces_c
        return (pl.ds(pl.multiple_of(r0 + (j // self.pieces_c) * pr, 16), pr), pl.ds(pl.multiple_of(c0 + lax.rem(j, self.pieces_c) * pw, 128), pw))

    def own(self, k):
        a, r0, c0, w = self.chunks[k]
        pr, pc = self.place(self.z, w, r0 + self.x * (self.rows // 2), c0)
        return self.targets[a].at[pr, pc]

    def absorb(self, stage, k):
        a, r0, c0, w = self.chunks[k]
        r, hr = self.rows, self.rows // 2
        for c in self.copies(stage, k):
            c.wait_recv()
        if stage == 0:
            for h in range(2):
                self.rc[k, h, :, :w] = self.rc[k, h, :, :w] + self.sources[a][h, self.fl, r0:r0 + r, self.cuts[a] + c0:self.cuts[a] + c0 + w]
        elif stage == 1:
            self.ry[k, :, :w] = self.ry[k, :, :w] + self.rc[k, self.fh, :, :w]
        elif stage == 2:
            mine = self.ry[k, pl.ds(pl.multiple_of(self.x * hr, hr), hr), :w]
            self.rx[k, :, :w] = self.rx[k, :, :w] + mine
        elif stage == 3:
            pr, pc = self.place(self.z, w)
            total = self.rx[k, pr, pc].astype(jnp.float32)
            for o in range(1, self.nz):
                total = total + self.rz[k, o - 1, :, :w // self.pieces_c].astype(jnp.float32)
            self.own(k)[...] = total.astype(jnp.bfloat16)

    def plan(self, entries, points, first, delay):
        lists = [[] for _ in points]
        for k in range(len(self.chunks)):
            for s in range(7):
                n = next(i for i, p in enumerate(points) if p >= entries[k] + (first + (s - 1) * delay if s else 0))
                lists[n].append((s, k))
        return lists

    def tick(self, live):
        for s, k in sorted(live, reverse=True):
            if s > 0:
                self.absorb(s - 1, k)
        for s, k in sorted(live, reverse=True):
            if s < 6:
                for c in self.copies(s, k):
                    c.start()

    def finish(self):
        for k in range(len(self.chunks)):
            for s in range(6):
                for c in self.copies(s, k):
                    c.wait_send()


def split_of(dp, rows=ROWS):
    nz = dp // 2
    pieces_c = min(nz, COLS // 128, 4)
    return pieces_c, max(rows, 32 * (nz // pieces_c))


def chunk_list(shapes, rows, cols=COLS):
    out = []
    for a, (r, c) in enumerate(shapes):
        w = min(c, cols)
        for c0 in range(0, c, w):
            for r0 in range(0, r, rows):
                out.append((a, r0, c0, w))
    return out


def reducer_scratch(dp, shapes, rows=ROWS, cols=COLS):
    nz = dp // 2
    pieces_c, rows = split_of(dp, rows)
    n = len(chunk_list(shapes, rows, cols))
    low = jnp.bfloat16
    return [
        pltpu.VMEM((n, 2, rows, cols), low),
        pltpu.VMEM((n, rows, cols), low),
        pltpu.VMEM((n, rows // 2, cols), low),
        pltpu.VMEM((n, nz - 1, rows // 2 // (nz // pieces_c), cols // pieces_c), low),
        pltpu.SemaphoreType.DMA((4, n)),
        pltpu.SemaphoreType.DMA((4, n)),
        pltpu.SemaphoreType.DMA((n, nz - 1)),
        pltpu.SemaphoreType.DMA((n, nz - 1)),
        pltpu.SemaphoreType.DMA((n, nz - 1)),
        pltpu.SemaphoreType.DMA((n, nz - 1)),
    ]


PARTS = 4


class Spread:

    def __init__(self, shard, full, s_one, r_one, s_part, r_part, parts):
        dp, f = lax.axis_index("dp"), lax.axis_index("fsdp")
        fh, fl = f // 2, f % 2
        self.f, self.x = f, dp % 2
        self.far = (1 - fh) * 2 + fl
        self.core = (dp, fh * 2 + (1 - fl))
        self.other = (dp, self.far)
        self.pair = ((dp // 2) * 2 + (1 - self.x), f)
        self.shard, self.full, self.parts = shard, full, parts
        self.s_one, self.r_one, self.s_part, self.r_part = s_one, r_one, s_part, r_part
        self.half = shard.shape[0] // 2
        self.rows = self.half // parts

    def span(self, half, i):
        return pl.ds(pl.multiple_of(half * self.half + i * self.rows, self.rows), self.rows)

    def send(self, src, dst, s, r, device):
        return pltpu.make_async_remote_copy(src_ref=src, dst_ref=dst, send_sem=s, recv_sem=r, device_id=device, device_id_type=pl.DeviceIdType.MESH)

    def whole(self):
        return self.send(self.shard, self.full.at[self.f], self.s_one, self.r_one, self.core)

    def across(self, i):
        rows = self.span(self.x, i)
        return self.send(self.shard.at[rows], self.full.at[self.f, rows], self.s_part.at[0, i], self.r_part.at[0, i], self.other)

    def onward(self, kind, i):
        rows = self.span(self.x if kind < 3 else 1 - self.x, i)
        ref = self.full.at[self.far, rows]
        return self.send(ref, ref, self.s_part.at[kind, i], self.r_part.at[kind, i], self.pair if kind == 1 else self.core)

    def begin(self):
        for i in range(self.parts):
            self.across(i).start()
        self.whole().start()

    def pump(self, i):
        self.across(i).wait_recv()
        self.onward(1, i).start()
        self.onward(2, i).start()

    def pump_pair(self, i):
        self.onward(1, i).wait_recv()
        self.onward(3, i).start()

    def land(self):
        for i in range(self.parts):
            self.onward(2, i).wait_recv()
            self.onward(3, i).wait_recv()

    def finish(self):
        self.whole().wait_send()
        for i in range(self.parts):
            self.across(i).wait_send()
            for kind in (1, 2, 3):
                self.onward(kind, i).wait_send()


def spread_sems(parts):
    return [pltpu.SemaphoreType.DMA, pltpu.SemaphoreType.DMA, pltpu.SemaphoreType.DMA((4, parts)), pltpu.SemaphoreType.DMA((4, parts))]


def enter_square():
    dp, f = lax.axis_index("dp"), lax.axis_index("fsdp")
    fh, fl = f // 2, f % 2
    barrier = pltpu.get_barrier_semaphore()
    for d in ((dp, fh * 2 + (1 - fl)), (dp, (1 - fh) * 2 + fl), ((dp // 2) * 2 + (1 - dp % 2), f)):
        pl.semaphore_signal(barrier, inc=1, device_id=d, device_id_type=pl.DeviceIdType.MESH)
    pl.semaphore_wait(barrier, 3)


def nt(a, b):
    return lax.dot_general(a, b, (((1,), (1,)), ((), ())), preferred_element_type=jnp.float32)


def front_kernel(dims, len_ref, tok_ref, sml_ref, inw_ref,
                 in_out, sml_out, norm_out, normt_out, inner_out, conv_out, pre_out, far_out, drive_out, bx_out, cx_out, dtrt_out, tap_ref,
                 in_vm, norm_vm, inner, conv, pre, far, drive, act, bx, cx, keep_ref, ptv, osem,
                 a0, a1, a2, a3, p0, p1, p2, p3, b0, b1, b2, b3):
    xw, rank, state, gain_w, width = dims
    t = tok_ref.shape[0]
    low = jnp.bfloat16
    f = lax.axis_index("fsdp")
    fh = f // 2
    outs = []

    def put(src, dst):
        c = pltpu.make_async_copy(src, dst, osem.at[len(outs)])
        c.start()
        outs.append(c)

    enter_square()
    cut = sml_ref.shape[0] - 32
    sm = Spread(sml_ref.at[cut:], sml_out.at[:, cut:], a0, a1, a2, a3, 1)
    sp = Spread(sml_ref.at[:cut], sml_out.at[:, :cut], p0, p1, p2, p3, 1)
    di = inner.shape[1]
    wi = Spread(inw_ref.at[:, :di], in_vm, b0, b1, b2, b3, PARTS)
    own_i = pltpu.make_async_copy(inw_ref.at[:, :di], in_vm.at[f], osem.at[40])
    sm.begin()
    wi.begin()
    sp.begin()
    own_i.start()
    sml_out[f] = sml_ref[...]
    spot = lax.broadcasted_iota(jnp.int32, keep_ref.shape, 0)
    start = jnp.zeros_like(spot)
    run = 0
    for c in range(len_ref.shape[1] - 1):
        run = run + len_ref[0, c]
        start = jnp.where(spot >= run, run, start)
    keep_ref[...] = (spot > start).astype(jnp.float32)
    for j in (1, 2, 3):
        tap_ref[j - 1] = (spot - j >= start).astype(jnp.float32)

    def units(r, _):
        rs = pl.ds(pl.multiple_of(r * 32, 32), 32)
        x = tok_ref[rs, :].astype(jnp.float32)
        conv[rs, :x.shape[1]] = x * lax.rsqrt(jnp.mean(x * x, axis=-1, keepdims=True) + 1e-05)
        return 0

    lax.fori_loop(0, t // 32, units, 0)

    sm.pump(0)
    sm.pump_pair(0)
    sm.whole().wait_recv()
    sm.land()
    at = xw + rank + state
    def gains(r, _):
        rs = pl.ds(pl.multiple_of(r * 64, 64), 64)
        for s in range(4):
            ks, half = slice(s * gain_w, (s + 1) * gain_w), slice((s % 2) * gain_w, (s % 2 + 1) * gain_w)
            v = (conv[rs, ks] * sml_out[s, at + 7:at + 8, :gain_w].astype(jnp.float32)).astype(low)
            norm_vm[s // 2, rs, half] = v
            norm_out[rs, ks] = v
        return 0

    lax.fori_loop(0, t // 64, gains, 0)
    for s in range(4):
        normt_out[s * gain_w:(s + 1) * gain_w, :] = norm_vm[s // 2, :, (s % 2) * gain_w:(s % 2 + 1) * gain_w].T
    own_i.wait()
    wi.whole().wait_recv()
    tile = 256

    def block(h, first, base, dst):
        def go(n, _):
            cols = pl.ds(pl.multiple_of(base + n * tile, tile), tile)
            here = pl.ds(pl.multiple_of(n * tile, tile), tile)
            acc = jnp.dot(norm_vm[h], jnp.concatenate([in_vm[2 * h, :, cols], in_vm[2 * h + 1, :, cols]], axis=0), preferred_element_type=jnp.float32)
            dst[:, here] = acc if first else dst[:, here] + acc
            return 0
        lax.fori_loop(0, dst.shape[1] // tile, go, 0)

    block(fh, True, 0, inner)
    for i in range(PARTS):
        wi.pump(i)
        if i > 0:
            wi.pump_pair(i - 1)
    wi.pump_pair(PARTS - 1)
    wi.land()
    for s in range(4):
        put(in_vm.at[s], in_out.at[s])
    block(1 - fh, False, 0, inner)
    put(inner, inner_out)
    sp.pump(0)

    per = width // 128

    for s in range(4):
        def taps(q, _, s=s):
            ln = pl.ds(pl.multiple_of(s * width + q * 128, 128), 128)
            sl = pl.ds(pl.multiple_of(q * 128, 128), 128)
            v = inner[:, ln]
            w = [sml_out[s, at + k:at + k + 1, sl].astype(jnp.float32) for k in range(4)]
            acc = sml_out[s, at + 4:at + 5, sl].astype(jnp.float32) + w[3] * v
            for j in (1, 2, 3):
                acc = acc + w[3 - j] * (pltpu.roll(v, j, 0) * tap_ref[j - 1])
            conv[:, ln] = acc
            a = acc * jax.nn.sigmoid(acc)
            drive[:, ln] = a
            act[:, ln] = a.astype(low)
            return 0

        lax.fori_loop(0, per, taps, 0)
        put(conv.at[:, s * width:(s + 1) * width], conv_out.at[:, s * width:(s + 1) * width])

    sp.pump_pair(0)
    sp.whole().wait_recv()
    sp.land()
    pt = jnp.zeros((2 * state, t), jnp.float32)
    dr = jnp.zeros((t, rank), jnp.float32)
    drt = jnp.zeros((rank, t), jnp.float32)
    for s in range(4):
        al = act[:, s * width:(s + 1) * width]
        pt = pt + nt(sml_out[s, rank:xw, :], al)
        dr = dr + nt(al, sml_out[s, :rank, :])
        drt = drt + nt(sml_out[s, :rank, :], al)
    dtr = dr.astype(low)
    dtrt_out[...] = drt.astype(low)
    ptv[...] = pt

    def wide(tb, _):
        part = ptv[:, pl.ds(pl.multiple_of(tb * 128, 128), 128)]
        for l in range(128):
            col = jnp.broadcast_to(part[:, l:l + 1], (2 * state, 128))
            bx[tb * 128 + l] = col[:state]
            cx[tb * 128 + l] = col[state:]
        return 0

    lax.fori_loop(0, t // 128, wide, 0)
    put(bx, bx_out)
    put(cx, cx_out)
    for s in range(4):
        cs = slice(s * width, (s + 1) * width)
        p = jnp.dot(dtr, sml_out[s, xw:xw + rank, :], preferred_element_type=jnp.float32) + sml_out[s, at + 5:at + 6, :].astype(jnp.float32)
        pre[:, cs] = p
        put(pre.at[:, cs], pre_out.at[:, cs])

        def steps(q, _, s=s):
            ln = pl.ds(pl.multiple_of(s * width + q * 128, 128), 128)

            def rows(r, _):
                rs = pl.ds(pl.multiple_of(r * 128, 128), 128)
                v = pre[rs, ln]
                st = jnp.maximum(v, 0.0) + jnp.log1p(jnp.exp(-jnp.abs(v)))
                drive[rs, ln] = drive[rs, ln] * st
                far[rs, ln] = jnp.where(keep_ref[rs, :] > 0, st, 1e30)
                return 0

            return lax.fori_loop(0, t // 128, rows, 0)

        lax.fori_loop(0, per, steps, 0)
        put(far.at[:, cs], far_out.at[:, cs])
        put(drive.at[:, cs], drive_out.at[:, cs])
    for g in (sm, sp, wi):
        g.finish()
    for c in outs:
        c.wait()


def front(lengths, tokens, packed, in_weight, dims):
    xw, rank, state, gain_w, width = dims
    t, d = tokens.shape
    di = 4 * width
    low, f32 = jnp.bfloat16, jnp.float32
    vm = pl.BlockSpec(memory_space=pltpu.VMEM)
    hb = pl.BlockSpec(memory_space=pl.ANY)
    sds = jax.ShapeDtypeStruct
    wide = sds((t, di), f32)
    lanes = sds((t, state, 128), f32)
    return pl.pallas_call(
        functools.partial(front_kernel, dims),
        in_specs=[pl.BlockSpec(memory_space=pltpu.SMEM), vm, vm, hb],
        out_specs=[hb, vm, vm, vm, hb, hb, hb, hb, hb, hb, hb, vm, vm],
        out_shape=[sds((4, gain_w, di), low), sds((4,) + packed.shape, low), sds((t, d), low), sds((d, t), low),
                   wide, wide, wide, wide, wide, lanes, lanes, sds((rank, t), low), sds((3, t, 128), f32)],
        scratch_shapes=[pltpu.VMEM((4, gain_w, di), low), pltpu.VMEM((2, t, d // 2), low)]
        + [pltpu.VMEM((t, di), f32)] * 5 + [pltpu.VMEM((t, di), low)] + [pltpu.VMEM((t, state, 128), f32)] * 2
        + [pltpu.VMEM((t, 128), f32), pltpu.VMEM((2 * state, t), f32), pltpu.SemaphoreType.DMA((42,))] + spread_sems(1) * 2 + spread_sems(PARTS),
        compiler_params=pltpu.CompilerParams(collective_id=3, has_side_effects=True, vmem_limit_bytes=63 << 20),
        name="front",
    )(lengths, tokens, packed, in_weight)


BACK_ROWS = 64
BACK_COLS = 512
BACK_FIRST, BACK_DELAY, BACK_GATE, BACK_NEXT = 2.0, 6.5, 2.4, 1.6


def tn(a, b):
    return lax.dot_general(a, b, (((0,), (0,)), ((), ())), preferred_element_type=jnp.float32)


def sum8(v):
    return jnp.sum(v.reshape(v.shape[0] // 8, 8, v.shape[1]), axis=0)


def back_kernel(dp, dims, za_h, gb_h, pre_h, dys_h, conv_h, inner_h, ina_h, inb_h, gl_h, nt_h, gg_ref, tok_ref, cot_ref, sml_ref, dtrt_ref, dbt_ref, rate_ref, tap_ref,
                gsh_ref, ish_ref, ssh_ref, ig_ref,
                za, gb, pre, dys, conv, inner, ina, inb, gl, normt, prelow, actlow, pt, agv, misc, gainv, ng, isrc, ssrc, csem, *comm):
    xw, rank, state, gain_w, width = dims
    t = tok_ref.shape[0]
    low = jnp.bfloat16
    at = xw + rank + state
    per = width // 128

    def fetch(k, src, dst):
        c = pltpu.make_async_copy(src, dst, csem.at[k])
        c.start()
        return c

    def slab(s):
        cs = slice(s * width, (s + 1) * width)
        return [fetch(s * 8 + k, h.at[:, cs], v) for k, (h, v) in enumerate(((conv_h, conv.at[:, cs]), (gb_h, gb.at[s % 2]), (pre_h, pre.at[s % 2]), (dys_h, dys.at[:, cs]), (za_h, za.at[s % 2])))]

    waits = [slab(0), slab(1)]
    late = [fetch(32, inner_h, inner), fetch(33, nt_h, normt), fetch(34, ina_h, ina), fetch(35, gl_h, gl), fetch(36, inb_h, inb)]
    red = Reducer(dp, (gg_ref, isrc, ssrc), (gsh_ref, ish_ref, ssh_ref), comm, BACK_ROWS, BACK_COLS, [gg_ref.shape[3] // 2, 0, 0])
    red.entry()
    misc[...] = jnp.zeros_like(misc)
    points = [1.3 * (i + 1) for i in range(4 * per)] + [22.0 + 3.6 * s + 1.7 * (h + 1) for s in range(4) for h in range(2)]
    points += [36.5 + i for i in range(8)] + [46.0 + 0.8 * i for i in range(120)]
    entries, seen = [], [0, 0, 0]
    for a, r0, c0, w in red.chunks:
        here = 1.3 + seen[0] * BACK_GATE if a == 0 else 46.0 if a == 2 else 22.01 + 3.6 * (c0 // width + 1)
        entries.append(max(here, entries[-1] + BACK_NEXT if entries and a else here))
        seen[a] += 1
    plan = red.plan(entries, points, BACK_FIRST, BACK_DELAY)
    pos = [0]

    def tick():
        red.tick(plan[pos[0]])
        pos[0] += 1

    rankt = jnp.zeros((rank, t), jnp.float32)
    for s in range(4):
        for c in waits[s]:
            c.wait()

        def tile(q, _, s=s):
            ln = pl.ds(pl.multiple_of(s * width + q * 128, 128), 128)
            lq = pl.ds(pl.multiple_of(q * 128, 128), 128)
            skip = sml_ref[s, at + 6:at + 7, lq].astype(jnp.float32)

            def rows(r, sums):
                rs = pl.ds(pl.multiple_of(r * 64, 64), 64)
                cv = conv[rs, ln]
                sg = jax.nn.sigmoid(cv)
                ac = cv * sg
                gv = gb[s % 2, rs, lq]
                pv = pre[s % 2, rs, lq]
                dy = dys[rs, ln]
                st = jnp.maximum(pv, 0.0) + jnp.log1p(jnp.exp(-jnp.abs(pv)))
                pg = (za[s % 2, rs, lq] * LN2 + gv * ac) * jax.nn.sigmoid(pv)
                prelow[rs, lq] = pg.astype(low)
                actlow[rs, ln] = ac.astype(low)
                dys[rs, ln] = dy * skip + gv * st
                conv[rs, ln] = sg * (1.0 + cv * (1.0 - sg))
                return sums[0] + sum8(pg), sums[1] + sum8(dy * ac)

            zero = jnp.zeros((8, 128), jnp.float32)
            bias, skips = lax.fori_loop(0, t // 64, rows, (zero, zero))
            misc[5:6, ln] = jnp.sum(bias, axis=0, keepdims=True)
            misc[6:7, ln] = jnp.sum(skips, axis=0, keepdims=True)
            return 0

        for half in range(2):
            lax.fori_loop(half * (per // 2), (half + 1) * (per // 2), tile, 0)
            for _ in range(per // 2):
                tick()
        if s < 2:
            waits.append(slab(s + 2))
        p = prelow[...]
        ssrc[s // 2, s % 2, xw:xw + rank, :] = jnp.dot(dtrt_ref[...], p, preferred_element_type=jnp.float32).astype(low)
        rankt = rankt + nt(sml_ref[s, xw:xw + rank, :], p)
    pt[:rank] = rankt.astype(low)
    pt[rank:] = dbt_ref[...].astype(low)
    for c in late[:2]:
        c.wait()
    for s in range(4):
        cs = slice(s * width, (s + 1) * width)
        agv[...] = tn(pt[...], sml_ref[s, :xw, :])
        ssrc[s // 2, s % 2, :xw, :] = jnp.dot(pt[...], actlow[:, cs], preferred_element_type=jnp.float32).astype(low)
        ssrc[s // 2, s % 2, xw + rank:at, :] = (-rate_ref[:, cs] * jnp.exp(sml_ref[s, xw + rank:at, :].astype(jnp.float32))).astype(low)

        def tile2(q, _, s=s):
            ln = pl.ds(pl.multiple_of(s * width + q * 128, 128), 128)
            lq = pl.ds(pl.multiple_of(q * 128, 128), 128)
            cg = (agv[:, lq] + dys[:, ln]) * conv[:, ln]
            v = inner[:, ln]
            ig = sml_ref[s, at + 3:at + 4, lq].astype(jnp.float32) * cg
            misc[3:4, ln] = jnp.sum(sum8(cg * v), axis=0, keepdims=True)
            misc[4:5, ln] = jnp.sum(sum8(cg), axis=0, keepdims=True)
            for j in (1, 2, 3):
                m = cg * tap_ref[j - 1]
                misc[3 - j:4 - j, ln] = jnp.sum(sum8(m * pltpu.roll(v, j, 0)), axis=0, keepdims=True)
                ig = ig + sml_ref[s, at + 3 - j:at + 4 - j, lq].astype(jnp.float32) * pltpu.roll(m, t - j, 0)
            actlow[:, ln] = ig.astype(low)
            return 0

        for half in range(2):
            lax.fori_loop(half * (per // 2), (half + 1) * (per // 2), tile2, 0)
            tick()

        def grads(k, _, cs=cs):
            rows = pl.ds(pl.multiple_of(k * gain_w, gain_w), gain_w)
            isrc[k // 2, k % 2, :, cs] = jnp.dot(normt[rows, :], actlow[:, cs], preferred_element_type=jnp.float32).astype(low)
            return 0

        lax.fori_loop(0, 4, grads, 0)
    for c in late[2:]:
        c.wait()
    for blk in range(8):
        tick()
        src = gl if blk < 4 else actlow
        base = (blk % 4) * width
        wsrc = inb if blk < 4 else ina

        def back_in(k, _, blk=blk, src=src, wsrc=wsrc, base=base):
            rows = pl.ds(pl.multiple_of(k * gain_w, gain_w), gain_w)
            part = nt(src[:, base:base + width], wsrc[k, :, base:base + width])
            ng[:, rows] = part if blk == 0 else ng[:, rows] + part
            return 0

        lax.fori_loop(0, 4, back_in, 0)
    for k in range(4):
        gainv[0:1, k * gain_w:(k + 1) * gain_w] = sml_ref[k, at + 7:at + 8, :gain_w].astype(jnp.float32)

    def fin(r, acc):
        rs = pl.ds(pl.multiple_of(r * 32, 32), 32)
        x = tok_ref[rs, :].astype(jnp.float32)
        inv = lax.rsqrt(jnp.mean(x * x, axis=-1, keepdims=True) + 1e-05)
        u = x * inv
        d = ng[rs, :]
        e = d * gainv[0:1, :]
        ig_ref[rs, :] = cot_ref[rs, :].astype(jnp.float32) + inv * (e - u * jnp.mean(e * u, axis=-1, keepdims=True))
        return acc + sum8(d * u)

    gsum = lax.fori_loop(0, t // 32, fin, jnp.zeros((8, ng.shape[1]), jnp.float32))
    gsum = jnp.sum(gsum, axis=0, keepdims=True)
    for k in range(4):
        misc[7:8, k * width:k * width + gain_w] = gsum[:, k * gain_w:(k + 1) * gain_w]
    for k in range(4):
        ssrc[k // 2, k % 2, at:at + 16, :] = misc[:, k * width:(k + 1) * width].astype(low)
        if ssrc.shape[2] > at + 16:
            ssrc[k // 2, k % 2, at + 16:, :] = jnp.zeros((ssrc.shape[2] - at - 16, width), low)
    while pos[0] < len(plan):
        tick()
    red.finish()


def back(dp, dims, za, gb, pre, dys, conv, inner, in_a, in_b, gate_low, normt, gg, tokens, cot, small, dtrt, dbt, rate, tapb):
    xw, rank, state, gain_w, width = dims
    t, d = tokens.shape
    di = 4 * width
    low, f32 = jnp.bfloat16, jnp.float32
    unit = split_of(dp, BACK_ROWS)[1]
    srows = -(-(xw + rank + state + 16) // unit) * unit
    shapes = [(gain_w, di // 2), (gain_w, di), (srows, width)]
    vm = pl.BlockSpec(memory_space=pltpu.VMEM)
    hb = pl.BlockSpec(memory_space=pl.ANY)
    sds = jax.ShapeDtypeStruct
    return pl.pallas_call(
        functools.partial(back_kernel, dp, dims),
        in_specs=[hb] * 10 + [vm] * 8,
        out_specs=[vm] * 4,
        out_shape=[sds(shapes[0], low), sds(shapes[1], low), sds(shapes[2], low), sds((t, d), f32)],
        scratch_shapes=[pltpu.VMEM((2, t, width), f32)] * 3 + [pltpu.VMEM((t, di), f32)] * 3
        + [pltpu.VMEM(in_a.shape, low), pltpu.VMEM(in_b.shape, low), pltpu.VMEM((t, di), low), pltpu.VMEM((d, t), low), pltpu.VMEM((t, width), low), pltpu.VMEM((t, di), low),
           pltpu.VMEM((xw, t), low), pltpu.VMEM((t, width), f32), pltpu.VMEM((16, di), f32), pltpu.VMEM((8, d), f32), pltpu.VMEM((t, d), f32),
           pltpu.VMEM((2, 2) + shapes[1], low), pltpu.VMEM((2, 2) + shapes[2], low), pltpu.SemaphoreType.DMA((37,))]
        + reducer_scratch(dp, shapes, BACK_ROWS, BACK_COLS),
        compiler_params=pltpu.CompilerParams(collective_id=1, has_side_effects=True, vmem_limit_bytes=63 << 20),
        name="back",
    )(za, gb, pre, dys, conv, inner, in_a, in_b, gate_low, normt, gg.reshape((2, 2, gain_w, di)), tokens, cot, small, dtrt, dbt, rate, tapb)


def last_kernel(dims, i_ref, ga_ref, gb_ref, o_ref, s_ref, x_ref, xo_ref, in_ref, og_ref, gain_ref, cw_ref, cb_ref, xp_ref, dw_ref, db_ref, al_ref, sk_ref):
    xw, rank, state, gain_w, width = dims
    f32 = jnp.float32
    half = i_ref.shape[1]
    n = 16
    step_i, step_o, step_x = i_ref.shape[0] // n, o_ref.shape[0] // n, x_ref.shape[0] // n

    def rows(r, _):
        ri, ro, rx = (pl.ds(pl.multiple_of(r * v, v), v) for v in (step_i, step_o, step_x))
        xo_ref[rx, :] = x_ref[rx, :]
        in_ref[ri, :half] = i_ref[ri, :].astype(f32)
        in_ref[ri, half:half + half // 2] = ga_ref[ri, :].astype(f32)
        in_ref[ri, half + half // 2:] = gb_ref[ri, :].astype(f32)
        og_ref[ro, :] = o_ref[ro, :].astype(f32)
        return 0

    lax.fori_loop(0, n, rows, 0)
    at = xw + rank + state
    xp_ref[...] = s_ref[:xw, :].astype(f32)
    dw_ref[...] = s_ref[xw:xw + rank, :].astype(f32)
    al_ref[...] = s_ref[xw + rank:at, :].astype(f32)
    tail = s_ref[at:at + 16, :].astype(f32)
    cw_ref[...] = tail[:4]
    cb_ref[...] = tail[4:5]
    db_ref[...] = tail[5:6]
    sk_ref[...] = tail[6:7]
    gain_ref[...] = tail[7:8, :gain_w]


def last(dims, ish, gsa, gsb, osh, ssh, grad):
    xw, rank, state, gain_w, width = dims
    f32 = jnp.float32
    sds = jax.ShapeDtypeStruct
    vm = pl.BlockSpec(memory_space=pltpu.VMEM)
    return pl.pallas_call(
        functools.partial(last_kernel, dims),
        in_specs=[vm] * 6,
        out_specs=[vm] * 11,
        out_shape=[sds(grad.shape, f32), sds((ish.shape[0], 2 * ish.shape[1]), f32), sds(osh.shape, f32), sds((1, gain_w), f32), sds((4, width), f32), sds((1, width), f32),
                   sds((xw, width), f32), sds((rank, width), f32), sds((1, width), f32), sds((state, width), f32), sds((1, width), f32)],
        compiler_params=pltpu.CompilerParams(vmem_limit_bytes=63 << 20),
        name="last",
    )(ish, gsa, gsb, osh, ssh, grad)


LANE = 128
NS = 16
TC = 64
CGF = 1024
CGB = 512


def bcast(ref, i, row):
    v = ref[i, pl.ds(row, 8, stride=0), :]
    return jnp.concatenate([v, v], axis=0)


def stage(src, dst):
    for i in range(dst.shape[0]):
        dst[i] = src[:, i * LANE:(i + 1) * LANE]


def fold(src, i):
    s = [src[i, pl.ds(q, 8, stride=8), :] for q in range(8)]
    return ((s[0] + s[1]) + (s[2] + s[3])) + ((s[4] + s[5]) + (s[6] + s[7]))


def fwd_kernel(dt_ref, dr_ref, b_ref, c_ref, a_ref, inw_ref, outw_ref, y_ref, hs_ref, inb_ref, all_ref,
               part, dts, drs, hst, bi, bo, lsem, b0, b1, b2, b3, c0, c1, c2, c3):
    step = pl.program_id(0) * pl.num_programs(1) + pl.program_id(1)
    di = inb_ref.shape[2]
    f = lax.axis_index("fsdp")
    wb = Spread(inw_ref.at[:, di:], inb_ref, b0, b1, b2, b3, PARTS)
    wo = Spread(outw_ref, all_ref, c0, c1, c2, c3, PARTS)
    into = [pltpu.make_async_copy(inw_ref.at[:, di:], bi, lsem.at[0]), pltpu.make_async_copy(outw_ref, bo, lsem.at[1])]
    away = [pltpu.make_async_copy(bi, inb_ref.at[f], lsem.at[2]), pltpu.make_async_copy(bo, all_ref.at[f], lsem.at[3])]

    @pl.when(step == 0)
    def _():
        enter_square()
        wb.begin()
        for c in into:
            c.start()

    @pl.when(step == 1)
    def _():
        for c in into:
            c.wait()
        for c in away:
            c.start()

    @pl.when(step == LATE)
    def _():
        wo.begin()

    for i in range(2 * PARTS):
        @pl.when(step == PUMPS[i])
        def _(i=i):
            (wb if i < PARTS else wo).pump(i % PARTS)
            if i > 0:
                (wb if i - 1 < PARTS else wo).pump_pair((i - 1) % PARTS)

    @pl.when(step == pl.num_programs(0) * pl.num_programs(1) - 1)
    def _():
        wo.pump_pair(PARTS - 1)
        for w in (wb, wo):
            w.whole().wait_recv()
            w.land()
            w.finish()
        for c in away:
            c.wait()

    cg = dt_ref.shape[1]
    tiles = cg // LANE
    tc = dt_ref.shape[0]

    @pl.when(pl.program_id(1) == 0)
    def _():
        hst[...] = jnp.zeros_like(hst)

    stage(dt_ref, dts)
    stage(dr_ref, drs)

    def group(g, carry):
        t0 = pl.multiple_of(g * 8, 8)
        hs = list(carry)
        for k in range(8):
            bt = b_ref[t0 + k]
            ct = c_ref[t0 + k]
            for i in range(tiles):
                ln = slice(i * LANE, (i + 1) * LANE)
                d = bcast(dts, i, t0 + k)
                u = bcast(drs, i, t0 + k)
                a = jnp.exp2(d * a_ref[:, ln])
                hs_ref[0, t0 + k, :, ln] = hs[i]
                h = a * hs[i] + bt * u
                hs[i] = h
                p = ct * h
                part[i, k * 8:(k + 1) * 8, :] = p[:8] + p[8:]
        for i in range(tiles):
            ln = slice(i * LANE, (i + 1) * LANE)
            y_ref[pl.ds(t0, 8), ln] = fold(part, i)
        return tuple(hs)

    init = tuple(hst[:, i * LANE:(i + 1) * LANE] for i in range(tiles))
    out = lax.fori_loop(0, tc // 8, group, init, unroll=2)
    for i in range(tiles):
        hst[:, i * LANE:(i + 1) * LANE] = out[i]
        hs_ref[0, tc, :, i * LANE:(i + 1) * LANE] = out[i]


PUMPS = (2, 4, 6, 8, 10, 12, 13, 14)
LATE = 0


def scan_forward(dt, dr, bx, cx, a2, in_weight, out_weight, tc=TC, cg=CGF):
    t, c = dt.shape
    nt, nc = t // tc, c // cg
    assert nt * nc > PUMPS[-1]
    return pl.pallas_call(
        fwd_kernel,
        grid=(nc, nt),
        in_specs=[
            pl.BlockSpec((tc, cg), lambda j, i: (i, j)),
            pl.BlockSpec((tc, cg), lambda j, i: (i, j)),
            pl.BlockSpec((tc, NS, LANE), lambda j, i: (i, 0, 0)),
            pl.BlockSpec((tc, NS, LANE), lambda j, i: (i, 0, 0)),
            pl.BlockSpec((NS, cg), lambda j, i: (0, j)),
            pl.BlockSpec(memory_space=pl.ANY),
            pl.BlockSpec(memory_space=pl.ANY),
        ],
        out_specs=[
            pl.BlockSpec((tc, cg), lambda j, i: (i, j)),
            pl.BlockSpec((1, tc + 1, NS, cg), lambda j, i: (i, 0, 0, j)),
            pl.BlockSpec(memory_space=pl.ANY),
            pl.BlockSpec(memory_space=pl.ANY),
        ],
        out_shape=[
            jax.ShapeDtypeStruct((t, c), jnp.float32),
            jax.ShapeDtypeStruct((nt, tc + 1, NS, c), jnp.float32),
            jax.ShapeDtypeStruct((4, in_weight.shape[0], c), jnp.bfloat16),
            jax.ShapeDtypeStruct((4,) + out_weight.shape, jnp.bfloat16),
        ],
        scratch_shapes=[pltpu.VMEM((cg // LANE, 64, LANE), jnp.float32)] + [pltpu.VMEM((cg // LANE, tc, LANE), jnp.float32)] * 2 + [pltpu.VMEM((NS, cg), jnp.float32), pltpu.VMEM((in_weight.shape[0], c), jnp.bfloat16), pltpu.VMEM(out_weight.shape, jnp.bfloat16), pltpu.SemaphoreType.DMA((4,))] + spread_sems(PARTS) * 2,
        compiler_params=pltpu.CompilerParams(vmem_limit_bytes=63 << 20, collective_id=4, has_side_effects=True),
        name="scan_forward",
    )(dt, dr, bx, cx, a2, in_weight, out_weight)


def bwd_kernel(dp, steps, dt_ref, dr_ref, dy_ref, b_ref, c_ref, a_ref, hs_ref, og_ref, gg_ref,
               za_ref, gb_ref, dbt_ref, rate_ref, os_ref, gs_ref,
               db_ref, dc_ref, pz, pg, dts, drs, dys, gst, rst, ores, gres, *comm):
    red = Reducer(dp, (og_ref, gg_ref), (ores, gres), comm, SCAN_ROWS)
    step = pl.program_id(0) * pl.num_programs(1) + pl.program_id(1)
    count = len(red.chunks)
    plan = red.plan([k * SCAN_RATE for k in range(count)], range(steps), SCAN_FIRST, SCAN_DELAY)

    def tree(lo, hi):
        if hi - lo == 1:
            if lo == 0:
                red.entry()
            red.tick(plan[lo])
            return
        mid = (lo + hi) // 2
        lax.cond(step < mid, lambda: tree(lo, mid), lambda: tree(mid, hi))

    tree(0, steps)

    @pl.when(step == pl.num_programs(0) * pl.num_programs(1) - 1)
    def _():
        red.finish()
        os_ref[...] = ores[...]
        gs_ref[...] = gres[...]

    cg = dt_ref.shape[1]
    tiles = cg // LANE
    tc = dt_ref.shape[0]
    j = pl.program_id(0)
    i_t = pl.program_id(1)
    nt = pl.num_programs(1)

    @pl.when(i_t == 0)
    def _():
        gst[...] = jnp.zeros_like(gst)
        rst[...] = jnp.zeros_like(rst)

    @pl.when(step == 0)
    def _():
        db_ref[...] = jnp.zeros_like(db_ref)
        dc_ref[...] = jnp.zeros_like(dc_ref)

    stage(dt_ref, dts)
    stage(dr_ref, drs)
    stage(dy_ref, dys)
    lanes = [slice(i * LANE, (i + 1) * LANE) for i in range(tiles)]

    base = pl.multiple_of((nt - 1 - i_t) * tc, tc)

    def bgroup(gi, carry):
        g = tc // 8 - 1 - gi
        t0 = pl.multiple_of(g * 8, 8)
        gs = list(carry[0])
        rs = list(carry[1])
        for k in range(7, -1, -1):
            bt = b_ref[t0 + k]
            ct = c_ref[t0 + k]
            accb = None
            for i in range(tiles):
                ln = lanes[i]
                d = bcast(dts, i, t0 + k)
                u = bcast(drs, i, t0 + k)
                w = bcast(dys, i, t0 + k)
                hnow = hs_ref[0, t0 + k + 1, :, ln]
                hprev = hs_ref[0, t0 + k, :, ln]
                a = jnp.exp2(d * a_ref[:, ln])
                gg = ct * w + gs[i]
                ga = gg * a
                z = ga * hprev
                rs[i] = rs[i] + z * d
                gs[i] = ga
                pa = z * a_ref[:, ln]
                pz[i, k * 8:(k + 1) * 8, :] = pa[:8] + pa[8:]
                pb = gg * bt
                pg[i, k * 8:(k + 1) * 8, :] = pb[:8] + pb[8:]
                vb = gg * u
                vc = w * hnow
                accb = vb if accb is None else accb + vb
                accc = vc if i == 0 else accc + vc
            row = base + t0 + k

            db_ref[row] = db_ref[row] + accb
            dc_ref[row] = dc_ref[row] + accc
        for i in range(tiles):
            ln = lanes[i]
            za_ref[pl.ds(t0, 8), ln] = fold(pz, i)
            gb_ref[pl.ds(t0, 8), ln] = fold(pg, i)
        return tuple(gs), tuple(rs)

    gs, rs = lax.fori_loop(0, tc // 8, bgroup, (tuple(gst[:, ln] for ln in lanes), tuple(rst[:, ln] for ln in lanes)), unroll=2)
    for i in range(tiles):
        gst[:, lanes[i]] = gs[i]
        rst[:, lanes[i]] = rs[i]

    @pl.when(i_t == nt - 1)
    def _():
        rate_ref[...] = rst[...]

    @pl.when(j == pl.num_programs(0) - 1)
    def _():
        block = pl.ds(pl.multiple_of((base // LANE) * LANE, LANE), LANE)
        lane = lax.broadcasted_iota(jnp.int32, (NS, LANE), 1)
        at = base % LANE

        def put(k, accs):
            row = base + k
            hit = lane == at + k
            return (jnp.where(hit, jnp.sum(db_ref[row], axis=-1, keepdims=True), accs[0]),
                    jnp.where(hit, jnp.sum(dc_ref[row], axis=-1, keepdims=True), accs[1]))

        got = lax.fori_loop(0, tc, put, (dbt_ref[:NS, block], dbt_ref[NS:, block]), unroll=8)
        dbt_ref[:NS, block] = got[0]
        dbt_ref[NS:, block] = got[1]


def scan_backward(dp, dt, dr, dy, bx, cx, a2, hs, og, gg, tc=TC, cg=CGB):
    t, c = dt.shape
    nt, nc = t // tc, c // cg
    row = pl.BlockSpec((tc, cg), lambda j, i: (nt - 1 - i, j))
    bc = pl.BlockSpec((tc, NS, LANE), lambda j, i: (nt - 1 - i, 0, 0))
    once = lambda s: pl.BlockSpec(s, lambda j, i: (0,) * len(s), pipeline_mode=pl.Buffered(1))
    og = og.reshape((2, 2) + og.shape[1:])
    gg = gg.reshape((2, 2) + gg.shape[1:])
    parts = [og.shape[2:], (gg.shape[2], gg.shape[3] // 2)]
    return pl.pallas_call(
        functools.partial(bwd_kernel, dp, nc * nt),
        grid=(nc, nt),
        in_specs=[row, row, row, bc, bc, pl.BlockSpec((NS, cg), lambda j, i: (0, j)),
                  pl.BlockSpec((1, tc + 1, NS, cg), lambda j, i: (nt - 1 - i, 0, 0, j)), once(og.shape), once((2, 2) + parts[1])],
        out_specs=[row, row, once((2 * NS, t)), pl.BlockSpec((NS, cg), lambda j, i: (0, j)), once(parts[0]), once(parts[1])],
        out_shape=[
            jax.ShapeDtypeStruct((t, c), jnp.float32),
            jax.ShapeDtypeStruct((t, c), jnp.float32),
            jax.ShapeDtypeStruct((2 * NS, t), jnp.float32),
            jax.ShapeDtypeStruct((NS, c), jnp.float32),
            jax.ShapeDtypeStruct(parts[0], jnp.bfloat16),
            jax.ShapeDtypeStruct(parts[1], jnp.bfloat16),
        ],
        scratch_shapes=[
            pltpu.VMEM((t, NS, LANE), jnp.float32), pltpu.VMEM((t, NS, LANE), jnp.float32),
            pltpu.VMEM((cg // LANE, 64, LANE), jnp.float32), pltpu.VMEM((cg // LANE, 64, LANE), jnp.float32),
            pltpu.VMEM((cg // LANE, tc, LANE), jnp.float32), pltpu.VMEM((cg // LANE, tc, LANE), jnp.float32), pltpu.VMEM((cg // LANE, tc, LANE), jnp.float32),
            pltpu.VMEM((NS, cg), jnp.float32), pltpu.VMEM((NS, cg), jnp.float32),
            pltpu.VMEM(parts[0], jnp.bfloat16), pltpu.VMEM(parts[1], jnp.bfloat16),
        ] + reducer_scratch(dp, parts, SCAN_ROWS),
        compiler_params=pltpu.CompilerParams(vmem_limit_bytes=60 << 20, collective_id=2, has_side_effects=True),
        name="scan_backward",
    )(dt, dr, dy, bx, cx, a2, hs, og, gg)


def pack_small(gain, conv_w, conv_b, xproj, dt_w, dt_b, alog, skip):
    width = conv_b.shape[-1]
    gain_row = jnp.pad(gain[None], ((0, 0), (0, width - gain.shape[0])))
    return jnp.concatenate(
        [xproj.T, dt_w, alog, conv_w, conv_b[None], dt_b[None], skip[None], gain_row], axis=0
    )


def body(
    tokens,
    cluster_lengths,
    norm_gain,
    in_weight,
    conv_weight,
    conv_bias,
    xproj_weight,
    dt_weight,
    dt_bias,
    a_log,
    skip_gain,
    out_weight,
    cotangent,
):
    low = jnp.bfloat16
    gain_shard = norm_gain.shape[0]
    width = conv_bias.shape[0]
    packed = pack_small(norm_gain, conv_weight, conv_bias, xproj_weight, dt_weight, dt_bias, a_log, skip_gain)
    packed = jnp.pad(packed, ((0, -packed.shape[0] % 32), (0, 0)))
    shards = lax.axis_size("fsdp")
    xw, rank, state = xproj_weight.shape[1], dt_weight.shape[0], a_log.shape[0]
    inner_width = shards * width
    (in_a, small, normed_low, normed_t, inner_in, conv_out, dt_pre, step_far, drive, bx, cx, dt_t, tapb) = front(
        cluster_lengths, tokens, packed, in_weight, (xw, rank, state, gain_shard, width)
    )
    rows = jnp.moveaxis(small, 0, 1).reshape(small.shape[1], inner_width)
    at = xw + rank
    decay_rate = -jnp.exp(rows[at : at + state].astype(jnp.float32))
    at += state
    at += KCONV
    skip_value = rows[at + 2].astype(jnp.float32)
    inputs_full = tokens.astype(jnp.float32)
    conv_act = silu_of(conv_out)
    rate2 = decay_rate * LOG2E
    scanned, starts, in_b, out_all = scan_forward(step_far, drive, bx, cx, rate2, in_weight, out_weight)
    out_full = out_all.reshape(-1, out_weight.shape[1])
    gate_in = matmul(normed_low, in_b.reshape(-1, inner_width))
    with_skip = scanned + skip_value * conv_act
    gate_act = silu_of(gate_in)
    gated_low = (with_skip * gate_act).astype(low)
    result = inputs_full + matmul(gated_low, out_full)
    output = result.astype(low)
    out_grad = left_inner(gated_low, cotangent)
    gated_grad = right_inner(cotangent, out_full)
    skip_part = gated_grad * gate_act
    gate_grad = gated_grad * with_skip * silu_slope(gate_in)
    gate_low = gate_grad.astype(low)
    gate_low_grad = left_inner(normed_low, gate_low).astype(low).reshape(shards, -1, inner_width)
    dp = lax.axis_size("dp")
    za, gb, dbt, rate_grad, out_share, gate_share_a = scan_backward(
        dp,
        step_far,
        drive,
        skip_part,
        bx,
        cx,
        rate2,
        starts,
        out_grad.astype(low).reshape(shards, -1, out_grad.shape[1]),
        gate_low_grad,
    )
    gate_share, inner_share, small_share, input_grad = back(
        dp, (xw, rank, state, gain_shard, width), za, gb, dt_pre, skip_part, conv_out, inner_in, in_a, in_b, gate_low,
        normed_t, gate_low_grad, tokens, cotangent, small, dt_t, dbt, rate_grad, tapb,
    )
    input_grad, in_grad, out_weight_grad, gain_g, conv_g, conv_b, xproj_g, dt_g, dt_b, alog_g, skip_g = last(
        (xw, rank, state, gain_shard, width), inner_share, gate_share_a, gate_share, out_share, small_share, input_grad
    )
    return (
        output, input_grad, gain_g[0], in_grad, conv_g, conv_b[0], xproj_g.T, dt_g, dt_b[0], alog_g, skip_g[0], out_weight_grad
    )


def solution(mesh):
    in_specs = (
        P(("dp", "fsdp"), None),
        P(("dp", "fsdp"), None),
        P("fsdp"),
        P("fsdp", None),
        P(None, "fsdp"),
        P("fsdp"),
        P("fsdp", None),
        P(None, "fsdp"),
        P("fsdp"),
        P(None, "fsdp"),
        P("fsdp"),
        P("fsdp", None),
        P(("dp", "fsdp"), None),
    )
    out_specs = (
        P(("dp", "fsdp"), None),
        P(("dp", "fsdp"), None),
        P("fsdp"),
        P("fsdp", None),
        P(None, "fsdp"),
        P("fsdp"),
        P("fsdp", None),
        P(None, "fsdp"),
        P("fsdp"),
        P(None, "fsdp"),
        P("fsdp"),
        P("fsdp", None),
    )
    return jax.shard_map(body, mesh=mesh, in_specs=in_specs, out_specs=out_specs, check_vma=False)
```
